256 devices in a mesh: seq: 8 (over z), tensor: 8 (over x, y_hi), dp: 4 (over y_lo, core).
Axes of the slice: x: 4, y: 4 (y_hi: 2, y_lo: 2; y = y_hi * 2 + y_lo), z: 8, core: 2. Of those that a mesh axis runs over, the one named last changes fastest.
Arguments:
- tokens: bfloat16 [4, 2048, 3072], P('dp', 'seq'), may hold values from -6 to 6
- cotangent: bfloat16 [4, 2048, 3072], P('dp', 'seq'), may hold values from -6 to 6
- qkv_weight: bfloat16 [3072, 3, 3072], P(('seq', 'dp'), None, 'tensor'), may hold values from -0.109375 to 0.109375
- out_weight: bfloat16 [3072, 3072], P(('seq', 'dp'), 'tensor'), may hold values from -0.109375 to 0.109375
Outputs:
- qkv_grad: float32 [3072, 3, 3072], P(('seq', 'dp'), None, 'tensor')
- out_grad: float32 [3072, 3072], P(('seq', 'dp'), 'tensor')
- branch_grad: bfloat16 [4, 2048, 3072], P('dp', 'seq', 'tensor')
The draws below stay inside these ranges and needn't reach their ends.
All inputs are finite; a program needn't handle non-finite values.
Results may differ from the reference program's by a relative error of at most 0.025.
Values may be sent and summed in bfloat16 or wider, within the bound.
A program may use at most 128 MiB of HBM per device.

```python
import jax
import jax.numpy as jnp
from jax import lax

D = 3072
HD = 128
TOK_DEV = 256
HEADS = 24
SEQ_LEN = 2048
BATCH = 4
N_SEQ = 8


def strengthened(drawn, key, source, target, blocks, factor):
    def block_of(axis_at):
        return (jnp.arange(drawn.shape[axis_at]) // (drawn.shape[axis_at] // blocks)).reshape((-1,) + (1,) * (drawn.ndim - 1 - axis_at))

    near = jax.random.permutation(key, blocks)[block_of(target)]
    second = (block_of(target) + blocks // 2) % blocks
    return jnp.where((block_of(source) == near) | (block_of(source) == second), factor * drawn, drawn)


def block_scale(stream_key, dims, shards, low, largest):
    loudness = 1.0
    for axis_at, blocks in shards:
        draws = jax.random.uniform(jax.random.fold_in(jax.random.fold_in(stream_key, 6), axis_at), (blocks,), jnp.float32, low / len(shards), largest / len(shards))
        loudness = loudness * jnp.repeat(jnp.exp(draws), dims[axis_at] // blocks).reshape((-1,) + (1,) * (len(dims) - 1 - axis_at))
    return loudness


def bell_draw(stream_key, extent, scale, most, split=(), held_as=jnp.bfloat16):
    values = jax.random.normal(stream_key, extent, jnp.float32) * scale
    if len(split) > 0:
        values = block_scale(stream_key, extent, split, -0.22, 0.18) * values
    return jnp.clip(values, min=-most, max=most).astype(held_as)


def bell_draw_with(rng, extent, scale, reach, shards, heavy, kind=jnp.bfloat16):
    result = scale * jax.random.normal(rng, extent, jnp.float32)
    if shards:
        result = result * block_scale(rng, extent, shards, -0.22, 0.18)
    return jnp.clip(strengthened(result, jax.random.fold_in(rng, 3), *heavy), -reach, reach).astype(kind)


def setup_inputs(seed: int = 0) -> dict:
    seeds = jax.random.split(jax.random.key(seed), 5)
    return {
        "tokens": bell_draw_with(seeds[0], (BATCH, SEQ_LEN, D), 1.0, 6.0, ((0, 4), (1, 8)), (1, 2, 8, 2.0)),
        "cotangent": bell_draw_with(seeds[1], (BATCH, SEQ_LEN, D), 1.0, 6.0, ((0, 4), (1, 8)), (1, 2, 8, 2.0)),
        "qkv_weight": bell_draw(seeds[2], (D, 3, HEADS * HD), D ** -0.5, 0.109375, ((0, 32), (2, 8))),
        "out_weight": bell_draw(seeds[3], (D, HEADS * HD), (HEADS * HD) ** -0.5, 0.109375, ((0, 32), (1, 8))),
    }


epsilon = 1e-06

def normalize(values):
    average = lax.optimization_barrier(jnp.mean(values, axis=-1, keepdims=True))
    centered = values - average
    inverse = lax.rsqrt(lax.optimization_barrier(jnp.mean(centered * centered, axis=-1, keepdims=True)) + epsilon)
    return (centered * inverse, inverse)

def normalize_back(gradient, normed, inverse):
    mean_grad = lax.optimization_barrier(jnp.mean(gradient, axis=-1, keepdims=True))
    mean_both = lax.optimization_barrier(jnp.mean(gradient * normed, axis=-1, keepdims=True))
    return (gradient - mean_grad - normed * mean_both) * inverse

def narrow(values):
    return lax.optimization_barrier(values.astype(jnp.bfloat16)).astype(jnp.float32)

def reference(tokens, cotangent, qkv_weight, out_weight):
    all_columns = HEADS * HD
    score_scale = HD ** (-0.5)
    flat_weight = qkv_weight.reshape(D, 3 * all_columns)
    qkv_total = jnp.zeros((D, 3 * all_columns), jnp.float32)
    out_total = jnp.zeros((D, all_columns), jnp.float32)
    branches = []
    for batch_row in range(BATCH):
        row_grads = cotangent[batch_row]
        normed, inverse = normalize(tokens[batch_row].astype(jnp.float32))
        unit_low = normed.astype(jnp.bfloat16)
        projected = jnp.dot(unit_low, flat_weight, preferred_element_type=jnp.float32)
        query_unit, query_inv = normalize(projected[:, :all_columns].reshape(SEQ_LEN, HEADS, HD))
        key_unit, key_inv = normalize(projected[:, all_columns:2 * all_columns].reshape(SEQ_LEN, HEADS, HD))
        query_low = narrow(query_unit)
        key_low = narrow(key_unit)
        value_low = narrow(projected[:, 2 * all_columns:].reshape(SEQ_LEN, HEADS, HD))
        scores = jnp.einsum('qhd,khd->hqk', query_low, key_low) * score_scale
        exponent = jnp.exp(scores)
        exp_total = lax.optimization_barrier(jnp.sum(exponent, axis=-1))
        attended = jnp.einsum('hqk,khd->qhd', narrow(exponent), value_low) / exp_total.T[:, :, None]
        attended_low = attended.astype(jnp.bfloat16)
        attended_wide = lax.optimization_barrier(attended_low).astype(jnp.float32)
        grad_low = jnp.dot(row_grads, out_weight, preferred_element_type=jnp.float32).astype(jnp.bfloat16)
        grad_wide = lax.optimization_barrier(grad_low).astype(jnp.float32).reshape(SEQ_LEN, HEADS, HD)
        row_delta = lax.optimization_barrier(jnp.sum(grad_wide * attended_wide, axis=-1))
        probability = exponent / exp_total[:, :, None]
        prob_grad = jnp.einsum('qhd,khd->hqk', grad_wide, value_low)
        grad_score = narrow(probability * (prob_grad - row_delta.T[:, :, None]) * score_scale)
        query_raw = jnp.einsum('hqk,khd->qhd', grad_score, key_low)
        key_raw = jnp.einsum('hqk,qhd->khd', grad_score, query_low)
        value_raw = jnp.einsum('hqk,qhd->khd', narrow(probability), grad_wide)
        query_back = normalize_back(query_raw, query_unit, query_inv)
        key_back = normalize_back(key_raw, key_unit, key_inv)
        qkv_low = jnp.concatenate([query_back.reshape(SEQ_LEN, all_columns), key_back.reshape(SEQ_LEN, all_columns), value_raw.reshape(SEQ_LEN, all_columns)], axis=1).astype(jnp.bfloat16)
        inner_grad = jnp.dot(qkv_low, flat_weight.T, preferred_element_type=jnp.float32)
        branches.append(normalize_back(inner_grad, normed, inverse).astype(jnp.bfloat16))
        attended_flat = attended_low.reshape(SEQ_LEN, all_columns)
        for block_index in range(N_SEQ):
            low_row = block_index * TOK_DEV
            high_row = low_row + TOK_DEV
            qkv_total = qkv_total + narrow(jnp.dot(unit_low[low_row:high_row].T, qkv_low[low_row:high_row], preferred_element_type=jnp.float32))
            out_total = out_total + narrow(jnp.dot(row_grads[low_row:high_row].T, attended_flat[low_row:high_row], preferred_element_type=jnp.float32))
    return (qkv_total.reshape(D, 3, all_columns), out_total, jnp.stack(branches))
```

```python
import jax
import jax.numpy as jnp
from jax import lax
from jax.experimental import pallas as pl
from jax.experimental.pallas import tpu as pltpu
from jax.sharding import PartitionSpec as P

HD = 128
MESH = pl.DeviceIdType.MESH
F32 = jnp.float32
BF16 = jnp.bfloat16


epsilon = 1e-06


def sent_together(arrays, axis, dim, along):
    both = jnp.concatenate(arrays, axis=along)
    result, at, done = (lax.all_gather(both, axis, axis=dim, tiled=True), 0, [])
    for a in arrays:
        done.append(lax.slice_in_dim(result, at, at + a.shape[along], axis=along))
        at += a.shape[along]
    return tuple(done)


def split_up(shard, dim, size):
    before, after = (shard.shape[:dim], shard.shape[dim + 1 :])
    return jnp.moveaxis(shard.reshape(*before, size, -1, *after), dim, 0)


def summed_on_arrival(shard, axis, dim):
    size = lax.axis_size(axis)
    pieces = lax.all_to_all(split_up(shard, dim, size), axis, 0, 0, tiled=True)
    return jnp.sum(pieces.astype(jnp.float32), axis=0)


def copy_for_each(shard, axis):
    copies = jnp.broadcast_to(shard, (lax.axis_size(axis), *shard.shape))
    return lax.all_to_all(copies, axis, split_axis=0, concat_axis=0, tiled=True)


def taken_together(shard, axis):
    everything = copy_for_each(shard, axis)
    return jnp.sum(everything, axis=0)


def in_one(arrays, axis):
    ends = [0]
    for a in arrays:
        ends.append(ends[-1] + a.size)
    subtotal = taken_together(jnp.concatenate([a.ravel() for a in arrays]), axis)
    return tuple((subtotal[b:e].reshape(a.shape) for a, b, e in zip(arrays, ends, ends[1:])))


def normalize(values):
    average = jnp.mean(values, axis=-1, keepdims=True)
    centered = values - average
    inverse = lax.rsqrt(jnp.mean(centered * centered, axis=-1, keepdims=True) + epsilon)
    return (centered * inverse, inverse)


def normalize_back(gradient, normed, inverse):
    mean_grad = jnp.mean(gradient, axis=-1, keepdims=True)
    mean_both = jnp.mean(gradient * normed, axis=-1, keepdims=True)
    return (gradient - mean_grad - normed * mean_both) * inverse


NZ = 8


def twice(a):
    return jnp.concatenate([a, a], axis=1)


def lane_mean(a):
    return jnp.broadcast_to(jnp.mean(a, axis=1, keepdims=True), a.shape)


def attention_kernel(
    heads,
    proj,
    grad,
    qkv_out,
    att_out,
    q_low,
    do,
    unit,
    inv,
    kv,
    ex,
    dp,
    wsum,
    tsum,
    rtot,
    delta,
    dq,
    part,
    sbuf,
    rbuf,
    send_ag,
    recv_ag,
    send_rs,
    recv_rs,
):
    me = lax.axis_index("seq")
    sides = (lax.rem(me + 1, NZ), lax.rem(me + NZ - 1, NZ))
    scale = HD ** (-0.5)
    width = heads * HD

    barrier = pltpu.get_barrier_semaphore()
    for side in sides:
        pl.semaphore_signal(barrier, inc=1, device_id={"seq": side}, device_id_type=MESH)

    for h in range(heads):
        for j in range(2):
            a = proj[:, (j * heads + h) * HD : (j * heads + h + 1) * HD]
            c = a - lane_mean(a)
            r = lax.rsqrt(lane_mean(c * c) + epsilon)
            u = c * r
            unit[j, h] = u
            inv[j, h] = r
            if j == 0:
                q_low[h] = u.astype(BF16)
            else:
                kv[me, 0, h] = u.astype(BF16)
        kv[me, 1, h] = proj[:, (2 * heads + h) * HD : (2 * heads + h + 1) * HD].astype(BF16)
        do[h] = grad[:, h * HD : (h + 1) * HD]
        wsum[h] = jnp.zeros_like(wsum[h])
        tsum[h] = jnp.zeros_like(tsum[h])
        dq[h] = jnp.zeros_like(dq[h])

    pl.semaphore_wait(barrier, 2)

    def gather(way, step, j):
        b = lax.rem(me + (NZ - step if way == 0 else step), NZ)
        return pltpu.make_async_remote_copy(
            src_ref=kv.at[b, j],
            dst_ref=kv.at[b, j],
            send_sem=send_ag.at[way, step, j],
            recv_sem=recv_ag.at[way, step, j],
            device_id={"seq": sides[way]},
            device_id_type=MESH,
        )

    def scatter(way, step, j):
        return pltpu.make_async_remote_copy(
            src_ref=sbuf.at[way, step, j],
            dst_ref=rbuf.at[way, step, j],
            send_sem=send_rs.at[way, step, j],
            recv_sem=recv_rs.at[way, step, j],
            device_id={"seq": sides[way]},
            device_id_type=MESH,
        )

    def goes(way, step, j):
        return step < 3 or j == way

    def forward(b, h):
        k = kv[b, 0, h]
        v = kv[b, 1, h]
        s = lax.dot_general(q_low[h], k, (((1,), (1,)), ((), ())), preferred_element_type=F32)
        e = jnp.exp(s * scale)
        ex[b, h] = e
        tsum[h] = tsum[h] + (e[:, :HD] + e[:, HD:])
        wsum[h] = wsum[h] + jnp.dot(e.astype(BF16), v, preferred_element_type=F32)
        dp[b, h] = lax.dot_general(
            do[h], v, (((1,), (1,)), ((), ())), preferred_element_type=F32
        )

    def forward_blocks(ahead, behind):
        def step(i, c):
            way = i // heads
            b = lax.rem(me + ahead + way * (behind - ahead), NZ)
            forward(b, lax.rem(i, heads))
            return c

        n = heads if ahead == behind else 2 * heads
        lax.fori_loop(0, n, step, 0)

    for j in range(2):
        for way in range(2):
            gather(way, 0, j).start()
    forward_blocks(0, 0)
    for step in range(3):
        for j in range(2):
            for way in range(2):
                gather(way, step, j).wait_recv()
                if goes(way, step + 1, j):
                    gather(way, step + 1, j).start()
        forward_blocks(NZ - 1 - step, 1 + step)
    gather(0, 3, 0).wait_recv()
    gather(1, 3, 1).wait_recv()
    forward_blocks(4, 4)

    for h in range(heads):
        total = jnp.broadcast_to(jnp.sum(tsum[h], axis=1, keepdims=True), tsum[h].shape)
        low = (wsum[h] / total).astype(BF16)
        att_out[:, h * HD : (h + 1) * HD] = low
        rtot[h] = 1.0 / total
        g = do[h].astype(F32) * low.astype(F32)
        delta[h] = jnp.broadcast_to(jnp.sum(g, axis=1, keepdims=True), g.shape)

    def backward(b, h, slot):
        p = ex[b, h] * twice(rtot[h])
        ds = (p * (dp[b, h] - twice(delta[h])) * scale).astype(BF16)
        dq[h] = dq[h] + jnp.dot(ds, kv[b, 0, h], preferred_element_type=F32)
        part[slot, 0, h] = lax.dot_general(
            ds, q_low[h], (((0,), (0,)), ((), ())), preferred_element_type=F32
        )
        part[slot, 1, h] = lax.dot_general(
            p.astype(BF16), do[h], (((0,), (0,)), ((), ())), preferred_element_type=F32
        )

    def backward_blocks(ahead, behind):
        def step(i, c):
            way = i // heads
            b = lax.rem(me + ahead + way * (behind - ahead), NZ)
            backward(b, lax.rem(i, heads), way)
            return c

        n = heads if ahead == behind else 2 * heads
        lax.fori_loop(0, n, step, 0)

    for step in range(4):
        ahead, behind = 4 - step, 4 + step
        backward_blocks(ahead, behind)
        for j in range(2):
            for way in range(2):
                if not goes(way, 3 - step, j):
                    continue
                slot = 0 if step == 0 else way
                if step > 0 and goes(way, 4 - step, j):
                    scatter(way, step - 1, j).wait_recv()
                    sbuf[way, step, j] = (
                        part[slot, j] + rbuf[way, step - 1, j].astype(F32)
                    ).astype(BF16)
                else:
                    sbuf[way, step, j] = part[slot, j].astype(BF16)
                scatter(way, step, j).start()
    backward_blocks(0, 0)

    def back(g, j, h):
        u = unit[j, h]
        return (g - lane_mean(g) - u * lane_mean(g * u)) * inv[j, h]

    for h in range(heads):
        qkv_out[:, h * HD : (h + 1) * HD] = back(dq[h], 0, h).astype(BF16)
    for j in range(2):
        for way in range(2):
            scatter(way, 3, j).wait_recv()
        for h in range(heads):
            g = part[0, j, h] + rbuf[0, 3, j, h].astype(F32) + rbuf[1, 3, j, h].astype(F32)
            if j == 0:
                g = back(g, 1, h)
            at = (j + 1) * width + h * HD
            qkv_out[:, at : at + HD] = g.astype(BF16)
    for step in range(4):
        for j in range(2):
            for way in range(2):
                if goes(way, step, j):
                    gather(way, step, j).wait_send()
                if goes(way, 3 - step, j):
                    scatter(way, step, j).wait_send()


def attention(proj, grad):
    rows = proj.shape[0]
    heads = grad.shape[1] // HD
    vmem = pl.BlockSpec(memory_space=pltpu.VMEM)
    one = (heads, rows, HD)
    return pl.pallas_call(
        lambda *refs: attention_kernel(heads, *refs),
        out_shape=(
            jax.ShapeDtypeStruct(proj.shape, BF16),
            jax.ShapeDtypeStruct(grad.shape, BF16),
        ),
        in_specs=[vmem, vmem],
        out_specs=(vmem, vmem),
        scratch_shapes=[
            pltpu.VMEM(one, BF16),
            pltpu.VMEM(one, BF16),
            pltpu.VMEM((2, *one), F32),
            pltpu.VMEM((2, *one), F32),
            pltpu.VMEM((NZ, 2, *one), BF16),
            pltpu.VMEM((NZ, heads, rows, rows), F32),
            pltpu.VMEM((NZ, heads, rows, rows), F32),
            pltpu.VMEM(one, F32),
            pltpu.VMEM(one, F32),
            pltpu.VMEM(one, F32),
            pltpu.VMEM(one, F32),
            pltpu.VMEM(one, F32),
            pltpu.VMEM((2, 2, *one), F32),
            pltpu.VMEM((2, 4, 2, *one), BF16),
            pltpu.VMEM((2, 4, 2, *one), BF16),
            pltpu.SemaphoreType.DMA((2, 4, 2)),
            pltpu.SemaphoreType.DMA((2, 4, 2)),
            pltpu.SemaphoreType.DMA((2, 4, 2)),
            pltpu.SemaphoreType.DMA((2, 4, 2)),
        ],
        compiler_params=pltpu.CompilerParams(
            collective_id=0, has_side_effects=True, vmem_limit_bytes=60 * 1024 * 1024
        ),
    )(proj, grad)


def local(tokens, cotangent, qkv_weight, out_weight):
    row_count = tokens.shape[1]
    feature_count = tokens.shape[2]
    column_count = out_weight.shape[1]
    own_rows = qkv_weight.shape[0]
    grad_rows = cotangent[0]
    normed, inverse = normalize(tokens[0].astype(jnp.float32))
    unit_low = normed.astype(jnp.bfloat16)
    flat_weight = qkv_weight.reshape(own_rows, 3 * column_count)
    piece_qkv, piece_out = sent_together((flat_weight, out_weight), ("seq", "dp"), 0, 1)
    piece_rows = piece_qkv.shape[0]
    left_rows = unit_low
    right_rows = grad_rows
    projected = jnp.dot(left_rows, piece_qkv, preferred_element_type=jnp.float32)
    attended_grad = jnp.dot(right_rows, piece_out, preferred_element_type=jnp.float32)
    full_qkv = piece_qkv
    projected, attended_grad, full_qkv = (projected, attended_grad, full_qkv)
    qkv_low, attended_low = attention(projected, attended_grad.astype(jnp.bfloat16))
    inner_grad = jnp.einsum("rc,dc->rd", qkv_low, full_qkv, preferred_element_type=jnp.float32)
    attended_flat = attended_low.reshape(row_count, column_count)
    share_width = feature_count // lax.axis_size("tensor")
    own_share = summed_on_arrival(inner_grad.astype(jnp.bfloat16), "tensor", 1)
    offset = lax.axis_index("tensor") * share_width
    unit_own = lax.dynamic_slice_in_dim(normed, offset, share_width, 1)
    row_sums = in_one(
        (
            jnp.sum(own_share, axis=1, keepdims=True),
            jnp.sum(own_share * unit_own, axis=1, keepdims=True),
        ),
        "tensor",
    )
    branch = (
        own_share - row_sums[0] / feature_count - unit_own * (row_sums[1] / feature_count)
    ) * inverse
    left_rows = unit_low
    right_rows = grad_rows
    qkv_term = jnp.einsum(
        "rd,rc->dc", left_rows, qkv_low, preferred_element_type=jnp.float32
    ).reshape(lax.axis_size(("seq", "dp")) * own_rows, 3, column_count)
    out_term = jnp.einsum(
        "rd,rc->dc", right_rows, attended_flat, preferred_element_type=jnp.float32
    )
    summed = lax.psum_scatter(
        jnp.concatenate([qkv_term, out_term[:, None, :]], axis=1).astype(jnp.bfloat16),
        ("seq", "dp"),
        scatter_dimension=0,
        tiled=True,
    ).astype(jnp.float32)
    return (summed[:, :3], summed[:, 3], branch.astype(jnp.bfloat16)[None])


def solution(mesh):
    return jax.shard_map(
        local,
        mesh=mesh,
        in_specs=(
            P("dp", "seq", None),
            P("dp", "seq", None),
            P(("seq", "dp"), None, "tensor"),
            P(("seq", "dp"), "tensor"),
        ),
        out_specs=(
            P(("seq", "dp"), None, "tensor"),
            P(("seq", "dp"), "tensor"),
            P("dp", "seq", "tensor"),
        ),
        check_vma=False,
    )
```

```python
import jax
import jax.numpy as jnp
from jax import lax
from jax.experimental import pallas as pl
from jax.experimental.pallas import tpu as pltpu
from jax.sharding import PartitionSpec as P

HD = 128
NZ = 8
NT = 8
NQ = 4
MESH = pl.DeviceIdType.MESH
F32 = jnp.float32
BF16 = jnp.bfloat16
LAST = (((1,), (1,)), ((), ()))
FIRST = (((0,), (0,)), ((), ()))
epsilon = 1e-06


def dot(a, b, dims=(((1,), (0,)), ((), ()))):
    return lax.dot_general(a, b, dims, preferred_element_type=F32)


def twice(a):
    return jnp.concatenate([a, a], axis=1)


def lane_mean(a):
    return jnp.broadcast_to(jnp.mean(a, axis=1, keepdims=True), a.shape)


def lane_sum(a):
    return jnp.broadcast_to(jnp.sum(a, axis=1, keepdims=True), a.shape)


def layer_kernel(
    heads,
    proj,
    grad,
    inverse,
    normed,
    weight,
    unit_t,
    cot_t,
    dw_out,
    branch_out,
    q_low,
    do,
    unit,
    inv,
    kv,
    ex,
    dp,
    wsum,
    tsum,
    rtot,
    delta,
    dq,
    sbuf,
    rbuf,
    act,
    low,
    ut,
    ct,
    w,
    nb,
    own_unit,
    sdw,
    rdw,
    dwp,
    xs,
    xr,
    ysend,
    yrecv,
    stats,
    send_ag,
    recv_ag,
    send_rs,
    recv_rs,
    send_tr,
    recv_tr,
    send_act,
    recv_act,
    send_dw,
    recv_dw,
    send_x,
    recv_x,
    send_y,
    recv_y,
    send_st,
    recv_st,
    load_w,
    load_n,
    load_t,
):
    me = lax.axis_index("seq")
    quad = lax.axis_index("dp")
    part = lax.axis_index("tensor")
    sides = (lax.rem(me + 1, NZ), lax.rem(me + NZ - 1, NZ))
    mates = (quad + 1 - 2 * lax.rem(quad, 2), lax.rem(quad + 2, NQ), NQ - 1 - quad)
    xsides = (lax.rem(part + 2, NT), lax.rem(part + NT - 2, NT))
    ymate = part + 1 - 2 * lax.rem(part, 2)
    yhalf = lax.rem(part, 2)
    xplace = part // 2
    scale = HD ** (-0.5)
    width = heads * HD
    features = NT * width

    barrier = pltpu.get_barrier_semaphore()
    for side in sides:
        pl.semaphore_signal(barrier, inc=1, device_id={"seq": side}, device_id_type=MESH)
    for mate in mates:
        pl.semaphore_signal(barrier, inc=1, device_id={"dp": mate}, device_id_type=MESH)
    for k in range(1, NT):
        pl.semaphore_signal(
            barrier, inc=1, device_id={"tensor": lax.rem(part + k, NT)}, device_id_type=MESH
        )

    def remote(src, dst, send, recv, where):
        return pltpu.make_async_remote_copy(
            src_ref=src,
            dst_ref=dst,
            send_sem=send,
            recv_sem=recv,
            device_id=where,
            device_id_type=MESH,
        )

    def gather(way, step, j):
        b = lax.rem(me + (NZ - step if way == 0 else step), NZ)
        return remote(
            kv.at[b, j],
            kv.at[b, j],
            send_ag.at[way, step, j],
            recv_ag.at[way, step, j],
            {"seq": sides[way]},
        )

    def scatter(way, step, j):
        return remote(
            sbuf.at[way, step, j],
            rbuf.at[way, step, j],
            send_rs.at[way, step, j],
            recv_rs.at[way, step, j],
            {"seq": sides[way]},
        )

    def weight_ring(way, step, half):
        return remote(
            sdw.at[way, step, half],
            rdw.at[way, step, half],
            send_dw.at[way, step, half],
            recv_dw.at[way, step, half],
            {"seq": sides[way]},
        )

    def transposed(k, which):
        src, dst = ((unit_t, ut), (cot_t, ct))[which]
        return remote(
            src.at[:, mates[k]],
            dst.at[quad],
            send_tr.at[k, which],
            recv_tr.at[k, which],
            {"dp": mates[k]},
        )

    def shared(group, k):
        block = act.at[group, quad if k < 2 else mates[1]]
        return remote(
            block,
            block,
            send_act.at[group, k],
            recv_act.at[group, k],
            {"dp": mates[1] if k == 1 else mates[0]},
        )

    def xring(way, step, half):
        return remote(
            xs.at[way, step, half],
            xr.at[way, step, half],
            send_x.at[way, step, half],
            recv_x.at[way, step, half],
            {"tensor": xsides[way]},
        )

    def ypair():
        return remote(ysend, yrecv, send_y, recv_y, {"tensor": ymate})

    def stat(k):
        return remote(
            stats.at[0],
            stats.at[k],
            send_st.at[k - 1],
            recv_st.at[k - 1],
            {"tensor": lax.rem(part + k, NT)},
        )

    def goes(way, step, j):
        return step < 3 or j == way

    load_weight = pltpu.make_async_copy(weight, w, load_w)
    load_weight.start()
    load_normed = [
        pltpu.make_async_copy(
            normed.at[:, t * width : (t + 1) * width], nb.at[t], load_n.at[t]
        )
        for t in range(NT)
    ]
    load_own = [
        pltpu.make_async_copy(unit_t.at[:, quad], ut.at[quad], load_t.at[0]),
        pltpu.make_async_copy(cot_t.at[:, quad], ct.at[quad], load_t.at[1]),
    ]
    for c in load_normed + load_own:
        c.start()

    for h in range(heads):
        for j in range(2):
            a = proj[:, (j * heads + h) * HD : (j * heads + h + 1) * HD]
            c = a - lane_mean(a)
            r = lax.rsqrt(lane_mean(c * c) + epsilon)
            u = c * r
            unit[j, h] = u
            inv[j, h] = r
            if j == 0:
                q_low[h] = u.astype(BF16)
            else:
                kv[me, 0, h] = u.astype(BF16)
        kv[me, 1, h] = proj[:, (2 * heads + h) * HD : (2 * heads + h + 1) * HD].astype(BF16)
        do[h] = grad[:, h * HD : (h + 1) * HD]
        wsum[h] = jnp.zeros_like(wsum[h])
        tsum[h] = jnp.zeros_like(tsum[h])
        dq[h] = jnp.zeros_like(dq[h])

    pl.semaphore_wait(barrier, 2 + 3 + NT - 1)

    def forward(b, h):
        k = kv[b, 0, h]
        v = kv[b, 1, h]
        e = jnp.exp(dot(q_low[h], k, LAST) * scale)
        ex[b, h] = e
        tsum[h] = tsum[h] + (e[:, :HD] + e[:, HD:])
        wsum[h] = wsum[h] + dot(e.astype(BF16), v)
        dp[b, h] = dot(do[h], v, LAST)

    def forward_blocks(ahead, behind):
        def step(i, c):
            b = lax.rem(me + ahead + (i // heads) * (behind - ahead), NZ)
            forward(b, lax.rem(i, heads))
            return c

        lax.fori_loop(0, heads if ahead == behind else 2 * heads, step, 0)

    for j in range(2):
        for way in range(2):
            gather(way, 0, j).start()
    for which in range(2):
        for k in range(3):
            transposed(k, which).start()
    forward_blocks(0, 0)
    for step in range(3):
        for j in range(2):
            for way in range(2):
                gather(way, step, j).wait_recv()
                if goes(way, step + 1, j):
                    gather(way, step + 1, j).start()
        forward_blocks(NZ - 1 - step, 1 + step)
    gather(0, 3, 0).wait_recv()
    gather(1, 3, 1).wait_recv()
    forward_blocks(4, 4)

    for h in range(heads):
        total = lane_sum(tsum[h])
        a = (wsum[h] / total).astype(BF16)
        act[0, quad, :, h * HD : (h + 1) * HD] = a
        rtot[h] = 1.0 / total
        delta[h] = lane_sum(do[h].astype(F32) * a.astype(F32))
    shared(0, 1).start()
    shared(0, 0).start()

    def backward(b, h):
        p = ex[b, h] * twice(rtot[h])
        ds = (p * (dp[b, h] - twice(delta[h])) * scale).astype(BF16)
        dq[h] = dq[h] + dot(ds, kv[b, 0, h])
        ex[b, h, :, :HD] = dot(ds, q_low[h], FIRST)
        ex[b, h, :, HD:] = dot(p.astype(BF16), do[h], FIRST)

    def backward_blocks(first, count):
        def step(i, c):
            n = first + i // heads
            away = (n + 1) // 2
            b = lax.rem(me + 4 + lax.rem(n, 2) * (NZ - 2 * away) + away, NZ)
            backward(b, lax.rem(i, heads))
            return c

        lax.fori_loop(0, count * heads, step, 0)

    def scatter_step(step):
        for j in range(2):
            for way in range(2):
                if not goes(way, 3 - step, j):
                    continue
                b = lax.rem(me + (4 - step if way == 0 else 4 + step), NZ)
                added = step > 0 and goes(way, 4 - step, j)
                if added:
                    scatter(way, step - 1, j).wait_recv()
                for h in range(heads):
                    g = ex[b, h, :, j * HD : (j + 1) * HD]
                    if added:
                        g = g + rbuf[way, step - 1, j, h].astype(F32)
                    sbuf[way, step, j, h] = g.astype(BF16)
                scatter(way, step, j).start()

    def relay(group):
        shared(group, 1).wait_recv()
        shared(group, 2).start()

    def back(g, j, h):
        u = unit[j, h]
        return (g - lane_mean(g) - u * lane_mean(g * u)) * inv[j, h]

    backward_blocks(0, 1)
    scatter_step(0)
    backward_blocks(1, 7)
    for h in range(heads):
        a = back(dq[h], 0, h).astype(BF16)
        act[1, quad, :, h * HD : (h + 1) * HD] = a
        low[:, h * HD : (h + 1) * HD] = a
    shared(1, 1).start()
    shared(1, 0).start()
    scatter_step(1)
    relay(0)
    scatter_step(2)
    relay(1)
    scatter_step(3)

    for c in load_own:
        c.wait()
    for which in range(2):
        for k in range(3):
            transposed(k, which).wait_recv()
    for group in range(2):
        shared(group, 0).wait_recv()
        shared(group, 2).wait_recv()

    def weight_block(z, half):
        for i in range(2):
            group = 2 * half + i
            left = ct if group == 0 else ut
            acc = dot(left[0, z], act[group, 0])
            for m in range(1, NQ):
                acc = acc + dot(left[m, z], act[group, m])
            dwp[z, half, :, i * width : (i + 1) * width] = acc

    def weight_blocks(half):
        def step(i, c):
            weight_block(lax.rem(me + 5 + i, NZ), half)
            return c

        lax.fori_loop(0, NZ - 1, step, 0)

    def weight_step(step, half):
        for way in range(2):
            if not goes(way, 3 - step, half):
                continue
            z = lax.rem(me + (4 - step if way == 0 else 4 + step), NZ)
            g = dwp[z, half]
            if step > 0 and goes(way, 4 - step, half):
                weight_ring(way, step - 1, half).wait_recv()
                g = g + rdw[way, step - 1, half].astype(F32)
            sdw[way, step, half] = g.astype(BF16)
            weight_ring(way, step, half).start()

    weight_block(lax.rem(me + 4, NZ), 0)
    weight_step(0, 0)
    weight_blocks(0)

    for j in range(2):
        for way in range(2):
            scatter(way, 3, j).wait_recv()
        for h in range(heads):
            g = ex[me, h, :, j * HD : (j + 1) * HD]
            g = g + rbuf[0, 3, j, h].astype(F32) + rbuf[1, 3, j, h].astype(F32)
            if j == 0:
                g = back(g, 1, h)
            a = g.astype(BF16)
            act[2 + j, quad, :, h * HD : (h + 1) * HD] = a
            low[:, (j + 1) * width + h * HD : (j + 1) * width + (h + 1) * HD] = a
        shared(2 + j, 1).start()
        shared(2 + j, 0).start()
        weight_step(1 + j, 0)

    load_weight.wait()
    for c in load_normed:
        c.wait()
    own_unit[...] = nb[part]

    def inner(i, sums):
        x = lax.rem(xplace + 2 + i // 2, 4)
        t = 2 * x + lax.rem(i, 2)
        g = dot(low[...], w[pl.ds(pl.multiple_of(t * width, width), width), :], LAST)
        both = g * nb[t]
        nb[t] = g
        one, two = sums
        for k in range(heads):
            one = one + g[:, k * HD : (k + 1) * HD]
            two = two + both[:, k * HD : (k + 1) * HD]
        return one, two

    def inner_step(step):
        for half in range(2):
            for way in range(2):
                if step == 0 and half != way:
                    continue
                x = lax.rem(xplace + (2 - step if way == 0 else 2 + step), 4)
                g = nb[2 * x + half]
                if step > 0 and half == way:
                    xring(way, 0, half).wait_recv()
                    g = g + xr[way, 0, half].astype(F32)
                xs[way, step, half] = g.astype(BF16)
                xring(way, step, half).start()

    zero = jnp.zeros((low.shape[0], HD), F32)
    sums = lax.fori_loop(0, 2, inner, (zero, zero))
    inner_step(0)
    sums = lax.fori_loop(2, NT, inner, sums)
    relay(2)
    for i in range(2):
        stats[0, i * 8 : (i + 1) * 8, :] = jnp.transpose(lane_sum(sums[i]))[:8]
    for k in range(1, NT):
        stat(k).start()
    inner_step(1)
    relay(3)
    weight_step(3, 0)

    for group in range(2, 4):
        shared(group, 0).wait_recv()
        shared(group, 2).wait_recv()
    weight_block(lax.rem(me + 4, NZ), 1)
    weight_step(0, 1)
    weight_blocks(1)
    weight_step(1, 1)

    def arrived(half):
        g = nb[2 * xplace + half]
        return g + xr[0, 1, half].astype(F32) + xr[1, 1, half].astype(F32)

    for way in range(2):
        for half in range(2):
            xring(way, 1, half).wait_recv()
    ysend[...] = arrived(1 - yhalf).astype(BF16)
    ypair().start()
    weight_step(2, 1)
    for k in range(1, NT):
        stat(k).wait_recv()
    weight_step(3, 1)

    total = stats[0]
    for k in range(1, NT):
        total = total + stats[k]
    row_mean = []
    for i in range(2):
        row = jnp.broadcast_to(total[i * 8 : i * 8 + 1, :], (HD, total.shape[1]))
        row_mean.append(jnp.transpose(row) / features)
    ypair().wait_recv()
    share = arrived(yhalf) + yrecv[...].astype(F32)
    for k in range(heads):
        at = slice(k * HD, (k + 1) * HD)
        g = share[:, at] - row_mean[0] - own_unit[:, at] * row_mean[1]
        branch_out[:, at] = (g * inverse[...]).astype(BF16)

    for half in range(2):
        g = dwp[me, half]
        for way in range(2):
            weight_ring(way, 3, half).wait_recv()
            g = g + rdw[way, 3, half].astype(F32)
        dw_out[half] = g

    for step in range(4):
        for j in range(2):
            for way in range(2):
                if goes(way, step, j):
                    gather(way, step, j).wait_send()
                if goes(way, 3 - step, j):
                    scatter(way, step, j).wait_send()
                    weight_ring(way, step, j).wait_send()
    for which in range(2):
        for k in range(3):
            transposed(k, which).wait_send()
    for group in range(4):
        for k in range(3):
            shared(group, k).wait_send()
    for way in range(2):
        xring(way, 0, way).wait_send()
        for half in range(2):
            xring(way, 1, half).wait_send()
    ypair().wait_send()
    for k in range(1, NT):
        stat(k).wait_send()


def layer(proj, grad, inverse, normed, weight, unit_t, cot_t):
    rows, width = grad.shape
    heads = width // HD
    vmem = pl.BlockSpec(memory_space=pltpu.VMEM)
    hbm = pl.BlockSpec(memory_space=pl.ANY)
    one = (heads, rows, HD)
    own = unit_t.shape[2]
    dma = pltpu.SemaphoreType.DMA
    return pl.pallas_call(
        lambda *refs: layer_kernel(heads, *refs),
        out_shape=(
            jax.ShapeDtypeStruct((2, own, 2 * width), F32),
            jax.ShapeDtypeStruct((rows, width), BF16),
        ),
        in_specs=[vmem, vmem, vmem, hbm, hbm, hbm, hbm],
        out_specs=(vmem, vmem),
        scratch_shapes=[
            pltpu.VMEM(one, BF16),
            pltpu.VMEM(one, BF16),
            pltpu.VMEM((2, *one), F32),
            pltpu.VMEM((2, *one), F32),
            pltpu.VMEM((NZ, 2, *one), BF16),
            pltpu.VMEM((NZ, heads, rows, rows), F32),
            pltpu.VMEM((NZ, heads, rows, rows), F32),
            pltpu.VMEM(one, F32),
            pltpu.VMEM(one, F32),
            pltpu.VMEM(one, F32),
            pltpu.VMEM(one, F32),
            pltpu.VMEM(one, F32),
            pltpu.VMEM((2, 4, 2, *one), BF16),
            pltpu.VMEM((2, 4, 2, *one), BF16),
            pltpu.VMEM((4, NQ, rows, width), BF16),
            pltpu.VMEM((rows, 3 * width), BF16),
            pltpu.VMEM((NQ, NZ, own, rows), BF16),
            pltpu.VMEM((NQ, NZ, own, rows), BF16),
            pltpu.VMEM(weight.shape, BF16),
            pltpu.VMEM((NT, rows, width), F32),
            pltpu.VMEM((rows, width), F32),
            pltpu.VMEM((2, 4, 2, own, 2 * width), BF16),
            pltpu.VMEM((2, 4, 2, own, 2 * width), BF16),
            pltpu.VMEM((NZ, 2, own, 2 * width), F32),
            pltpu.VMEM((2, 2, 2, rows, width), BF16),
            pltpu.VMEM((2, 2, 2, rows, width), BF16),
            pltpu.VMEM((rows, width), BF16),
            pltpu.VMEM((rows, width), BF16),
            pltpu.VMEM((NT, 16, rows), F32),
            dma((2, 4, 2)),
            dma((2, 4, 2)),
            dma((2, 4, 2)),
            dma((2, 4, 2)),
            dma((3, 2)),
            dma((3, 2)),
            dma((4, 3)),
            dma((4, 3)),
            dma((2, 4, 2)),
            dma((2, 4, 2)),
            dma((2, 2, 2)),
            dma((2, 2, 2)),
            dma,
            dma,
            dma((NT - 1,)),
            dma((NT - 1,)),
            dma,
            dma((NT,)),
            dma((2,)),
        ],
        compiler_params=pltpu.CompilerParams(
            collective_id=0, has_side_effects=True, vmem_limit_bytes=62 * 1024 * 1024
        ),
    )(proj, grad, inverse, normed, weight, unit_t, cot_t)


def normalize(values):
    average = jnp.mean(values, axis=-1, keepdims=True)
    centered = values - average
    inverse = lax.rsqrt(jnp.mean(centered * centered, axis=-1, keepdims=True) + epsilon)
    return (centered * inverse, inverse)


def local(tokens, cotangent, qkv_weight, out_weight):
    rows = tokens.shape[1]
    width = out_weight.shape[1]
    own = qkv_weight.shape[0]
    grad_rows = cotangent[0]
    normed, inverse = normalize(tokens[0].astype(F32))
    unit_low = normed.astype(BF16)
    both = jnp.concatenate([qkv_weight.reshape(own, 3 * width), out_weight], axis=1)
    weights = lax.all_gather(both, ("seq", "dp"), axis=0, tiled=True)
    full_qkv, full_out = weights[:, : 3 * width], weights[:, 3 * width :]
    proj = dot(unit_low, full_qkv)
    grad = dot(grad_rows, full_out).astype(BF16)
    inverse = jnp.broadcast_to(inverse, (rows, HD))
    unit_t = unit_low.T.reshape(NZ, NQ, own, rows)
    cot_t = grad_rows.T.reshape(NZ, NQ, own, rows)
    dw, branch = layer(proj, grad, inverse, normed, full_qkv, unit_t, cot_t)
    out_grad = dw[0, :, :width]
    qkv_grad = jnp.stack([dw[0, :, width:], dw[1, :, :width], dw[1, :, width:]], axis=1)
    return (qkv_grad, out_grad, branch[None])


def solution(mesh):
    return jax.shard_map(
        local,
        mesh=mesh,
        in_specs=(
            P("dp", "seq", None),
            P("dp", "seq", None),
            P(("seq", "dp"), None, "tensor"),
            P(("seq", "dp"), "tensor"),
        ),
        out_specs=(
            P(("seq", "dp"), None, "tensor"),
            P(("seq", "dp"), "tensor"),
            P("dp", "seq", "tensor"),
        ),
        check_vma=False,
    )
```

```python
import jax
import jax.numpy as jnp
from jax import lax
from jax.experimental import pallas as pl
from jax.experimental.pallas import tpu as pltpu
from jax.sharding import PartitionSpec as P

HD = 128
NZ = 8
NT = 8
NQ = 4
MESH = pl.DeviceIdType.MESH
F32 = jnp.float32
BF16 = jnp.bfloat16
LAST = (((1,), (1,)), ((), ()))
FIRST = (((0,), (0,)), ((), ()))
epsilon = 1e-06


def dot(a, b, dims=(((1,), (0,)), ((), ()))):
    return lax.dot_general(a, b, dims, preferred_element_type=F32)


def twice(a):
    return jnp.concatenate([a, a], axis=1)


def lane_mean(a):
    return jnp.broadcast_to(jnp.mean(a, axis=1, keepdims=True), a.shape)


def lane_sum(a):
    return jnp.broadcast_to(jnp.sum(a, axis=1, keepdims=True), a.shape)


def layer_kernel(
    heads,
    proj,
    grad,
    norm,
    tokens,
    weight,
    unit_t,
    cot_t,
    dw_out,
    branch_out,
    q_low,
    do,
    unit,
    inv,
    kv,
    ex,
    dp,
    wsum,
    tsum,
    rtot,
    delta,
    dq,
    sbuf,
    rbuf,
    act,
    low,
    ut,
    ct,
    w,
    tb,
    nb,
    sdw,
    rdw,
    dwp,
    xs,
    xr,
    ysend,
    yrecv,
    stats,
    send_ag,
    recv_ag,
    send_rs,
    recv_rs,
    send_tr,
    recv_tr,
    send_act,
    recv_act,
    send_dw,
    recv_dw,
    send_x,
    recv_x,
    send_y,
    recv_y,
    send_st,
    recv_st,
    load_w,
    load_n,
    load_t,
):
    me = lax.axis_index("seq")
    quad = lax.axis_index("dp")
    part = lax.axis_index("tensor")
    sides = (lax.rem(me + 1, NZ), lax.rem(me + NZ - 1, NZ))
    mates = (quad + 1 - 2 * lax.rem(quad, 2), lax.rem(quad + 2, NQ), NQ - 1 - quad)
    xsides = (lax.rem(part + 2, NT), lax.rem(part + NT - 2, NT))
    ymate = part + 1 - 2 * lax.rem(part, 2)
    yhalf = lax.rem(part, 2)
    xplace = part // 2
    scale = HD ** (-0.5)
    width = heads * HD
    features = NT * width

    barrier = pltpu.get_barrier_semaphore()
    for side in sides:
        pl.semaphore_signal(barrier, inc=1, device_id={"seq": side}, device_id_type=MESH)
    for mate in mates:
        pl.semaphore_signal(barrier, inc=1, device_id={"dp": mate}, device_id_type=MESH)
    for k in range(1, NT):
        pl.semaphore_signal(
            barrier, inc=1, device_id={"tensor": lax.rem(part + k, NT)}, device_id_type=MESH
        )

    def remote(src, dst, send, recv, where):
        return pltpu.make_async_remote_copy(
            src_ref=src,
            dst_ref=dst,
            send_sem=send,
            recv_sem=recv,
            device_id=where,
            device_id_type=MESH,
        )

    def gather(way, step, j):
        b = lax.rem(me + (NZ - step if way == 0 else step), NZ)
        return remote(
            kv.at[b, j],
            kv.at[b, j],
            send_ag.at[way, step, j],
            recv_ag.at[way, step, j],
            {"seq": sides[way]},
        )

    def scatter(way, step, j):
        return remote(
            sbuf.at[way, step, j],
            rbuf.at[way, step, j],
            send_rs.at[way, step, j],
            recv_rs.at[way, step, j],
            {"seq": sides[way]},
        )

    def weight_ring(way, step, half):
        return remote(
            sdw.at[way, step, half],
            rdw.at[way, step, half],
            send_dw.at[way, step, half],
            recv_dw.at[way, step, half],
            {"seq": sides[way]},
        )

    def transposed(k, which):
        src, dst = ((unit_t, ut), (cot_t, ct))[which]
        return remote(
            src.at[:, mates[k]],
            dst.at[quad],
            send_tr.at[k, which],
            recv_tr.at[k, which],
            {"dp": mates[k]},
        )

    def shared(group, k):
        block = act.at[group, quad if k < 2 else mates[1]]
        return remote(
            block,
            block,
            send_act.at[group, k],
            recv_act.at[group, k],
            {"dp": mates[1] if k == 1 else mates[0]},
        )

    def xring(way, step, half):
        return remote(
            xs.at[way, step, half],
            xr.at[way, step, half],
            send_x.at[way, step, half],
            recv_x.at[way, step, half],
            {"tensor": xsides[way]},
        )

    def ypair():
        return remote(ysend, yrecv, send_y, recv_y, {"tensor": ymate})

    def stat(k):
        return remote(
            stats.at[0],
            stats.at[k],
            send_st.at[k - 1],
            recv_st.at[k - 1],
            {"tensor": lax.rem(part + k, NT)},
        )

    def goes(way, step, j):
        return step < 3 or j == way

    load_weight = [
        pltpu.make_async_copy(weight.at[j // 2, :, j % 2], w.at[j], load_w.at[j])
        for j in range(3)
    ]
    load_tokens = [
        pltpu.make_async_copy(
            tokens.at[:, t * width : (t + 1) * width], tb.at[t], load_n.at[t]
        )
        for t in range(NT)
    ]
    load_own = [
        pltpu.make_async_copy(unit_t.at[:, quad], ut.at[quad], load_t.at[0]),
        pltpu.make_async_copy(cot_t.at[:, quad], ct.at[quad], load_t.at[1]),
    ]
    for c in load_weight + load_tokens + load_own:
        c.start()

    for h in range(heads):
        for j in range(2):
            a = proj[:, (j * heads + h) * HD : (j * heads + h + 1) * HD]
            c = a - lane_mean(a)
            r = lax.rsqrt(lane_mean(c * c) + epsilon)
            u = c * r
            unit[j, h] = u
            inv[j, h] = r
            if j == 0:
                q_low[h] = u.astype(BF16)
            else:
                kv[me, 0, h] = u.astype(BF16)
        kv[me, 1, h] = proj[:, (2 * heads + h) * HD : (2 * heads + h + 1) * HD].astype(BF16)
        do[h] = grad[:, h * HD : (h + 1) * HD]
        wsum[h] = jnp.zeros_like(wsum[h])
        tsum[h] = jnp.zeros_like(tsum[h])
        dq[h] = jnp.zeros_like(dq[h])

    pl.semaphore_wait(barrier, 2 + 3 + NT - 1)

    def forward(b, h):
        k = kv[b, 0, h]
        v = kv[b, 1, h]
        e = jnp.exp(dot(q_low[h], k, LAST) * scale)
        ex[b, h] = e
        tsum[h] = tsum[h] + (e[:, :HD] + e[:, HD:])
        wsum[h] = wsum[h] + dot(e.astype(BF16), v)
        dp[b, h] = dot(do[h], v, LAST)

    def forward_blocks(ahead, behind):
        def step(i, c):
            b = lax.rem(me + ahead + (i // heads) * (behind - ahead), NZ)
            forward(b, lax.rem(i, heads))
            return c

        lax.fori_loop(0, heads if ahead == behind else 2 * heads, step, 0)

    for j in range(2):
        for way in range(2):
            gather(way, 0, j).start()
    for which in range(2):
        for k in range(3):
            transposed(k, which).start()
    forward_blocks(0, 0)
    for step in range(3):
        for j in range(2):
            for way in range(2):
                gather(way, step, j).wait_recv()
                if goes(way, step + 1, j):
                    gather(way, step + 1, j).start()
        forward_blocks(NZ - 1 - step, 1 + step)
    gather(0, 3, 0).wait_recv()
    gather(1, 3, 1).wait_recv()
    forward_blocks(4, 4)

    for h in range(heads):
        total = lane_sum(tsum[h])
        a = (wsum[h] / total).astype(BF16)
        act[0, quad, :, h * HD : (h + 1) * HD] = a
        rtot[h] = 1.0 / total
        delta[h] = lane_sum(do[h].astype(F32) * a.astype(F32))
    shared(0, 1).start()
    shared(0, 0).start()

    def backward(b, h):
        p = ex[b, h] * twice(rtot[h])
        ds = (p * (dp[b, h] - twice(delta[h])) * scale).astype(BF16)
        dq[h] = dq[h] + dot(ds, kv[b, 0, h])
        ex[b, h, :, :HD] = dot(ds, q_low[h], FIRST)
        ex[b, h, :, HD:] = dot(p.astype(BF16), do[h], FIRST)

    def backward_blocks(first, count):
        def step(i, c):
            n = first + i // heads
            away = (n + 1) // 2
            b = lax.rem(me + 4 + lax.rem(n, 2) * (NZ - 2 * away) + away, NZ)
            backward(b, lax.rem(i, heads))
            return c

        lax.fori_loop(0, count * heads, step, 0)

    def scatter_step(step):
        for j in range(2):
            for way in range(2):
                if not goes(way, 3 - step, j):
                    continue
                b = lax.rem(me + (4 - step if way == 0 else 4 + step), NZ)
                added = step > 0 and goes(way, 4 - step, j)
                if added:
                    scatter(way, step - 1, j).wait_recv()
                for h in range(heads):
                    g = ex[b, h, :, j * HD : (j + 1) * HD]
                    if added:
                        g = g + rbuf[way, step - 1, j, h].astype(F32)
                    sbuf[way, step, j, h] = g.astype(BF16)
                scatter(way, step, j).start()

    def relay(group):
        shared(group, 1).wait_recv()
        shared(group, 2).start()

    def back(g, j, h):
        u = unit[j, h]
        return (g - lane_mean(g) - u * lane_mean(g * u)) * inv[j, h]

    backward_blocks(0, 1)
    scatter_step(0)
    backward_blocks(1, 7)
    for h in range(heads):
        a = back(dq[h], 0, h).astype(BF16)
        act[1, quad, :, h * HD : (h + 1) * HD] = a
        low[:, h * HD : (h + 1) * HD] = a
    shared(1, 1).start()
    shared(1, 0).start()
    scatter_step(1)
    relay(0)
    scatter_step(2)
    relay(1)
    scatter_step(3)

    for c in load_own:
        c.wait()
    for which in range(2):
        for k in range(3):
            transposed(k, which).wait_recv()
    for group in range(2):
        shared(group, 0).wait_recv()
        shared(group, 2).wait_recv()

    def weight_block(z, half):
        for i in range(2):
            group = 2 * half + i
            left = ct if group == 0 else ut
            acc = dot(left[0, z], act[group, 0])
            for m in range(1, NQ):
                acc = acc + dot(left[m, z], act[group, m])
            dwp[z, half, :, i * width : (i + 1) * width] = acc

    def weight_blocks(half):
        def step(i, c):
            weight_block(lax.rem(me + 5 + i, NZ), half)
            return c

        lax.fori_loop(0, NZ - 1, step, 0)

    def weight_step(step, half):
        for way in range(2):
            if not goes(way, 3 - step, half):
                continue
            z = lax.rem(me + (4 - step if way == 0 else 4 + step), NZ)
            g = dwp[z, half]
            if step > 0 and goes(way, 4 - step, half):
                weight_ring(way, step - 1, half).wait_recv()
                g = g + rdw[way, step - 1, half].astype(F32)
            sdw[way, step, half] = g.astype(BF16)
            weight_ring(way, step, half).start()

    weight_block(lax.rem(me + 4, NZ), 0)
    weight_step(0, 0)
    weight_blocks(0)

    for j in range(2):
        for way in range(2):
            scatter(way, 3, j).wait_recv()
        for h in range(heads):
            g = ex[me, h, :, j * HD : (j + 1) * HD]
            g = g + rbuf[0, 3, j, h].astype(F32) + rbuf[1, 3, j, h].astype(F32)
            if j == 0:
                g = back(g, 1, h)
            a = g.astype(BF16)
            act[2 + j, quad, :, h * HD : (h + 1) * HD] = a
            low[:, (j + 1) * width + h * HD : (j + 1) * width + (h + 1) * HD] = a
        shared(2 + j, 1).start()
        shared(2 + j, 0).start()
        weight_step(1 + j, 0)

    for c in load_weight + load_tokens:
        c.wait()

    def inner(i, sums):
        x = lax.rem(xplace + 2 + i // 2, 4)
        t = 2 * x + lax.rem(i, 2)
        blocks = pl.ds(pl.multiple_of(t * NQ, NQ), NQ)
        g = dot(low[:, :width], w[0, blocks].reshape(width, width), LAST)
        for j in range(1, 3):
            left = low[:, j * width : (j + 1) * width]
            g = g + dot(left, w[j, blocks].reshape(width, width), LAST)
        nb[t] = g
        one, two = sums
        for k in range(heads):
            at = slice(k * HD, (k + 1) * HD)
            one = one + g[:, at]
            two = two + g[:, at] * ((tb[t, :, at].astype(F32) - norm[0]) * norm[1])
        return one, two

    def inner_step(step):
        for half in range(2):
            for way in range(2):
                if step == 0 and half != way:
                    continue
                x = lax.rem(xplace + (2 - step if way == 0 else 2 + step), 4)
                g = nb[2 * x + half]
                if step > 0 and half == way:
                    xring(way, 0, half).wait_recv()
                    g = g + xr[way, 0, half].astype(F32)
                xs[way, step, half] = g.astype(BF16)
                xring(way, step, half).start()

    zero = jnp.zeros((low.shape[0], HD), F32)
    sums = lax.fori_loop(0, 2, inner, (zero, zero))
    inner_step(0)
    sums = lax.fori_loop(2, NT, inner, sums)
    relay(2)
    for i in range(2):
        stats[0, i * 8 : (i + 1) * 8, :] = jnp.transpose(lane_sum(sums[i]))[:8]
    for k in range(1, NT):
        stat(k).start()
    inner_step(1)
    relay(3)
    weight_step(3, 0)

    for group in range(2, 4):
        shared(group, 0).wait_recv()
        shared(group, 2).wait_recv()
    weight_block(lax.rem(me + 4, NZ), 1)
    weight_step(0, 1)
    weight_blocks(1)
    weight_step(1, 1)

    def arrived(half):
        g = nb[2 * xplace + half]
        return g + xr[0, 1, half].astype(F32) + xr[1, 1, half].astype(F32)

    for way in range(2):
        for half in range(2):
            xring(way, 1, half).wait_recv()
    ysend[...] = arrived(1 - yhalf).astype(BF16)
    ypair().start()
    weight_step(2, 1)
    for k in range(1, NT):
        stat(k).wait_recv()
    weight_step(3, 1)

    total = stats[0]
    for k in range(1, NT):
        total = total + stats[k]
    row_mean = []
    for i in range(2):
        row = jnp.broadcast_to(total[i * 8 : i * 8 + 1, :], (HD, total.shape[1]))
        row_mean.append(jnp.transpose(row) / features)
    ypair().wait_recv()
    share = arrived(yhalf) + yrecv[...].astype(F32)
    for k in range(heads):
        at = slice(k * HD, (k + 1) * HD)
        own_unit = (tb[part, :, at].astype(F32) - norm[0]) * norm[1]
        g = share[:, at] - row_mean[0] - own_unit * row_mean[1]
        branch_out[:, at] = (g * norm[1]).astype(BF16)

    for half in range(2):
        g = dwp[me, half]
        for way in range(2):
            weight_ring(way, 3, half).wait_recv()
            g = g + rdw[way, 3, half].astype(F32)
        dw_out[half] = g

    for step in range(4):
        for j in range(2):
            for way in range(2):
                if goes(way, step, j):
                    gather(way, step, j).wait_send()
                if goes(way, 3 - step, j):
                    scatter(way, step, j).wait_send()
                    weight_ring(way, step, j).wait_send()
    for which in range(2):
        for k in range(3):
            transposed(k, which).wait_send()
    for group in range(4):
        for k in range(3):
            shared(group, k).wait_send()
    for way in range(2):
        xring(way, 0, way).wait_send()
        for half in range(2):
            xring(way, 1, half).wait_send()
    ypair().wait_send()
    for k in range(1, NT):
        stat(k).wait_send()


def layer(proj, grad, norm, tokens, weight, unit_t, cot_t):
    rows, width = grad.shape
    heads = width // HD
    vmem = pl.BlockSpec(memory_space=pltpu.VMEM)
    hbm = pl.BlockSpec(memory_space=pl.ANY)
    one = (heads, rows, HD)
    own = unit_t.shape[2]
    dma = pltpu.SemaphoreType.DMA
    return pl.pallas_call(
        lambda *refs: layer_kernel(heads, *refs),
        out_shape=(
            jax.ShapeDtypeStruct((2, own, 2 * width), F32),
            jax.ShapeDtypeStruct((rows, width), BF16),
        ),
        in_specs=[vmem, vmem, vmem, hbm, hbm, hbm, hbm],
        out_specs=(vmem, vmem),
        scratch_shapes=[
            pltpu.VMEM(one, BF16),
            pltpu.VMEM(one, BF16),
            pltpu.VMEM((2, *one), F32),
            pltpu.VMEM((2, *one), F32),
            pltpu.VMEM((NZ, 2, *one), BF16),
            pltpu.VMEM((NZ, heads, rows, rows), F32),
            pltpu.VMEM((NZ, heads, rows, rows), F32),
            pltpu.VMEM(one, F32),
            pltpu.VMEM(one, F32),
            pltpu.VMEM(one, F32),
            pltpu.VMEM(one, F32),
            pltpu.VMEM(one, F32),
            pltpu.VMEM((2, 4, 2, *one), BF16),
            pltpu.VMEM((2, 4, 2, *one), BF16),
            pltpu.VMEM((4, NQ, rows, width), BF16),
            pltpu.VMEM((rows, 3 * width), BF16),
            pltpu.VMEM((NQ, NZ, own, rows), BF16),
            pltpu.VMEM((NQ, NZ, own, rows), BF16),
            pltpu.VMEM((3, NZ * NQ, own, width), BF16),
            pltpu.VMEM((NT, rows, width), BF16),
            pltpu.VMEM((NT, rows, width), F32),
            pltpu.VMEM((2, 4, 2, own, 2 * width), BF16),
            pltpu.VMEM((2, 4, 2, own, 2 * width), BF16),
            pltpu.VMEM((NZ, 2, own, 2 * width), F32),
            pltpu.VMEM((2, 2, 2, rows, width), BF16),
            pltpu.VMEM((2, 2, 2, rows, width), BF16),
            pltpu.VMEM((rows, width), BF16),
            pltpu.VMEM((rows, width), BF16),
            pltpu.VMEM((NT, 16, rows), F32),
            dma((2, 4, 2)),
            dma((2, 4, 2)),
            dma((2, 4, 2)),
            dma((2, 4, 2)),
            dma((3, 2)),
            dma((3, 2)),
            dma((4, 3)),
            dma((4, 3)),
            dma((2, 4, 2)),
            dma((2, 4, 2)),
            dma((2, 2, 2)),
            dma((2, 2, 2)),
            dma,
            dma,
            dma((NT - 1,)),
            dma((NT - 1,)),
            dma((3,)),
            dma((NT,)),
            dma((2,)),
        ],
        compiler_params=pltpu.CompilerParams(
            collective_id=0, has_side_effects=True, vmem_limit_bytes=62 * 1024 * 1024
        ),
    )(proj, grad, norm, tokens, weight, unit_t, cot_t)


def weights_kernel(
    tokens,
    cot,
    own_qkv,
    own_out,
    proj_out,
    grad_out,
    norm_out,
    ut_out,
    ct_out,
    g_out,
    g,
    tz,
    uz,
    cz,
    acc,
    send_za,
    recv_za,
    send_zb,
    recv_zb,
    send_ya,
    recv_ya,
    send_yb,
    recv_yb,
    send_da,
    recv_da,
    send_db,
    recv_db,
    load_g,
    load_t,
    load_c,
    keep,
):
    me = lax.axis_index("seq")
    quad = lax.axis_index("dp")
    sides = (lax.rem(me + 1, NZ), lax.rem(me + NZ - 1, NZ))
    mates = (quad + 1 - 2 * lax.rem(quad, 2), lax.rem(quad + 2, NQ), NQ - 1 - quad)
    width = own_out.shape[1]
    features = NZ * width

    barrier = pltpu.get_barrier_semaphore()
    for side in sides:
        pl.semaphore_signal(barrier, inc=1, device_id={"seq": side}, device_id_type=MESH)
    for mate in mates[:2]:
        pl.semaphore_signal(barrier, inc=1, device_id={"dp": mate}, device_id_type=MESH)

    mine = me * NQ + quad
    load_own = [
        pltpu.make_async_copy(own_qkv.at[0], g.at[0, mine, 0], load_g.at[0]),
        pltpu.make_async_copy(own_qkv.at[1], g.at[0, mine, 1], load_g.at[1]),
        pltpu.make_async_copy(own_qkv.at[2], g.at[1, mine, 0], load_g.at[2]),
        pltpu.make_async_copy(own_out, g.at[1, mine, 1], load_g.at[3]),
    ]
    load_tok = [
        pltpu.make_async_copy(tokens.at[:, z * width : (z + 1) * width], tz.at[z], load_t.at[z])
        for z in range(NZ)
    ]
    load_cot = [
        pltpu.make_async_copy(cot.at[:, z * width : (z + 1) * width], cz.at[z], load_c.at[z])
        for z in range(NZ)
    ]
    for c in load_own + load_tok + load_cot:
        c.start()

    def remote(block, send, recv, where):
        return pltpu.make_async_remote_copy(
            src_ref=block,
            dst_ref=block,
            send_sem=send,
            recv_sem=recv,
            device_id=where,
            device_id_type=MESH,
        )

    classes = (quad, mates[1])

    def place(i):
        if i == 0:
            return me
        if i >= 7:
            return lax.rem(me + 4, NZ)
        step, way = (i - 1) // 2, (i - 1) % 2
        return lax.rem(me + (NZ - 1 - step if way == 0 else 1 + step), NZ)

    def first_half(i, who):
        b = place(i) * NQ + classes[who]
        return g.at[0, b, i - 7] if i >= 7 else g.at[0, b]

    def second_half(i, who):
        return g.at[1, place(i) * NQ + classes[who]]

    def index(way, step):
        return 0 if step == 0 else 1 + 2 * (step - 1) + way

    def za(way, step):
        z = lax.rem(me + (NZ - step if way == 0 else step), NZ)
        b = z * NQ + quad
        return remote(
            g.at[0, b, way] if step == 3 else g.at[0, b],
            send_za.at[way, step],
            recv_za.at[way, step],
            {"seq": sides[way]},
        )

    def zb(who, way, step):
        z = lax.rem(me + (NZ - step if way == 0 else step), NZ)
        return remote(
            g.at[1, z * NQ + classes[who]],
            send_zb.at[who, way, step],
            recv_zb.at[who, way, step],
            {"seq": sides[way]},
        )

    def ya(i):
        return remote(first_half(i, 0), send_ya.at[i], recv_ya.at[i], {"dp": mates[1]})

    def yb():
        return remote(second_half(0, 0), send_yb, recv_yb, {"dp": mates[1]})

    def da(who, i):
        return remote(
            first_half(i, who), send_da.at[who, i], recv_da.at[who, i], {"dp": mates[0]}
        )

    def db(who, i):
        return remote(
            second_half(i, who), send_db.at[who, i], recv_db.at[who, i], {"dp": mates[0]}
        )

    for c in load_own:
        c.wait()
    pl.semaphore_wait(barrier, 4)
    for way in range(2):
        za(way, 0).start()
    yb().start()
    ya(0).start()
    for way in range(2):
        zb(0, way, 0).start()
    da(0, 0).start()
    db(0, 0).start()

    rows = tz.shape[1]
    zero = jnp.zeros((rows, HD), F32)
    for c in load_tok:
        c.wait()

    def fold(a):
        s = a[:, :HD]
        for k in range(1, width // HD):
            s = s + a[:, k * HD : (k + 1) * HD]
        return s

    def wide(a):
        return jnp.concatenate([a] * (width // HD), axis=1)

    def add_sum(z, s):
        return s + fold(tz[z].astype(F32))

    average = lane_sum(lax.fori_loop(0, NZ, add_sum, zero)) / features

    def add_square(z, s):
        c = tz[z].astype(F32) - wide(average)
        return s + fold(c * c)

    inverse = lax.rsqrt(lane_sum(lax.fori_loop(0, NZ, add_square, zero)) / features + epsilon)
    norm_out[0] = average
    norm_out[1] = inverse

    yb().wait_recv()
    for way in range(2):
        zb(1, way, 0).start()
    db(1, 0).start()

    def low(z, c):
        uz[z] = ((tz[z].astype(F32) - wide(average)) * wide(inverse)).astype(BF16)
        return c

    lax.fori_loop(0, NZ, low, 0)
    for i in range(4):
        acc[i] = jnp.zeros_like(acc[i])
    for c in load_cot:
        c.wait()

    def turn(z, c):
        for src, dst in ((uz, ut_out), (cz, ct_out)):
            a = jnp.transpose(src[z])
            dst[z] = a.reshape(dst.shape[1:])
        return c

    def product(z, slot):
        blocks = pl.ds(pl.multiple_of(z * NQ, NQ), NQ)
        for half in range(2):
            for i in range(2):
                w = g[half, blocks, i].reshape(width, width)
                left = cz if half + i == 2 else uz
                acc[2 * half + i] = acc[2 * half + i] + dot(left[z], w)
            pltpu.make_async_copy(
                g.at[half, blocks], g_out.at[half, blocks], keep.at[slot, half]
            ).start()

    def products(i):
        if i == 0 or i >= 7:
            product(place(i), 0 if i == 0 else 7)
        else:
            product(place(i), i)
            product(place(i + 1), i + 1)

    def other_core(i):
        for who in range(2):
            da(who, i).wait_recv()
            if i < 8:
                db(who, i).wait_recv()

    def next_chip(i):
        ya(i).wait_recv()
        da(1, i).start()

    for step in range(3):
        for way in range(2):
            i = index(way, step + 1)
            za(way, step).wait_recv()
            za(way, step + 1).start()
            ya(i).start()
            da(0, i).start()
        for who in range(2):
            for way in range(2):
                zb(who, way, step).wait_recv()
                if step < 2 or who == way:
                    zb(who, way, step + 1).start()
                db(who, index(way, step + 1)).start()
        if step == 0:
            next_chip(0)
            other_core(0)
            products(0)
        else:
            first = index(0, step)
            for way in range(2):
                next_chip(first + way)
            for way in range(2):
                other_core(first + way)
            products(first)
        lax.fori_loop(2 * step, 2 * step + 2, turn, 0)
    for way in range(2):
        za(way, 3).wait_recv()
        ya(7 + way).start()
        da(0, 7 + way).start()
    lax.fori_loop(6, 8, turn, 0)
    for i in range(5, 7):
        next_chip(i)
    for way in range(2):
        zb(way, way, 3).wait_recv()
        db(way, 7).start()
    for i in range(5, 7):
        other_core(i)
    products(5)
    for i in range(7, 9):
        next_chip(i)
    for i in range(7, 9):
        other_core(i)
    products(7)

    for j in range(3):
        proj_out[:, j * width : (j + 1) * width] = acc[j]
    grad_out[...] = acc[3].astype(BF16)

    for slot in range(NZ):
        for half in range(2):
            blocks = pl.ds(0, NQ)
            pltpu.make_async_copy(
                g.at[half, blocks], g_out.at[half, blocks], keep.at[slot, half]
            ).wait()
    for way in range(2):
        for step in range(4):
            za(way, step).wait_send()
            for who in range(2):
                if step < 3 or who == way:
                    zb(who, way, step).wait_send()
    for i in range(9):
        ya(i).wait_send()
        for who in range(2):
            da(who, i).wait_send()
            if i < 8:
                db(who, i).wait_send()
    yb().wait_send()


def project(tokens, cot, own_qkv, own_out):
    rows, features = tokens.shape
    own, width = own_out.shape
    vmem = pl.BlockSpec(memory_space=pltpu.VMEM)
    hbm = pl.BlockSpec(memory_space=pl.ANY)
    dma = pltpu.SemaphoreType.DMA
    blocks = (2, NZ * NQ, 2, own, width)
    turned = (NZ, NQ, own, rows)
    return pl.pallas_call(
        weights_kernel,
        out_shape=(
            jax.ShapeDtypeStruct((rows, 3 * width), F32),
            jax.ShapeDtypeStruct((rows, width), BF16),
            jax.ShapeDtypeStruct((2, rows, HD), F32),
            jax.ShapeDtypeStruct(turned, BF16),
            jax.ShapeDtypeStruct(turned, BF16),
            jax.ShapeDtypeStruct(blocks, BF16),
        ),
        in_specs=[hbm] * 4,
        out_specs=(vmem, vmem, vmem, vmem, vmem, hbm),
        scratch_shapes=[
            pltpu.VMEM(blocks, BF16),
            pltpu.VMEM((NZ, rows, width), BF16),
            pltpu.VMEM((NZ, rows, width), BF16),
            pltpu.VMEM((NZ, rows, width), BF16),
            pltpu.VMEM((4, rows, width), F32),
            dma((2, 4)),
            dma((2, 4)),
            dma((2, 2, 4)),
            dma((2, 2, 4)),
            dma((9,)),
            dma((9,)),
            dma,
            dma,
            dma((2, 9)),
            dma((2, 9)),
            dma((2, 8)),
            dma((2, 8)),
            dma((4,)),
            dma((NZ,)),
            dma((NZ,)),
            dma((NZ, 2)),
        ],
        compiler_params=pltpu.CompilerParams(
            collective_id=1, has_side_effects=True, vmem_limit_bytes=60 * 1024 * 1024
        ),
    )(tokens, cot, own_qkv, own_out)


def local(tokens, cotangent, qkv_weight, out_weight):
    width = out_weight.shape[1]
    proj, grad, norm, unit_t, cot_t, weights = project(
        tokens[0], cotangent[0], jnp.transpose(qkv_weight, (1, 0, 2)), out_weight
    )
    dw, branch = layer(proj, grad, norm, tokens[0], weights, unit_t, cot_t)
    out_grad = dw[0, :, :width]
    qkv_grad = jnp.stack([dw[0, :, width:], dw[1, :, :width], dw[1, :, width:]], axis=1)
    return (qkv_grad, out_grad, branch[None])


def solution(mesh):
    return jax.shard_map(
        local,
        mesh=mesh,
        in_specs=(
            P("dp", "seq", None),
            P("dp", "seq", None),
            P(("seq", "dp"), None, "tensor"),
            P(("seq", "dp"), "tensor"),
        ),
        out_specs=(
            P(("seq", "dp"), None, "tensor"),
            P(("seq", "dp"), "tensor"),
            P("dp", "seq", "tensor"),
        ),
        check_vma=False,
    )
```

```python
import jax
import jax.numpy as jnp
from jax import lax
from jax.experimental import pallas as pl
from jax.experimental.pallas import tpu as pltpu
from jax.sharding import PartitionSpec as P

HD = 128
NZ = 8
NT = 8
NQ = 4
MESH = pl.DeviceIdType.MESH
F32 = jnp.float32
BF16 = jnp.bfloat16
LAST = (((1,), (1,)), ((), ()))
FIRST = (((0,), (0,)), ((), ()))
epsilon = 1e-06


def dot(a, b, dims=(((1,), (0,)), ((), ()))):
    return lax.dot_general(a, b, dims, preferred_element_type=F32)


def twice(a):
    return jnp.concatenate([a, a], axis=1)


def lane_mean(a):
    return jnp.broadcast_to(jnp.mean(a, axis=1, keepdims=True), a.shape)


def lane_sum(a):
    return jnp.broadcast_to(jnp.sum(a, axis=1, keepdims=True), a.shape)


def layer_kernel(
    heads,
    tokens,
    cot,
    own_qkv,
    own_out,
    qkv_out,
    out_out,
    branch_out,
    q_low,
    do,
    unit,
    inv,
    kv,
    ex,
    dp,
    wsum,
    tsum,
    rtot,
    delta,
    dq,
    sbuf,
    rbuf,
    act,
    low,
    ut,
    ct,
    us,
    cs,
    g,
    tb,
    nb,
    norm,
    sdw,
    rdw,
    dwp,
    xs,
    xr,
    ysend,
    yrecv,
    stats,
    send_ag,
    recv_ag,
    send_rs,
    recv_rs,
    send_tr,
    recv_tr,
    send_act,
    recv_act,
    send_dw,
    recv_dw,
    send_x,
    recv_x,
    send_y,
    recv_y,
    send_st,
    recv_st,
    send_za,
    recv_za,
    send_zb,
    recv_zb,
    send_ya,
    recv_ya,
    send_yb,
    recv_yb,
    send_da,
    recv_da,
    send_db,
    recv_db,
    load_g,
    load_t,
    load_c,
):
    me = lax.axis_index("seq")
    quad = lax.axis_index("dp")
    part = lax.axis_index("tensor")
    sides = (lax.rem(me + 1, NZ), lax.rem(me + NZ - 1, NZ))
    mates = (quad + 1 - 2 * lax.rem(quad, 2), lax.rem(quad + 2, NQ), NQ - 1 - quad)
    xsides = (lax.rem(part + 2, NT), lax.rem(part + NT - 2, NT))
    ymate = part + 1 - 2 * lax.rem(part, 2)
    yhalf = lax.rem(part, 2)
    xplace = part // 2
    scale = HD ** (-0.5)
    width = heads * HD
    features = NT * width

    barrier = pltpu.get_barrier_semaphore()
    for side in sides:
        pl.semaphore_signal(barrier, inc=1, device_id={"seq": side}, device_id_type=MESH)
    for mate in mates:
        pl.semaphore_signal(barrier, inc=1, device_id={"dp": mate}, device_id_type=MESH)
    for k in range(1, NT):
        pl.semaphore_signal(
            barrier, inc=1, device_id={"tensor": lax.rem(part + k, NT)}, device_id_type=MESH
        )

    def remote(src, dst, send, recv, where):
        return pltpu.make_async_remote_copy(
            src_ref=src,
            dst_ref=dst,
            send_sem=send,
            recv_sem=recv,
            device_id=where,
            device_id_type=MESH,
        )

    def gather(way, step, j):
        b = lax.rem(me + (NZ - step if way == 0 else step), NZ)
        return remote(
            kv.at[b, j],
            kv.at[b, j],
            send_ag.at[way, step, j],
            recv_ag.at[way, step, j],
            {"seq": sides[way]},
        )

    def scatter(way, step, j):
        return remote(
            sbuf.at[way, step, j],
            rbuf.at[way, step, j],
            send_rs.at[way, step, j],
            recv_rs.at[way, step, j],
            {"seq": sides[way]},
        )

    def weight_ring(way, step, group):
        return remote(
            sdw.at[way, step, group],
            rdw.at[way, step, group],
            send_dw.at[way, step, group],
            recv_dw.at[way, step, group],
            {"seq": sides[way]},
        )

    def transposed(k, which):
        src, dst = ((us, ut), (cs, ct))[which]
        return remote(
            src.at[:, mates[k]],
            dst.at[quad],
            send_tr.at[k, which],
            recv_tr.at[k, which],
            {"dp": mates[k]},
        )

    def shared(group, k):
        block = act.at[group, quad if k < 2 else mates[1]]
        return remote(
            block,
            block,
            send_act.at[group, k],
            recv_act.at[group, k],
            {"dp": mates[1] if k == 1 else mates[0]},
        )

    def xring(way, step, half):
        return remote(
            xs.at[way, step, half],
            xr.at[way, step, half],
            send_x.at[way, step, half],
            recv_x.at[way, step, half],
            {"tensor": xsides[way]},
        )

    def ypair():
        return remote(ysend, yrecv, send_y, recv_y, {"tensor": ymate})

    def stat(k):
        return remote(
            stats.at[0],
            stats.at[k],
            send_st.at[k - 1],
            recv_st.at[k - 1],
            {"tensor": lax.rem(part + k, NT)},
        )

    def goes(way, step, j):
        return step < 3 or j % 2 == way

    mine = me * NQ + quad
    load_own = [
        pltpu.make_async_copy(own_qkv.at[1], g.at[0, 0, mine], load_g.at[0]),
        pltpu.make_async_copy(own_qkv.at[2], g.at[0, 1, mine], load_g.at[1]),
        pltpu.make_async_copy(own_qkv.at[0], g.at[1, 0, mine], load_g.at[2]),
        pltpu.make_async_copy(own_out, g.at[1, 1, mine], load_g.at[3]),
    ]
    load_tokens = [
        pltpu.make_async_copy(tokens.at[:, z * width : (z + 1) * width], tb.at[z], load_t.at[z])
        for z in range(NZ)
    ]
    load_cot = [
        pltpu.make_async_copy(
            cot.at[:, (z * heads + h) * HD : (z * heads + h + 1) * HD],
            sbuf.at[z // 4, z % 4, 1, h],
            load_c.at[z, h],
        )
        for z in range(NZ)
        for h in range(heads)
    ]
    for c in load_own + load_tokens + load_cot:
        c.start()

    classes = (quad, mates[1])
    half_rows = own_out.shape[0] // 2

    def place(i):
        if i == 0:
            return me
        if i >= 7:
            return lax.rem(me + 4, NZ)
        step, way = (i - 1) // 2, (i - 1) % 2
        return lax.rem(me + (NZ - 1 - step if way == 0 else 1 + step), NZ)

    def first_array(p, i, who):
        b = place(i) * NQ + classes[who]
        if i >= 7:
            return g.at[p, 0, b, (i - 7) * half_rows : (i - 6) * half_rows]
        return g.at[p, 0, b]

    def second_array(p, i, who):
        return g.at[p, 1, place(i) * NQ + classes[who]]

    def index(way, step):
        return 0 if step == 0 else 1 + 2 * (step - 1) + way

    def same(block, send, recv, where):
        return remote(block, block, send, recv, where)

    def za(p, way, step):
        return same(
            g.at[p, 0, lax.rem(me + (NZ - step if way == 0 else step), NZ) * NQ + quad]
            if step < 3
            else g.at[
                p,
                0,
                lax.rem(me + (NZ - step if way == 0 else step), NZ) * NQ + quad,
                way * half_rows : (way + 1) * half_rows,
            ],
            send_za.at[p, way, step],
            recv_za.at[p, way, step],
            {"seq": sides[way]},
        )

    def zb(p, who, way, step):
        z = lax.rem(me + (NZ - step if way == 0 else step), NZ)
        return same(
            g.at[p, 1, z * NQ + classes[who]],
            send_zb.at[p, who, way, step],
            recv_zb.at[p, who, way, step],
            {"seq": sides[way]},
        )

    def ya(p, i):
        return same(
            first_array(p, i, 0), send_ya.at[p, i], recv_ya.at[p, i], {"dp": mates[1]}
        )

    def yb(p):
        return same(second_array(p, 0, 0), send_yb.at[p], recv_yb.at[p], {"dp": mates[1]})

    def da(p, who, i):
        return same(
            first_array(p, i, who),
            send_da.at[p, who, i],
            recv_da.at[p, who, i],
            {"dp": mates[0]},
        )

    def db(p, who, i):
        return same(
            second_array(p, i, who),
            send_db.at[p, who, i],
            recv_db.at[p, who, i],
            {"dp": mates[0]},
        )

    for c in load_own:
        c.wait()
    pl.semaphore_wait(barrier, 2 + 3 + NT - 1)
    for p in range(2):
        for way in range(2):
            za(p, way, 0).start()
        yb(p).start()
        ya(p, 0).start()
        for way in range(2):
            zb(p, 0, way, 0).start()
        da(p, 0, 0).start()
        db(p, 0, 0).start()

    rows = tb.shape[1]
    blank = jnp.zeros((rows, HD), F32)
    for c in load_tokens:
        c.wait()

    def fold(a):
        s = a[:, :HD]
        for k in range(1, heads):
            s = s + a[:, k * HD : (k + 1) * HD]
        return s

    def wide(a):
        return jnp.concatenate([a] * heads, axis=1)

    def add_sum(z, s):
        return s + fold(tb[z].astype(F32))

    average = lane_sum(lax.fori_loop(0, NZ, add_sum, blank)) / features

    def add_square(z, s):
        c = tb[z].astype(F32) - wide(average)
        return s + fold(c * c)

    norm[0] = average
    norm[1] = lax.rsqrt(lane_sum(lax.fori_loop(0, NZ, add_square, blank)) / features + epsilon)

    for p in range(2):
        yb(p).wait_recv()
        for way in range(2):
            zb(p, 1, way, 0).start()
        db(p, 1, 0).start()

    def lower(z, c):
        for h in range(heads):
            a = tb[z, :, h * HD : (h + 1) * HD].astype(F32)
            sbuf[z // 4, lax.rem(z, 4), 0, h] = ((a - norm[0]) * norm[1]).astype(BF16)
        return c

    lax.fori_loop(0, NZ, lower, 0)
    for i in range(4):
        nb[i] = jnp.zeros_like(nb[i])
    for c in load_cot:
        c.wait()

    def low_rows(z, which):
        return jnp.concatenate(
            [sbuf[z // 4, lax.rem(z, 4), which, h] for h in range(heads)], axis=1
        )

    def turn(first, count):
        def step(z, c):
            for which, (dst, kept) in enumerate(((us, ut), (cs, ct))):
                dst[z] = jnp.transpose(low_rows(z, which)).reshape(dst.shape[1:])
                kept[quad, z] = dst[z, quad]
            return c

        lax.fori_loop(first, first + count, step, 0)

    def products(p, i):
        def one(z):
            blocks = pl.ds(pl.multiple_of(z * NQ, NQ), NQ)
            for j in range(2):
                left = low_rows(z, 1 if p + j == 2 else 0)
                nb[2 * p + j] = nb[2 * p + j] + dot(left, g[p, j, blocks].reshape(width, width))

        if i == 0 or i >= 7:
            one(place(i))
        else:

            def step(n, c):
                d = (i + 1) // 2
                one(lax.rem(me + NZ - d + 2 * d * n, NZ))
                return c

            lax.fori_loop(0, 2, step, 0)

    def other_core(p, i):
        for who in range(2):
            da(p, who, i).wait_recv()
            if i < 8:
                db(p, who, i).wait_recv()

    def next_chip(p, i):
        ya(p, i).wait_recv()
        da(p, 1, i).start()

    def ring_step(p, step):
        for way in range(2):
            i = index(way, step + 1)
            za(p, way, step).wait_recv()
            za(p, way, step + 1).start()
            ya(p, i).start()
            da(p, 0, i).start()
        for who in range(2):
            for way in range(2):
                zb(p, who, way, step).wait_recv()
                if step < 2 or who == way:
                    zb(p, who, way, step + 1).start()
                db(p, who, index(way, step + 1)).start()

    def ring_last(p):
        for way in range(2):
            za(p, way, 3).wait_recv()
            ya(p, 7 + way).start()
            da(p, 0, 7 + way).start()
        for way in range(2):
            zb(p, way, way, 3).wait_recv()
            db(p, way, 7).start()

    def settle(p, step):
        these = (0,) if step == 0 else (2 * step - 1, 2 * step) if step < 4 else (7, 8)
        for i in these:
            next_chip(p, i)
        for i in these:
            other_core(p, i)
        products(p, these[0])

    def normal(a, j, h):
        c = a - lane_mean(a)
        r = lax.rsqrt(lane_mean(c * c) + epsilon)
        u = c * r
        unit[j, h] = u
        inv[j, h] = r
        return u.astype(BF16)

    ring_step(0, 0)
    turn(0, 2)
    settle(0, 0)
    ring_step(0, 1)
    settle(0, 1)
    turn(2, 2)
    ring_step(1, 0)
    ring_step(0, 2)
    settle(0, 2)
    turn(4, 2)
    ring_step(1, 1)
    settle(1, 0)
    ring_last(0)
    settle(0, 3)
    ring_step(1, 2)
    settle(0, 4)
    for h in range(heads):
        at = slice(h * HD, (h + 1) * HD)
        kv[me, 0, h] = normal(nb[0, :, at], 1, h)
        kv[me, 1, h] = nb[1, :, at].astype(BF16)
    for j in range(2):
        for way in range(2):
            gather(way, 0, j).start()
    settle(1, 1)
    settle(1, 2)
    turn(6, 2)
    ring_last(1)
    for which in range(2):
        for k in range(3):
            transposed(k, which).start()
    settle(1, 3)
    settle(1, 4)
    for h in range(heads):
        at = slice(h * HD, (h + 1) * HD)
        q_low[h] = normal(nb[2, :, at], 0, h)
        do[h] = nb[3, :, at].astype(BF16)
        wsum[h] = jnp.zeros_like(wsum[h])
        tsum[h] = jnp.zeros_like(tsum[h])
        dq[h] = jnp.zeros_like(dq[h])

    def forward(b, h):
        k = kv[b, 0, h]
        v = kv[b, 1, h]
        e = jnp.exp(dot(q_low[h], k, LAST) * scale)
        ex[b, h] = e
        tsum[h] = tsum[h] + (e[:, :HD] + e[:, HD:])
        wsum[h] = wsum[h] + dot(e.astype(BF16), v)
        dp[b, h] = dot(do[h], v, LAST)

    def forward_blocks(ahead, behind):
        def step(i, c):
            b = lax.rem(me + ahead + (i // heads) * (behind - ahead), NZ)
            forward(b, lax.rem(i, heads))
            return c

        lax.fori_loop(0, heads if ahead == behind else 2 * heads, step, 0)

    forward_blocks(0, 0)
    for step in range(3):
        for j in range(2):
            for way in range(2):
                gather(way, step, j).wait_recv()
                if goes(way, step + 1, j):
                    gather(way, step + 1, j).start()
        forward_blocks(NZ - 1 - step, 1 + step)
    gather(0, 3, 0).wait_recv()
    gather(1, 3, 1).wait_recv()
    forward_blocks(4, 4)

    for h in range(heads):
        total = lane_sum(tsum[h])
        a = (wsum[h] / total).astype(BF16)
        act[0, quad, :, h * HD : (h + 1) * HD] = a
        rtot[h] = 1.0 / total
        delta[h] = lane_sum(do[h].astype(F32) * a.astype(F32))
    shared(0, 1).start()
    shared(0, 0).start()

    def backward(b, h):
        p = ex[b, h] * twice(rtot[h])
        ds = (p * (dp[b, h] - twice(delta[h])) * scale).astype(BF16)
        dq[h] = dq[h] + dot(ds, kv[b, 0, h])
        ex[b, h, :, :HD] = dot(ds, q_low[h], FIRST)
        ex[b, h, :, HD:] = dot(p.astype(BF16), do[h], FIRST)

    def backward_blocks(first, count):
        def step(i, c):
            n = first + i // heads
            away = (n + 1) // 2
            b = lax.rem(me + 4 + lax.rem(n, 2) * (NZ - 2 * away) + away, NZ)
            backward(b, lax.rem(i, heads))
            return c

        lax.fori_loop(0, count * heads, step, 0)

    def scatter_step(step):
        for j in range(2):
            for way in range(2):
                if not goes(way, 3 - step, j):
                    continue
                b = lax.rem(me + (4 - step if way == 0 else 4 + step), NZ)
                added = step > 0 and goes(way, 4 - step, j)
                if added:
                    scatter(way, step - 1, j).wait_recv()
                for h in range(heads):
                    val = ex[b, h, :, j * HD : (j + 1) * HD]
                    if added:
                        val = val + rbuf[way, step - 1, j, h].astype(F32)
                    sbuf[way, step, j, h] = val.astype(BF16)
                scatter(way, step, j).start()

    def relay(group):
        shared(group, 1).wait_recv()
        shared(group, 2).start()

    def back(val, j, h):
        u = unit[j, h]
        return (val - lane_mean(val) - u * lane_mean(val * u)) * inv[j, h]

    backward_blocks(0, 1)
    scatter_step(0)
    backward_blocks(1, 7)
    for h in range(heads):
        a = back(dq[h], 0, h).astype(BF16)
        act[1, quad, :, h * HD : (h + 1) * HD] = a
        low[:, h * HD : (h + 1) * HD] = a
    shared(1, 1).start()
    shared(1, 0).start()
    scatter_step(1)
    relay(0)
    scatter_step(2)
    relay(1)
    scatter_step(3)

    for which in range(2):
        for k in range(3):
            transposed(k, which).wait_recv()
    for group in range(2):
        shared(group, 0).wait_recv()
        shared(group, 2).wait_recv()

    def weight_block(z, group):
        left = ct if group == 0 else ut
        acc = dot(left[0, z], act[group, 0])
        for m in range(1, NQ):
            acc = acc + dot(left[m, z], act[group, m])
        dwp[z, group] = acc

    def weight_blocks(*groups):
        def step(i, c):
            for group in groups:
                weight_block(lax.rem(me + 5 + i, NZ), group)
            return c

        lax.fori_loop(0, NZ - 1, step, 0)

    def weight_step(step, group):
        for way in range(2):
            if not goes(way, 3 - step, group):
                continue
            z = lax.rem(me + (4 - step if way == 0 else 4 + step), NZ)
            val = dwp[z, group]
            if step > 0 and goes(way, 4 - step, group):
                weight_ring(way, step - 1, group).wait_recv()
                val = val + rdw[way, step - 1, group].astype(F32)
            sdw[way, step, group] = val.astype(BF16)
            weight_ring(way, step, group).start()

    for group in range(2):
        weight_block(lax.rem(me + 4, NZ), group)
        weight_step(0, group)
    weight_blocks(0, 1)

    for j in range(2):
        for way in range(2):
            scatter(way, 3, j).wait_recv()
        for h in range(heads):
            val = ex[me, h, :, j * HD : (j + 1) * HD]
            val = val + rbuf[0, 3, j, h].astype(F32) + rbuf[1, 3, j, h].astype(F32)
            if j == 0:
                val = back(val, 1, h)
            a = val.astype(BF16)
            act[2 + j, quad, :, h * HD : (h + 1) * HD] = a
            low[:, (j + 1) * width + h * HD : (j + 1) * width + (h + 1) * HD] = a
        shared(2 + j, 1).start()
        shared(2 + j, 0).start()
        for group in range(2):
            weight_step(1 + j, group)

    def inner(n, sums):
        x = lax.rem(xplace + 2 + n // 2, 4)
        t = 2 * x + lax.rem(n, 2)
        blocks = pl.ds(pl.multiple_of(t * NQ, NQ), NQ)
        a = jnp.zeros_like(nb[t])
        for j, (p, i) in enumerate(((1, 0), (0, 0), (0, 1))):
            left = low[:, j * width : (j + 1) * width]
            a = a + dot(left, g[p, i, blocks].reshape(width, width), LAST)
        nb[t] = a
        one, two = sums
        for k in range(heads):
            at = slice(k * HD, (k + 1) * HD)
            one = one + a[:, at]
            two = two + a[:, at] * ((tb[t, :, at].astype(F32) - norm[0]) * norm[1])
        return one, two

    def piece(x, half):
        return nb[2 * x + (1 - yhalf if half == 0 else yhalf)]

    def inner_step(step):
        for half in range(2):
            for way in range(2):
                if step == 0 and half != way:
                    continue
                x = lax.rem(xplace + (2 - step if way == 0 else 2 + step), 4)
                val = piece(x, half)
                if step > 0 and half == way:
                    xring(way, 0, half).wait_recv()
                    val = val + xr[way, 0, half].astype(F32)
                xs[way, step, half] = val.astype(BF16)
                xring(way, step, half).start()

    def arrived(half):
        for way in range(2):
            xring(way, 1, half).wait_recv()
        val = piece(xplace, half)
        return val + xr[0, 1, half].astype(F32) + xr[1, 1, half].astype(F32)

    far = lax.rem(me + 4, NZ)
    zero = jnp.zeros((low.shape[0], HD), F32)
    sums = lax.fori_loop(0, 2, inner, (zero, zero))
    inner_step(0)
    sums = lax.fori_loop(2, 4, inner, sums)
    relay(2)
    sums = lax.fori_loop(4, NT, inner, sums)
    shared(2, 0).wait_recv()
    shared(2, 2).wait_recv()
    weight_block(far, 2)
    weight_step(0, 2)
    for i in range(2):
        stats[0, i * 8 : (i + 1) * 8, :] = jnp.transpose(lane_sum(sums[i]))[:8]
    for k in range(1, NT):
        stat(k).start()
    relay(3)
    weight_blocks(2)
    for group in range(2):
        weight_step(3, group)
    inner_step(1)
    weight_step(1, 2)
    shared(3, 0).wait_recv()
    shared(3, 2).wait_recv()
    weight_block(far, 3)
    weight_step(0, 3)
    weight_blocks(3)
    weight_step(2, 2)
    ysend[...] = arrived(0).astype(BF16)
    ypair().start()
    weight_step(1, 3)
    weight_step(3, 2)
    weight_step(2, 3)
    for k in range(1, NT):
        stat(k).wait_recv()
    total = stats[0]
    for k in range(1, NT):
        total = total + stats[k]
    row_mean = []
    for i in range(2):
        row = jnp.broadcast_to(total[i * 8 : i * 8 + 1, :], (HD, total.shape[1]))
        row_mean.append(jnp.transpose(row) / features)
    share = arrived(1)
    weight_step(3, 3)

    ypair().wait_recv()
    share = share + yrecv[...].astype(F32)
    for k in range(heads):
        at = slice(k * HD, (k + 1) * HD)
        own_unit = (tb[part, :, at].astype(F32) - norm[0]) * norm[1]
        val = share[:, at] - row_mean[0] - own_unit * row_mean[1]
        branch_out[:, at] = (val * norm[1]).astype(BF16)

    for group in range(4):
        val = dwp[me, group]
        for way in range(2):
            weight_ring(way, 3, group).wait_recv()
            val = val + rdw[way, 3, group].astype(F32)
        if group == 0:
            out_out[...] = val
        else:
            qkv_out[group - 1] = val

    for p in range(2):
        for way in range(2):
            for step in range(4):
                za(p, way, step).wait_send()
                for who in range(2):
                    if step < 3 or who == way:
                        zb(p, who, way, step).wait_send()
        for i in range(9):
            ya(p, i).wait_send()
            for who in range(2):
                da(p, who, i).wait_send()
                if i < 8:
                    db(p, who, i).wait_send()
        yb(p).wait_send()
    for step in range(4):
        for j in range(2):
            for way in range(2):
                if goes(way, step, j):
                    gather(way, step, j).wait_send()
                if goes(way, 3 - step, j):
                    scatter(way, step, j).wait_send()
                    weight_ring(way, step, j).wait_send()
                    weight_ring(way, step, j + 2).wait_send()
    for which in range(2):
        for k in range(3):
            transposed(k, which).wait_send()
    for group in range(4):
        for k in range(3):
            shared(group, k).wait_send()
    for way in range(2):
        xring(way, 0, way).wait_send()
        for half in range(2):
            xring(way, 1, half).wait_send()
    ypair().wait_send()
    for k in range(1, NT):
        stat(k).wait_send()


def layer(tokens, cot, own_qkv, own_out):
    rows = tokens.shape[0]
    own, width = own_out.shape
    heads = width // HD
    vmem = pl.BlockSpec(memory_space=pltpu.VMEM)
    hbm = pl.BlockSpec(memory_space=pl.ANY)
    one = (heads, rows, HD)
    dma = pltpu.SemaphoreType.DMA
    return pl.pallas_call(
        lambda *refs: layer_kernel(heads, *refs),
        out_shape=(
            jax.ShapeDtypeStruct((3, own, width), F32),
            jax.ShapeDtypeStruct((own, width), F32),
            jax.ShapeDtypeStruct((rows, width), BF16),
        ),
        in_specs=[hbm] * 4,
        out_specs=(vmem, vmem, vmem),
        scratch_shapes=[
            pltpu.VMEM(one, BF16),
            pltpu.VMEM(one, BF16),
            pltpu.VMEM((2, *one), F32),
            pltpu.VMEM((2, *one), F32),
            pltpu.VMEM((NZ, 2, *one), BF16),
            pltpu.VMEM((NZ, heads, rows, rows), F32),
            pltpu.VMEM((NZ, heads, rows, rows), F32),
            pltpu.VMEM(one, F32),
            pltpu.VMEM(one, F32),
            pltpu.VMEM(one, F32),
            pltpu.VMEM(one, F32),
            pltpu.VMEM(one, F32),
            pltpu.VMEM((2, 4, 2, *one), BF16),
            pltpu.VMEM((2, 4, 2, *one), BF16),
            pltpu.VMEM((4, NQ, rows, width), BF16),
            pltpu.VMEM((rows, 3 * width), BF16),
            pltpu.VMEM((NQ, NZ, own, rows), BF16),
            pltpu.VMEM((NQ, NZ, own, rows), BF16),
            pltpu.VMEM((NZ, NQ, own, rows), BF16),
            pltpu.VMEM((NZ, NQ, own, rows), BF16),
            pltpu.VMEM((2, 2, NZ * NQ, own, width), BF16),
            pltpu.VMEM((NT, rows, width), BF16),
            pltpu.VMEM((NT, rows, width), F32),
            pltpu.VMEM((2, rows, HD), F32),
            pltpu.VMEM((2, 4, 4, own, width), BF16),
            pltpu.VMEM((2, 4, 4, own, width), BF16),
            pltpu.VMEM((NZ, 4, own, width), F32),
            pltpu.VMEM((2, 2, 2, rows, width), BF16),
            pltpu.VMEM((2, 2, 2, rows, width), BF16),
            pltpu.VMEM((rows, width), BF16),
            pltpu.VMEM((rows, width), BF16),
            pltpu.VMEM((NT, 16, rows), F32),
            dma((2, 4, 2)),
            dma((2, 4, 2)),
            dma((2, 4, 2)),
            dma((2, 4, 2)),
            dma((3, 2)),
            dma((3, 2)),
            dma((4, 3)),
            dma((4, 3)),
            dma((2, 4, 4)),
            dma((2, 4, 4)),
            dma((2, 2, 2)),
            dma((2, 2, 2)),
            dma,
            dma,
            dma((NT - 1,)),
            dma((NT - 1,)),
            dma((2, 2, 4)),
            dma((2, 2, 4)),
            dma((2, 2, 2, 4)),
            dma((2, 2, 2, 4)),
            dma((2, 9)),
            dma((2, 9)),
            dma((2,)),
            dma((2,)),
            dma((2, 2, 9)),
            dma((2, 2, 9)),
            dma((2, 2, 8)),
            dma((2, 2, 8)),
            dma((4,)),
            dma((NZ,)),
            dma((NZ, heads)),
        ],
        compiler_params=pltpu.CompilerParams(
            collective_id=0, has_side_effects=True, vmem_limit_bytes=67_043_328
        ),
    )(tokens, cot, own_qkv, own_out)


def finish(*arrays):
    def kernel(*refs):
        for i in range(len(arrays)):
            refs[len(arrays) + i][...] = refs[i][...]

    vmem = pl.BlockSpec(memory_space=pltpu.VMEM)
    return pl.pallas_call(
        kernel,
        out_shape=tuple(jax.ShapeDtypeStruct(a.shape, a.dtype) for a in arrays),
        in_specs=[vmem] * len(arrays),
        out_specs=(vmem,) * len(arrays),
    )(*arrays)


def local(tokens, cotangent, qkv_weight, out_weight):
    qkv_grad, out_grad, branch = finish(
        *layer(tokens[0], cotangent[0], jnp.transpose(qkv_weight, (1, 0, 2)), out_weight)
    )
    return (jnp.transpose(qkv_grad, (1, 0, 2)), out_grad, branch[None])


def solution(mesh):
    return jax.shard_map(
        local,
        mesh=mesh,
        in_specs=(
            P("dp", "seq", None),
            P("dp", "seq", None),
            P(("seq", "dp"), None, "tensor"),
            P(("seq", "dp"), "tensor"),
        ),
        out_specs=(
            P(("seq", "dp"), None, "tensor"),
            P(("seq", "dp"), "tensor"),
            P("dp", "seq", "tensor"),
        ),
        check_vma=False,
    )
```

```python
import jax
import jax.numpy as jnp
from jax import lax
from jax.experimental import pallas as pl
from jax.experimental.pallas import tpu as pltpu
from jax.sharding import PartitionSpec as P

HD = 128
NZ = 8
NT = 8
NQ = 4
MESH = pl.DeviceIdType.MESH
F32 = jnp.float32
BF16 = jnp.bfloat16
LAST = (((1,), (1,)), ((), ()))
FIRST = (((0,), (0,)), ((), ()))
epsilon = 1e-06


def dot(a, b, dims=(((1,), (0,)), ((), ()))):
    return lax.dot_general(a, b, dims, preferred_element_type=F32)


def twice(a):
    return jnp.concatenate([a, a], axis=1)


def lane_mean(a):
    return jnp.broadcast_to(jnp.mean(a, axis=1, keepdims=True), a.shape)


def lane_sum(a):
    return jnp.broadcast_to(jnp.sum(a, axis=1, keepdims=True), a.shape)


def layer_kernel(
    heads,
    tokens,
    cot,
    own_qkv,
    own_out,
    qkv_out,
    out_out,
    branch_out,
    q_low,
    do,
    unit,
    inv,
    kv,
    ex,
    dp,
    wsum,
    tsum,
    rtot,
    delta,
    dq,
    sbuf,
    rbuf,
    act,
    low,
    ut,
    ct,
    us,
    cs,
    g,
    tb,
    nb,
    norm,
    sdw,
    rdw,
    dwp,
    xs,
    xr,
    ysend,
    yrecv,
    stats,
    send_ag,
    recv_ag,
    send_rs,
    recv_rs,
    send_tr,
    recv_tr,
    send_act,
    recv_act,
    send_dw,
    recv_dw,
    send_x,
    recv_x,
    send_y,
    recv_y,
    send_st,
    recv_st,
    send_w,
    recv_za,
    recv_zb,
    recv_ya,
    recv_yb,
    recv_d,
    load_g,
    load_t,
    load_c,
):
    me = lax.axis_index("seq")
    quad = lax.axis_index("dp")
    part = lax.axis_index("tensor")
    sides = (lax.rem(me + 1, NZ), lax.rem(me + NZ - 1, NZ))
    mates = (quad + 1 - 2 * lax.rem(quad, 2), lax.rem(quad + 2, NQ), NQ - 1 - quad)
    xsides = (lax.rem(part + 2, NT), lax.rem(part + NT - 2, NT))
    ymate = part + 1 - 2 * lax.rem(part, 2)
    yhalf = lax.rem(part, 2)
    xplace = part // 2
    scale = HD ** (-0.5)
    width = heads * HD
    features = NT * width
    half_block = tokens.shape[0] // 2

    barrier = pltpu.get_barrier_semaphore()
    for side in sides:
        pl.semaphore_signal(barrier, inc=1, device_id={"seq": side}, device_id_type=MESH)
    for mate in mates:
        pl.semaphore_signal(barrier, inc=1, device_id={"dp": mate}, device_id_type=MESH)
    for k in range(1, NT):
        pl.semaphore_signal(
            barrier, inc=1, device_id={"tensor": lax.rem(part + k, NT)}, device_id_type=MESH
        )

    def remote(src, dst, send, recv, where):
        return pltpu.make_async_remote_copy(
            src_ref=src,
            dst_ref=dst,
            send_sem=send,
            recv_sem=recv,
            device_id=where,
            device_id_type=MESH,
        )

    def gather(way, step, j):
        b = lax.rem(me + (NZ - step if way == 0 else step), NZ)
        return remote(
            kv.at[b, j],
            kv.at[b, j],
            send_ag,
            recv_ag.at[way, step, j],
            {"seq": sides[way]},
        )

    def scatter(way, step, j):
        part_of = pl.ds(way * half_block, half_block) if step == 0 else pl.ds(0, 2 * half_block)
        return remote(
            sbuf.at[way, step, j, :, part_of],
            rbuf.at[way, step, j, :, part_of],
            send_rs,
            recv_rs.at[way, step, j],
            {"seq": sides[way]},
        )

    def weight_ring(way, step, group):
        return remote(
            sdw.at[way, step, group],
            rdw.at[way, step, group],
            send_dw,
            recv_dw.at[way, step, group],
            {"seq": sides[way]},
        )

    def transposed(k, which):
        src, dst = ((us, ut), (cs, ct))[which]
        return remote(
            src.at[:, mates[k]],
            dst.at[quad],
            send_tr.at[which],
            recv_tr.at[which],
            {"dp": mates[k]},
        )

    def shared(group, k):
        block = act.at[group, quad if k < 2 else mates[1]]
        return remote(
            block,
            block,
            send_act,
            recv_act.at[group, k],
            {"dp": mates[1] if k == 1 else mates[0]},
        )

    def xring(way, step, half):
        return remote(
            xs.at[way, step, half],
            xr.at[way, step, half],
            send_x,
            recv_x.at[way, step, half],
            {"tensor": xsides[way]},
        )

    def ypair():
        return remote(ysend, yrecv, send_y, recv_y, {"tensor": ymate})

    def stat(k):
        return remote(
            stats.at[0],
            stats.at[k],
            send_st,
            recv_st,
            {"tensor": lax.rem(part + k, NT)},
        )

    def goes(way, step, j):
        return step < 3 or j % 2 == way

    mine = me * NQ + quad
    load_own = [
        pltpu.make_async_copy(own_qkv.at[1], g.at[0, 0, mine], load_g),
        pltpu.make_async_copy(own_qkv.at[2], g.at[0, 1, mine], load_g),
        pltpu.make_async_copy(own_qkv.at[0], g.at[1, 0, mine], load_g),
        pltpu.make_async_copy(own_out, g.at[1, 1, mine], load_g),
    ]
    load_tokens = [
        pltpu.make_async_copy(tokens.at[:, z * width : (z + 1) * width], tb.at[z], load_t)
        for z in range(NZ)
    ]
    load_cot = [
        pltpu.make_async_copy(
            cot.at[:, (z * heads + h) * HD : (z * heads + h + 1) * HD],
            sbuf.at[z // 4, z % 4, 1, h],
            load_c,
        )
        for z in range(NZ)
        for h in range(heads)
    ]
    for c in load_own + load_tokens + load_cot:
        c.start()

    classes = (quad, mates[1])
    half_rows = own_out.shape[0] // 2

    def place(i):
        if i == 0:
            return me
        if i >= 7:
            return lax.rem(me + 4, NZ)
        step, way = (i - 1) // 2, (i - 1) % 2
        return lax.rem(me + (NZ - 1 - step if way == 0 else 1 + step), NZ)

    def first_array(p, i, who):
        b = place(i) * NQ + classes[who]
        if i >= 7:
            return g.at[p, 0, b, (i - 7) * half_rows : (i - 6) * half_rows]
        return g.at[p, 0, b]

    def second_array(p, i, who):
        return g.at[p, 1, place(i) * NQ + classes[who]]

    def stage(i):
        return 4 if i >= 7 else (i + 1) // 2

    def index(way, step):
        return 0 if step == 0 else 1 + 2 * (step - 1) + way

    def same(block, send, recv, where):
        return remote(block, block, send, recv, where)

    def za(p, way, step):
        return same(
            g.at[p, 0, lax.rem(me + (NZ - step if way == 0 else step), NZ) * NQ + quad]
            if step < 3
            else g.at[
                p,
                0,
                lax.rem(me + (NZ - step if way == 0 else step), NZ) * NQ + quad,
                way * half_rows : (way + 1) * half_rows,
            ],
            send_w,
            recv_za.at[p, way, step],
            {"seq": sides[way]},
        )

    def zb(p, who, way, step):
        z = lax.rem(me + (NZ - step if way == 0 else step), NZ)
        return same(
            g.at[p, 1, z * NQ + classes[who]],
            send_w,
            recv_zb.at[p, who, way, step],
            {"seq": sides[way]},
        )

    def ya(p, i):
        return same(
            first_array(p, i, 0), send_w, recv_ya.at[p, stage(i)], {"dp": mates[1]}
        )

    def yb(p):
        return same(second_array(p, 0, 0), send_w, recv_yb.at[p], {"dp": mates[1]})

    def da(p, who, i):
        return same(
            first_array(p, i, who),
            send_w,
            recv_d.at[p, stage(i)],
            {"dp": mates[0]},
        )

    def db(p, who, i):
        return same(
            second_array(p, i, who),
            send_w,
            recv_d.at[p, stage(i)],
            {"dp": mates[0]},
        )

    def whole(ref, sem):
        return pltpu.make_async_copy(ref, ref, sem)

    def units(n):
        return g.at[0, 0, 0:n]

    def all_sent(ref, sem):
        remote(ref, ref, sem, sem, {"seq": sides[0]}).wait_send()

    def all_here(ref, sem):
        remote(ref, ref, sem, sem, {"seq": sides[0]}).wait_recv()

    whole(units(4), load_g).wait()
    pl.semaphore_wait(barrier, 2 + 3 + NT - 1)
    for way in range(2):
        za(0, way, 0).start()
    for p in range(2):
        yb(p).start()
    for way in range(2):
        zb(0, 0, way, 0).start()
    for p in range(2):
        ya(p, 0).start()
    for way in range(2):
        za(1, way, 0).start()
    for p in range(2):
        da(p, 0, 0).start()
        db(p, 0, 0).start()

    rows = tb.shape[1]
    blank = jnp.zeros((rows, HD), F32)
    whole(tb, load_t).wait()

    def fold(a):
        s = a[:, :HD]
        for k in range(1, heads):
            s = s + a[:, k * HD : (k + 1) * HD]
        return s

    def wide(a):
        return jnp.concatenate([a] * heads, axis=1)

    def add_sum(z, s):
        return s + fold(tb[z].astype(F32))

    average = lane_sum(lax.fori_loop(0, NZ, add_sum, blank)) / features

    def add_square(z, s):
        c = tb[z].astype(F32) - wide(average)
        return s + fold(c * c)

    norm[0] = average
    norm[1] = lax.rsqrt(lane_sum(lax.fori_loop(0, NZ, add_square, blank)) / features + epsilon)

    yb(0).wait_recv()
    for way in range(2):
        zb(0, 1, way, 0).start()
    db(0, 1, 0).start()

    def lower(z, c):
        for h in range(heads):
            a = tb[z, :, h * HD : (h + 1) * HD].astype(F32)
            sbuf[z // 4, lax.rem(z, 4), 0, h] = ((a - norm[0]) * norm[1]).astype(BF16)
        return c

    lax.fori_loop(0, NZ, lower, 0)
    for i in range(4):
        nb[i] = jnp.zeros_like(nb[i])
    whole(sbuf.at[:, :, 1], load_c).wait()

    def low_rows(z, which):
        return jnp.concatenate(
            [sbuf[z // 4, lax.rem(z, 4), which, h] for h in range(heads)], axis=1
        )

    def turn(first, count):
        def step(z, c):
            for which, (dst, kept) in enumerate(((us, ut), (cs, ct))):
                dst[z] = jnp.transpose(low_rows(z, which)).reshape(dst.shape[1:])
                kept[quad, z] = dst[z, quad]
            return c

        lax.fori_loop(first, first + count, step, 0)

    def products(p, i):
        def one(z):
            blocks = pl.ds(pl.multiple_of(z * NQ, NQ), NQ)
            for j in range(2):
                left = low_rows(z, 1 if p + j == 2 else 0)
                nb[2 * p + j] = nb[2 * p + j] + dot(left, g[p, j, blocks].reshape(width, width))

        if i == 0 or i >= 7:
            one(place(i))
        else:

            def step(n, c):
                d = (i + 1) // 2
                one(lax.rem(me + NZ - d + 2 * d * n, NZ))
                return c

            lax.fori_loop(0, 2, step, 0)

    def ring_step(p, step):
        for way in range(2):
            i = index(way, step + 1)
            za(p, way, step).wait_recv()
            za(p, way, step + 1).start()
            ya(p, i).start()
            da(p, 0, i).start()
        for who in range(2):
            for way in range(2):
                zb(p, who, way, step).wait_recv()
                if step < 2 or who == way:
                    zb(p, who, way, step + 1).start()
                db(p, who, index(way, step + 1)).start()

    def ring_last(p):
        for way in range(2):
            za(p, way, 3).wait_recv()
            ya(p, 7 + way).start()
            da(p, 0, 7 + way).start()
        for way in range(2):
            zb(p, way, way, 3).wait_recv()
            db(p, way, 7).start()

    def settle(p, step):
        these = (0,) if step == 0 else (2 * step - 1, 2 * step) if step < 4 else (7, 8)
        all_here(units(2 if 0 < step < 4 else 1), recv_ya.at[p, step])
        for i in these:
            da(p, 1, i).start()
        all_here(units(8 if 0 < step < 4 else 4), recv_d.at[p, step])
        products(p, these[0])

    def normal(a, j, h):
        c = a - lane_mean(a)
        r = lax.rsqrt(lane_mean(c * c) + epsilon)
        u = c * r
        unit[j, h] = u
        inv[j, h] = r
        return u.astype(BF16)

    ring_step(0, 0)
    turn(0, 2)
    yb(1).wait_recv()
    db(1, 1, 0).start()
    settle(0, 0)
    ring_step(0, 1)
    for who in range(2):
        for way in range(2):
            zb(1, who, way, 0).start()
    turn(2, 2)
    settle(0, 1)
    ring_step(0, 2)
    settle(0, 2)
    ring_step(1, 0)
    ring_last(0)
    turn(4, 2)
    settle(1, 0)
    settle(0, 3)
    ring_step(1, 1)
    settle(0, 4)
    for h in range(heads):
        at = slice(h * HD, (h + 1) * HD)
        kv[me, 0, h] = normal(nb[0, :, at], 1, h)
        kv[me, 1, h] = nb[1, :, at].astype(BF16)
    ring_step(1, 2)
    for j in range(2):
        for way in range(2):
            gather(way, 0, j).start()
    settle(1, 1)
    turn(6, 2)
    settle(1, 2)
    ring_last(1)
    for which in range(2):
        for k in range(3):
            transposed(k, which).start()
    settle(1, 3)
    settle(1, 4)
    for h in range(heads):
        at = slice(h * HD, (h + 1) * HD)
        q_low[h] = normal(nb[2, :, at], 0, h)
        do[h] = nb[3, :, at].astype(BF16)
        wsum[h] = jnp.zeros_like(wsum[h])
        tsum[h] = jnp.zeros_like(tsum[h])
        dq[h] = jnp.zeros_like(dq[h])

    def forward(b, h):
        k = kv[b, 0, h]
        v = kv[b, 1, h]
        e = jnp.exp(dot(q_low[h], k, LAST) * scale)
        ex[b, h] = e
        tsum[h] = tsum[h] + (e[:, :HD] + e[:, HD:])
        wsum[h] = wsum[h] + dot(e.astype(BF16), v)
        dp[b, h] = dot(do[h], v, LAST)

    def forward_blocks(ahead, behind):
        def step(i, c):
            b = lax.rem(me + ahead + (i // heads) * (behind - ahead), NZ)
            forward(b, lax.rem(i, heads))
            return c

        lax.fori_loop(0, heads if ahead == behind else 2 * heads, step, 0)

    forward_blocks(0, 0)
    for step in range(3):
        for j in range(2):
            for way in range(2):
                gather(way, step, j).wait_recv()
                if goes(way, step + 1, j):
                    gather(way, step + 1, j).start()
        forward_blocks(NZ - 1 - step, 1 + step)
    gather(0, 3, 0).wait_recv()
    gather(1, 3, 1).wait_recv()
    forward_blocks(4, 4)

    for h in range(heads):
        total = lane_sum(tsum[h])
        a = (wsum[h] / total).astype(BF16)
        act[0, quad, :, h * HD : (h + 1) * HD] = a
        rtot[h] = 1.0 / total
        delta[h] = lane_sum(do[h].astype(F32) * a.astype(F32))
    shared(0, 1).start()
    shared(0, 0).start()

    def backward(b, h):
        p = ex[b, h] * twice(rtot[h])
        ds = (p * (dp[b, h] - twice(delta[h])) * scale).astype(BF16)
        dq[h] = dq[h] + dot(ds, kv[b, 0, h])
        ex[b, h, :, :HD] = dot(ds, q_low[h], FIRST)
        ex[b, h, :, HD:] = dot(p.astype(BF16), do[h], FIRST)

    def backward_blocks(first, count):
        def step(i, c):
            n = first + i // heads
            away = (n + 1) // 2
            b = lax.rem(me + 4 + lax.rem(n, 2) * (NZ - 2 * away) + away, NZ)
            backward(b, lax.rem(i, heads))
            return c

        lax.fori_loop(0, count * heads, step, 0)

    def scatter_step(step):
        for j in range(2):
            for way in range(2):
                b = lax.rem(me + (4 - step if way == 0 else 4 + step), NZ)
                if step > 0:
                    scatter(way, step - 1, j).wait_recv()
                for h in range(heads):
                    for r in range(2):
                        if step == 0 and r != way:
                            continue
                        at = slice(r * half_block, (r + 1) * half_block)
                        val = ex[b, h, at, j * HD : (j + 1) * HD]
                        if step > 1 or step == 1 and r == way:
                            val = val + rbuf[way, step - 1, j, h, at].astype(F32)
                        sbuf[way, step, j, h, at] = val.astype(BF16)
                scatter(way, step, j).start()

    def relay(group):
        shared(group, 1).wait_recv()
        shared(group, 2).start()

    def back(val, j, h):
        u = unit[j, h]
        return (val - lane_mean(val) - u * lane_mean(val * u)) * inv[j, h]

    backward_blocks(0, 1)
    scatter_step(0)
    backward_blocks(1, 2)
    scatter_step(1)
    backward_blocks(3, 5)
    for h in range(heads):
        a = back(dq[h], 0, h).astype(BF16)
        act[1, quad, :, h * HD : (h + 1) * HD] = a
        low[:, h * HD : (h + 1) * HD] = a
    shared(1, 1).start()
    shared(1, 0).start()
    relay(0)
    scatter_step(2)
    relay(1)
    scatter_step(3)

    for which, there in enumerate((ut, ct)):
        all_here(there.at[0 : NQ - 1], recv_tr.at[which])
    for group in range(2):
        shared(group, 0).wait_recv()
        shared(group, 2).wait_recv()

    def weight_blocks(group):
        left = ct if group == 0 else ut
        tall = (left.shape[1] * left.shape[2], left.shape[3])
        for m in range(NQ):
            val = dot(left[m].reshape(tall), act[group, m])
            if m:
                val = val + dwp[group]
            dwp[group] = val

    own_rows = own_out.shape[0]

    def weight_part(z, group):
        return dwp[group, pl.ds(pl.multiple_of(z * own_rows, own_rows), own_rows), :]

    def weight_step(step, group):
        for way in range(2):
            if not goes(way, 3 - step, group):
                continue
            val = weight_part(lax.rem(me + (4 - step if way == 0 else 4 + step), NZ), group)
            if step > 0 and goes(way, 4 - step, group):
                weight_ring(way, step - 1, group).wait_recv()
                val = val + rdw[way, step - 1, group].astype(F32)
            sdw[way, step, group] = val.astype(BF16)
            weight_ring(way, step, group).start()

    for group in range(2):
        weight_blocks(group)
        weight_step(0, group)

    for j in range(2):
        for way in range(2):
            scatter(way, 3, j).wait_recv()
        for h in range(heads):
            val = ex[me, h, :, j * HD : (j + 1) * HD]
            val = val + rbuf[0, 3, j, h].astype(F32) + rbuf[1, 3, j, h].astype(F32)
            if j == 0:
                val = back(val, 1, h)
            a = val.astype(BF16)
            act[2 + j, quad, :, h * HD : (h + 1) * HD] = a
            low[:, (j + 1) * width + h * HD : (j + 1) * width + (h + 1) * HD] = a
        shared(2 + j, 1).start()
        shared(2 + j, 0).start()
    for group in range(2):
        weight_step(1, group)

    def inner(n, sums):
        x = lax.rem(xplace + 2 + n // 2, 4)
        t = 2 * x + lax.rem(n, 2)
        blocks = pl.ds(pl.multiple_of(t * NQ, NQ), NQ)
        a = jnp.zeros_like(nb[t])
        for j, (p, i) in enumerate(((1, 0), (0, 0), (0, 1))):
            left = low[:, j * width : (j + 1) * width]
            a = a + dot(left, g[p, i, blocks].reshape(width, width), LAST)
        nb[t] = a
        one, two = sums
        for k in range(heads):
            at = slice(k * HD, (k + 1) * HD)
            one = one + a[:, at]
            two = two + a[:, at] * ((tb[t, :, at].astype(F32) - norm[0]) * norm[1])
        return one, two

    def piece(x, half):
        return nb[2 * x + (1 - yhalf if half == 0 else yhalf)]

    def inner_step(step):
        for half in range(2):
            for way in range(2):
                if step == 0 and half != way:
                    continue
                x = lax.rem(xplace + (2 - step if way == 0 else 2 + step), 4)
                val = piece(x, half)
                if step > 0 and half == way:
                    xring(way, 0, half).wait_recv()
                    val = val + xr[way, 0, half].astype(F32)
                xs[way, step, half] = val.astype(BF16)
                xring(way, step, half).start()

    def arrived(half):
        for way in range(2):
            xring(way, 1, half).wait_recv()
        val = piece(xplace, half)
        return val + xr[0, 1, half].astype(F32) + xr[1, 1, half].astype(F32)

    zero = jnp.zeros((low.shape[0], HD), F32)
    sums = lax.fori_loop(0, 2, inner, (zero, zero))
    inner_step(0)
    sums = lax.fori_loop(2, 6, inner, sums)
    relay(2)
    sums = lax.fori_loop(6, NT, inner, sums)
    for i in range(2):
        stats[0, i * 8 : (i + 1) * 8, :] = jnp.transpose(lane_sum(sums[i]))[:8]
    for k in range(1, NT):
        stat(k).start()
    shared(2, 0).wait_recv()
    shared(2, 2).wait_recv()
    weight_blocks(2)
    weight_step(0, 2)
    relay(3)
    inner_step(1)
    for group in range(2):
        weight_step(2, group)
    shared(3, 0).wait_recv()
    shared(3, 2).wait_recv()
    weight_blocks(3)
    weight_step(0, 3)
    weight_step(1, 2)
    weight_step(1, 3)
    for group in range(2):
        weight_step(3, group)
    weight_step(2, 2)
    ysend[...] = arrived(0).astype(BF16)
    ypair().start()
    weight_step(2, 3)
    weight_step(3, 2)
    all_here(stats.at[0 : NT - 1], recv_st)
    total = stats[0]
    for k in range(1, NT):
        total = total + stats[k]
    row_mean = []
    for i in range(2):
        row = jnp.broadcast_to(total[i * 8 : i * 8 + 1, :], (HD, total.shape[1]))
        row_mean.append(jnp.transpose(row) / features)
    share = arrived(1)
    weight_step(3, 3)

    ypair().wait_recv()
    share = share + yrecv[...].astype(F32)
    for k in range(heads):
        at = slice(k * HD, (k + 1) * HD)
        own_unit = (tb[part, :, at].astype(F32) - norm[0]) * norm[1]
        val = share[:, at] - row_mean[0] - own_unit * row_mean[1]
        branch_out[:, at] = (val * norm[1]).astype(BF16)

    for group in range(4):
        val = weight_part(me, group)
        for way in range(2):
            weight_ring(way, 3, group).wait_recv()
            val = val + rdw[way, 3, group].astype(F32)
        if group == 0:
            out_out[...] = val
        else:
            qkv_out[group - 1] = val

    all_sent(g.at[:, :, 0 : NZ * NQ - 1], send_w)
    all_sent(kv.at[0 : NZ - 1], send_ag)
    all_sent(kv.at[0 : NZ - 1], send_rs)
    all_sent(units(28), send_dw)
    for which, here in enumerate((ut, ct)):
        all_sent(here.at[0 : NQ - 1], send_tr.at[which])
    all_sent(act.at[0:3], send_act)
    all_sent(act.at[0:3, 0:2], send_x)
    ypair().wait_send()
    all_sent(stats.at[0 : NT - 1], send_st)


def layer(tokens, cot, own_qkv, own_out):
    rows = tokens.shape[0]
    own, width = own_out.shape
    heads = width // HD
    vmem = pl.BlockSpec(memory_space=pltpu.VMEM)
    hbm = pl.BlockSpec(memory_space=pl.ANY)
    one = (heads, rows, HD)
    dma = pltpu.SemaphoreType.DMA
    return pl.pallas_call(
        lambda *refs: layer_kernel(heads, *refs),
        out_shape=(
            jax.ShapeDtypeStruct((3, own, width), F32),
            jax.ShapeDtypeStruct((own, width), F32),
            jax.ShapeDtypeStruct((rows, width), BF16),
        ),
        in_specs=[hbm] * 4,
        out_specs=(vmem, vmem, vmem),
        scratch_shapes=[
            pltpu.VMEM(one, BF16),
            pltpu.VMEM(one, BF16),
            pltpu.VMEM((2, *one), F32),
            pltpu.VMEM((2, *one), F32),
            pltpu.VMEM((NZ, 2, *one), BF16),
            pltpu.VMEM((NZ, heads, rows, rows), F32),
            pltpu.VMEM((NZ, heads, rows, rows), F32),
            pltpu.VMEM(one, F32),
            pltpu.VMEM(one, F32),
            pltpu.VMEM(one, F32),
            pltpu.VMEM(one, F32),
            pltpu.VMEM(one, F32),
            pltpu.VMEM((2, 4, 2, *one), BF16),
            pltpu.VMEM((2, 4, 2, *one), BF16),
            pltpu.VMEM((4, NQ, rows, width), BF16),
            pltpu.VMEM((rows, 3 * width), BF16),
            pltpu.VMEM((NQ, NZ, own, rows), BF16),
            pltpu.VMEM((NQ, NZ, own, rows), BF16),
            pltpu.VMEM((NZ, NQ, own, rows), BF16),
            pltpu.VMEM((NZ, NQ, own, rows), BF16),
            pltpu.VMEM((2, 2, NZ * NQ, own, width), BF16),
            pltpu.VMEM((NT, rows, width), BF16),
            pltpu.VMEM((NT, rows, width), F32),
            pltpu.VMEM((2, rows, HD), F32),
            pltpu.VMEM((2, 4, 4, own, width), BF16),
            pltpu.VMEM((2, 4, 4, own, width), BF16),
            pltpu.VMEM((4, NZ * own, width), F32),
            pltpu.VMEM((2, 2, 2, rows, width), BF16),
            pltpu.VMEM((2, 2, 2, rows, width), BF16),
            pltpu.VMEM((rows, width), BF16),
            pltpu.VMEM((rows, width), BF16),
            pltpu.VMEM((NT, 16, rows), F32),
            dma,
            dma((2, 4, 2)),
            dma,
            dma((2, 4, 2)),
            dma((2,)),
            dma((2,)),
            dma,
            dma((4, 3)),
            dma,
            dma((2, 4, 4)),
            dma,
            dma((2, 2, 2)),
            dma,
            dma,
            dma,
            dma,
            dma,
            dma((2, 2, 4)),
            dma((2, 2, 2, 4)),
            dma((2, 5)),
            dma((2,)),
            dma((2, 5)),
            dma,
            dma,
            dma,
        ],
        compiler_params=pltpu.CompilerParams(
            collective_id=0, has_side_effects=True, vmem_limit_bytes=67_043_328
        ),
    )(tokens, cot, own_qkv, own_out)


def finish(*arrays):
    def kernel(*refs):
        for i in range(len(arrays)):
            refs[len(arrays) + i][...] = refs[i][...]

    vmem = pl.BlockSpec(memory_space=pltpu.VMEM)
    return pl.pallas_call(
        kernel,
        out_shape=tuple(jax.ShapeDtypeStruct(a.shape, a.dtype) for a in arrays),
        in_specs=[vmem] * len(arrays),
        out_specs=(vmem,) * len(arrays),
    )(*arrays)


def local(tokens, cotangent, qkv_weight, out_weight):
    qkv_grad, out_grad, branch = finish(
        *layer(tokens[0], cotangent[0], jnp.transpose(qkv_weight, (1, 0, 2)), out_weight)
    )
    return (jnp.transpose(qkv_grad, (1, 0, 2)), out_grad, branch[None])


def solution(mesh):
    return jax.shard_map(
        local,
        mesh=mesh,
        in_specs=(
            P("dp", "seq", None),
            P("dp", "seq", None),
            P(("seq", "dp"), None, "tensor"),
            P(("seq", "dp"), "tensor"),
        ),
        out_specs=(
            P(("seq", "dp"), None, "tensor"),
            P(("seq", "dp"), "tensor"),
            P("dp", "seq", "tensor"),
        ),
        check_vma=False,
    )
```

```python
import jax
import jax.numpy as jnp
from jax import lax
from jax.experimental import pallas as pl
from jax.experimental.pallas import tpu as pltpu
from jax.sharding import PartitionSpec as P

HD = 128
NZ = 8
NT = 8
NQ = 4
MESH = pl.DeviceIdType.MESH
F32 = jnp.float32
BF16 = jnp.bfloat16
LAST = (((1,), (1,)), ((), ()))
FIRST = (((0,), (0,)), ((), ()))
epsilon = 1e-06


def dot(a, b, dims=(((1,), (0,)), ((), ()))):
    return lax.dot_general(a, b, dims, preferred_element_type=F32)


def twice(a):
    return jnp.concatenate([a, a], axis=1)


def lane_mean(a):
    return jnp.broadcast_to(jnp.mean(a, axis=1, keepdims=True), a.shape)


def lane_sum(a):
    return jnp.broadcast_to(jnp.sum(a, axis=1, keepdims=True), a.shape)


def layer_kernel(
    heads,
    tokens,
    cot,
    own_qkv,
    own_out,
    qkv_out,
    out_out,
    branch_out,
    q_low,
    do,
    unit,
    inv,
    kv,
    ex,
    dp,
    wsum,
    tsum,
    rtot,
    delta,
    dq,
    sbuf,
    rbuf,
    act,
    low,
    ut,
    ct,
    us,
    cs,
    g,
    tb,
    nb,
    norm,
    sdw,
    rdw,
    dwp,
    xs,
    xr,
    ysend,
    yrecv,
    stats,
    send_ag,
    recv_ag,
    send_rs,
    recv_rs,
    send_tr,
    recv_tr,
    send_act,
    recv_act,
    send_dw,
    recv_dw,
    send_x,
    recv_x,
    send_y,
    recv_y,
    send_st,
    recv_st,
    send_w,
    recv_za,
    recv_zb,
    recv_ya,
    recv_yb,
    recv_d,
    load_g,
    load_t,
    load_c,
):
    me = lax.axis_index("seq")
    quad = lax.axis_index("dp")
    part = lax.axis_index("tensor")
    sides = (lax.rem(me + 1, NZ), lax.rem(me + NZ - 1, NZ))
    mates = (quad + 1 - 2 * lax.rem(quad, 2), lax.rem(quad + 2, NQ), NQ - 1 - quad)
    xsides = (lax.rem(part + 2, NT), lax.rem(part + NT - 2, NT))
    ymate = part + 1 - 2 * lax.rem(part, 2)
    yhalf = lax.rem(part, 2)
    xplace = part // 2
    scale = HD ** (-0.5)
    width = heads * HD
    features = NT * width
    half_block = tokens.shape[0] // 2

    barrier = pltpu.get_barrier_semaphore()
    for side in sides:
        pl.semaphore_signal(barrier, inc=1, device_id={"seq": side}, device_id_type=MESH)
    for mate in mates:
        pl.semaphore_signal(barrier, inc=1, device_id={"dp": mate}, device_id_type=MESH)
    for k in range(1, NT):
        pl.semaphore_signal(
            barrier, inc=1, device_id={"tensor": lax.rem(part + k, NT)}, device_id_type=MESH
        )

    def remote(src, dst, send, recv, where):
        return pltpu.make_async_remote_copy(
            src_ref=src,
            dst_ref=dst,
            send_sem=send,
            recv_sem=recv,
            device_id=where,
            device_id_type=MESH,
        )

    def gather(way, step, j):
        b = lax.rem(me + (NZ - step if way == 0 else step), NZ)
        return remote(
            kv.at[b, j],
            kv.at[b, j],
            send_ag,
            recv_ag.at[way, step, j],
            {"seq": sides[way]},
        )

    def scatter(way, step, j):
        part_of = pl.ds(way * half_block, half_block) if step == 0 else pl.ds(0, 2 * half_block)
        return remote(
            sbuf.at[way, step, j, :, part_of],
            rbuf.at[way, step, j, :, part_of],
            send_rs,
            recv_rs.at[way, step, j],
            {"seq": sides[way]},
        )

    def weight_ring(way, step, group):
        return remote(
            sdw.at[way, step, group],
            rdw.at[way, step, group],
            send_dw,
            recv_dw.at[way, step, group],
            {"seq": sides[way]},
        )

    def transposed(k, which):
        src, dst = ((us, ut), (cs, ct))[which]
        return remote(
            src.at[:, mates[k]],
            dst.at[quad],
            send_tr.at[which],
            recv_tr.at[which],
            {"dp": mates[k]},
        )

    def shared(group, k):
        block = act.at[group, quad if k < 2 else mates[1]]
        return remote(
            block,
            block,
            send_act,
            recv_act.at[group, k],
            {"dp": mates[1] if k == 1 else mates[0]},
        )

    def xring(way, step, half):
        return remote(
            xs.at[way, step, half],
            xr.at[way, step, half],
            send_x,
            recv_x.at[way, step, half],
            {"tensor": xsides[way]},
        )

    def ypair():
        return remote(ysend, yrecv, send_y, recv_y, {"tensor": ymate})

    def stat(k):
        return remote(
            stats.at[0],
            stats.at[k],
            send_st,
            recv_st,
            {"tensor": lax.rem(part + k, NT)},
        )

    def goes(way, step, j):
        return step < 3 or j % 2 == way

    mine = me * NQ + quad
    load_own = [
        pltpu.make_async_copy(own_qkv.at[1], g.at[0, 0, mine], load_g),
        pltpu.make_async_copy(own_qkv.at[2], g.at[0, 1, mine], load_g),
        pltpu.make_async_copy(own_qkv.at[0], g.at[1, 0, mine], load_g),
        pltpu.make_async_copy(own_out, g.at[1, 1, mine], load_g),
    ]
    load_tokens = [
        pltpu.make_async_copy(tokens.at[:, z * width : (z + 1) * width], tb.at[z], load_t)
        for z in range(NZ)
    ]
    load_cot = [
        pltpu.make_async_copy(
            cot.at[:, (z * heads + h) * HD : (z * heads + h + 1) * HD],
            sbuf.at[z // 4, z % 4, 1, h],
            load_c,
        )
        for z in range(NZ)
        for h in range(heads)
    ]
    for c in load_own + load_tokens + load_cot:
        c.start()

    classes = (quad, mates[1])
    half_rows = own_out.shape[0] // 2

    def place(i):
        if i == 0:
            return me
        if i >= 7:
            return lax.rem(me + 4, NZ)
        step, way = (i - 1) // 2, (i - 1) % 2
        return lax.rem(me + (NZ - 1 - step if way == 0 else 1 + step), NZ)

    def first_array(p, i, who):
        b = place(i) * NQ + classes[who]
        if i >= 7:
            return g.at[p, 0, b, (i - 7) * half_rows : (i - 6) * half_rows]
        return g.at[p, 0, b]

    def second_array(p, i, who):
        return g.at[p, 1, place(i) * NQ + classes[who]]

    def stage(i):
        return 4 if i >= 7 else (i + 1) // 2

    def index(way, step):
        return 0 if step == 0 else 1 + 2 * (step - 1) + way

    def same(block, send, recv, where):
        return remote(block, block, send, recv, where)

    def za(p, way, step):
        return same(
            g.at[p, 0, lax.rem(me + (NZ - step if way == 0 else step), NZ) * NQ + quad]
            if step < 3
            else g.at[
                p,
                0,
                lax.rem(me + (NZ - step if way == 0 else step), NZ) * NQ + quad,
                way * half_rows : (way + 1) * half_rows,
            ],
            send_w,
            recv_za.at[p, way, step],
            {"seq": sides[way]},
        )

    def zb(p, who, way, step):
        z = lax.rem(me + (NZ - step if way == 0 else step), NZ)
        return same(
            g.at[p, 1, z * NQ + classes[who]],
            send_w,
            recv_zb.at[p, who, way, step],
            {"seq": sides[way]},
        )

    def ya(p, i):
        return same(
            first_array(p, i, 0), send_w, recv_ya.at[p, stage(i)], {"dp": mates[1]}
        )

    def yb(p):
        return same(second_array(p, 0, 0), send_w, recv_yb.at[p], {"dp": mates[1]})

    def da(p, who, i):
        return same(
            first_array(p, i, who),
            send_w,
            recv_d.at[p, stage(i)],
            {"dp": mates[0]},
        )

    def db(p, who, i):
        return same(
            second_array(p, i, who),
            send_w,
            recv_d.at[p, stage(i)],
            {"dp": mates[0]},
        )

    def whole(ref, sem):
        return pltpu.make_async_copy(ref, ref, sem)

    def units(n):
        return g.at[0, 0, 0:n]

    def all_sent(ref, sem):
        remote(ref, ref, sem, sem, {"seq": sides[0]}).wait_send()

    def all_here(ref, sem):
        remote(ref, ref, sem, sem, {"seq": sides[0]}).wait_recv()

    whole(units(4), load_g).wait()
    pl.semaphore_wait(barrier, 2 + 3 + NT - 1)
    for way in range(2):
        za(0, way, 0).start()
    for p in range(2):
        yb(p).start()
    for way in range(2):
        zb(0, 0, way, 0).start()
    for p in range(2):
        ya(p, 0).start()
    for way in range(2):
        za(1, way, 0).start()
    for p in range(2):
        da(p, 0, 0).start()
        db(p, 0, 0).start()

    rows = tb.shape[1]
    blank = jnp.zeros((rows, HD), F32)
    whole(tb, load_t).wait()

    def fold(a):
        s = a[:, :HD]
        for k in range(1, heads):
            s = s + a[:, k * HD : (k + 1) * HD]
        return s

    def wide(a):
        return jnp.concatenate([a] * heads, axis=1)

    def add_sum(z, s):
        return s + fold(tb[z].astype(F32))

    average = lane_sum(lax.fori_loop(0, NZ, add_sum, blank)) / features

    def add_square(z, s):
        c = tb[z].astype(F32) - wide(average)
        return s + fold(c * c)

    norm[0] = average
    norm[1] = lax.rsqrt(lane_sum(lax.fori_loop(0, NZ, add_square, blank)) / features + epsilon)

    yb(0).wait_recv()
    for way in range(2):
        zb(0, 1, way, 0).start()
    db(0, 1, 0).start()

    def lower(z, c):
        for h in range(heads):
            a = tb[z, :, h * HD : (h + 1) * HD].astype(F32)
            sbuf[z // 4, lax.rem(z, 4), 0, h] = ((a - norm[0]) * norm[1]).astype(BF16)
        return c

    lax.fori_loop(0, NZ, lower, 0)
    for i in range(4):
        nb[i] = jnp.zeros_like(nb[i])
    whole(sbuf.at[:, :, 1], load_c).wait()

    def low_rows(z, which):
        return jnp.concatenate(
            [sbuf[z // 4, lax.rem(z, 4), which, h] for h in range(heads)], axis=1
        )

    def turn(first, count):
        def step(z, c):
            for which, (dst, kept) in enumerate(((us, ut), (cs, ct))):
                dst[z] = jnp.transpose(low_rows(z, which)).reshape(dst.shape[1:])
                kept[quad, z] = dst[z, quad]
            return c

        lax.fori_loop(first, first + count, step, 0)

    def products(p, i):
        def one(z):
            blocks = pl.ds(pl.multiple_of(z * NQ, NQ), NQ)
            for j in range(2):
                left = low_rows(z, 1 if p + j == 2 else 0)
                nb[2 * p + j] = nb[2 * p + j] + dot(left, g[p, j, blocks].reshape(width, width))

        if i == 0 or i >= 7:
            one(place(i))
        else:

            def step(n, c):
                d = (i + 1) // 2
                one(lax.rem(me + NZ - d + 2 * d * n, NZ))
                return c

            lax.fori_loop(0, 2, step, 0)

    def ring_step(p, step):
        for way in range(2):
            i = index(way, step + 1)
            za(p, way, step).wait_recv()
            za(p, way, step + 1).start()
            ya(p, i).start()
            da(p, 0, i).start()
        for who in range(2):
            for way in range(2):
                zb(p, who, way, step).wait_recv()
                if step < 2 or who == way:
                    zb(p, who, way, step + 1).start()
                db(p, who, index(way, step + 1)).start()

    def ring_last(p):
        for way in range(2):
            za(p, way, 3).wait_recv()
            ya(p, 7 + way).start()
            da(p, 0, 7 + way).start()
        for way in range(2):
            zb(p, way, way, 3).wait_recv()
            db(p, way, 7).start()

    def settle(p, step):
        these = (0,) if step == 0 else (2 * step - 1, 2 * step) if step < 4 else (7, 8)
        all_here(units(2 if 0 < step < 4 else 1), recv_ya.at[p, step])
        for i in these:
            da(p, 1, i).start()
        all_here(units(8 if 0 < step < 4 else 4), recv_d.at[p, step])
        products(p, these[0])

    def normal(a, j, h):
        c = a - lane_mean(a)
        r = lax.rsqrt(lane_mean(c * c) + epsilon)
        u = c * r
        unit[j, h] = u
        inv[j, h] = r
        return u.astype(BF16)

    ring_step(0, 0)
    turn(0, 2)
    yb(1).wait_recv()
    db(1, 1, 0).start()
    settle(0, 0)
    ring_step(0, 1)
    for who in range(2):
        for way in range(2):
            zb(1, who, way, 0).start()
    turn(2, 2)
    settle(0, 1)
    ring_step(0, 2)
    settle(0, 2)
    ring_step(1, 0)
    ring_last(0)
    turn(4, 2)
    settle(1, 0)
    ring_step(1, 1)
    settle(0, 3)
    settle(0, 4)
    for h in range(heads):
        at = slice(h * HD, (h + 1) * HD)
        kv[me, 0, h] = normal(nb[0, :, at], 1, h)
        kv[me, 1, h] = nb[1, :, at].astype(BF16)
    for way in range(2):
        gather(way, 0, 0).start()
    ring_step(1, 2)
    for way in range(2):
        gather(way, 0, 1).start()
    settle(1, 1)
    turn(6, 2)
    settle(1, 2)
    ring_last(1)
    for which in range(2):
        for k in range(3):
            transposed(k, which).start()
    for way in range(2):
        gather(way, 0, 0).wait_recv()
        gather(way, 1, 0).start()
    settle(1, 3)
    settle(1, 4)
    for h in range(heads):
        at = slice(h * HD, (h + 1) * HD)
        q_low[h] = normal(nb[2, :, at], 0, h)
        do[h] = nb[3, :, at].astype(BF16)
        wsum[h] = jnp.zeros_like(wsum[h])
        tsum[h] = jnp.zeros_like(tsum[h])
        dq[h] = jnp.zeros_like(dq[h])

    def forward(b, h):
        k = kv[b, 0, h]
        v = kv[b, 1, h]
        e = jnp.exp(dot(q_low[h], k, LAST) * scale)
        ex[b, h] = e
        tsum[h] = tsum[h] + (e[:, :HD] + e[:, HD:])
        wsum[h] = wsum[h] + dot(e.astype(BF16), v)
        dp[b, h] = dot(do[h], v, LAST)

    def forward_blocks(ahead, behind):
        def step(i, c):
            b = lax.rem(me + ahead + (i // heads) * (behind - ahead), NZ)
            forward(b, lax.rem(i, heads))
            return c

        lax.fori_loop(0, heads if ahead == behind else 2 * heads, step, 0)

    forward_blocks(0, 0)
    for step in range(3):
        for j in range(2):
            for way in range(2):
                if step == 0 and j == 0:
                    continue
                gather(way, step, j).wait_recv()
                if goes(way, step + 1, j):
                    gather(way, step + 1, j).start()
        forward_blocks(NZ - 1 - step, 1 + step)
    gather(0, 3, 0).wait_recv()
    gather(1, 3, 1).wait_recv()
    forward_blocks(4, 4)

    for h in range(heads):
        total = lane_sum(tsum[h])
        a = (wsum[h] / total).astype(BF16)
        act[0, quad, :, h * HD : (h + 1) * HD] = a
        rtot[h] = 1.0 / total
        delta[h] = lane_sum(do[h].astype(F32) * a.astype(F32))
    shared(0, 1).start()
    shared(0, 0).start()

    def backward(b, h):
        p = ex[b, h] * twice(rtot[h])
        ds = (p * (dp[b, h] - twice(delta[h])) * scale).astype(BF16)
        dq[h] = dq[h] + dot(ds, kv[b, 0, h])
        ex[b, h, :, :HD] = dot(ds, q_low[h], FIRST)
        ex[b, h, :, HD:] = dot(p.astype(BF16), do[h], FIRST)

    def backward_blocks(first, count):
        def step(i, c):
            n = first + i // heads
            away = (n + 1) // 2
            b = lax.rem(me + 4 + lax.rem(n, 2) * (NZ - 2 * away) + away, NZ)
            backward(b, lax.rem(i, heads))
            return c

        lax.fori_loop(0, count * heads, step, 0)

    def scatter_step(step):
        for j in range(2):
            for way in range(2):
                b = lax.rem(me + (4 - step if way == 0 else 4 + step), NZ)
                if step > 0:
                    scatter(way, step - 1, j).wait_recv()
                for h in range(heads):
                    for r in range(2):
                        if step == 0 and r != way:
                            continue
                        at = slice(r * half_block, (r + 1) * half_block)
                        val = ex[b, h, at, j * HD : (j + 1) * HD]
                        if step > 1 or step == 1 and r == way:
                            val = val + rbuf[way, step - 1, j, h, at].astype(F32)
                        sbuf[way, step, j, h, at] = val.astype(BF16)
                scatter(way, step, j).start()

    def relay(group):
        shared(group, 1).wait_recv()
        shared(group, 2).start()

    def back(val, j, h):
        u = unit[j, h]
        return (val - lane_mean(val) - u * lane_mean(val * u)) * inv[j, h]

    backward_blocks(0, 1)
    scatter_step(0)
    backward_blocks(1, 2)
    scatter_step(1)
    backward_blocks(3, 5)
    for h in range(heads):
        a = back(dq[h], 0, h).astype(BF16)
        act[1, quad, :, h * HD : (h + 1) * HD] = a
        low[:, h * HD : (h + 1) * HD] = a
    shared(1, 1).start()
    shared(1, 0).start()
    relay(0)
    scatter_step(2)
    relay(1)

    for which, there in enumerate((ut, ct)):
        all_here(there.at[0 : NQ - 1], recv_tr.at[which])
    for group in range(2):
        shared(group, 0).wait_recv()
        shared(group, 2).wait_recv()

    def weight_blocks(group):
        left = ct if group == 0 else ut
        tall = (left.shape[1] * left.shape[2], left.shape[3])
        for m in range(NQ):
            val = dot(left[m].reshape(tall), act[group, m])
            if m:
                val = val + dwp[group]
            dwp[group] = val

    own_rows = own_out.shape[0]

    def weight_part(z, group):
        return dwp[group, pl.ds(pl.multiple_of(z * own_rows, own_rows), own_rows), :]

    def weight_step(step, group):
        for way in range(2):
            if not goes(way, 3 - step, group):
                continue
            val = weight_part(lax.rem(me + (4 - step if way == 0 else 4 + step), NZ), group)
            if step > 0 and goes(way, 4 - step, group):
                weight_ring(way, step - 1, group).wait_recv()
                val = val + rdw[way, step - 1, group].astype(F32)
            sdw[way, step, group] = val.astype(BF16)
            weight_ring(way, step, group).start()

    def early_ring(way, step):
        both = slice(0, 2)
        return remote(
            sdw.at[way, step, both],
            rdw.at[way, step, both],
            send_dw,
            recv_dw.at[way, step, 0],
            {"seq": sides[way]},
        )

    def early_step(step):
        for way in range(2):
            if step == 1:
                weight_ring(way, 0, way).wait_recv()
            else:
                early_ring(way, step - 1).wait_recv()
            z = lax.rem(me + (4 - step if way == 0 else 4 + step), NZ)
            for group in range(2):
                val = weight_part(z, group)
                if step > 1 or group == way:
                    val = val + rdw[way, step - 1, group].astype(F32)
                sdw[way, step, group] = val.astype(BF16)
            early_ring(way, step).start()

    for group in range(2):
        weight_blocks(group)
        weight_step(0, group)
    scatter_step(3)
    early_step(1)

    for j in range(2):
        for way in range(2):
            scatter(way, 3, j).wait_recv()
        for h in range(heads):
            val = ex[me, h, :, j * HD : (j + 1) * HD]
            val = val + rbuf[0, 3, j, h].astype(F32) + rbuf[1, 3, j, h].astype(F32)
            if j == 0:
                val = back(val, 1, h)
            a = val.astype(BF16)
            act[2 + j, quad, :, h * HD : (h + 1) * HD] = a
            low[:, (j + 1) * width + h * HD : (j + 1) * width + (h + 1) * HD] = a
        shared(2 + j, 1).start()
        shared(2 + j, 0).start()

    def inner(n, sums):
        x = lax.rem(xplace + 2 + n // 2, 4)
        t = 2 * x + lax.rem(n, 2)
        blocks = pl.ds(pl.multiple_of(t * NQ, NQ), NQ)
        a = jnp.zeros_like(nb[t])
        for j, (p, i) in enumerate(((1, 0), (0, 0), (0, 1))):
            left = low[:, j * width : (j + 1) * width]
            a = a + dot(left, g[p, i, blocks].reshape(width, width), LAST)
        nb[t] = a
        one, two = sums
        for k in range(heads):
            at = slice(k * HD, (k + 1) * HD)
            one = one + a[:, at]
            two = two + a[:, at] * ((tb[t, :, at].astype(F32) - norm[0]) * norm[1])
        return one, two

    def piece(x, half):
        return nb[2 * x + (1 - yhalf if half == 0 else yhalf)]

    def inner_step(step):
        for half in range(2):
            for way in range(2):
                if step == 0 and half != way:
                    continue
                x = lax.rem(xplace + (2 - step if way == 0 else 2 + step), 4)
                val = piece(x, half)
                if step > 0 and half == way:
                    xring(way, 0, half).wait_recv()
                    val = val + xr[way, 0, half].astype(F32)
                xs[way, step, half] = val.astype(BF16)
                xring(way, step, half).start()

    def arrived(half):
        for way in range(2):
            xring(way, 1, half).wait_recv()
        val = piece(xplace, half)
        return val + xr[0, 1, half].astype(F32) + xr[1, 1, half].astype(F32)

    zero = jnp.zeros((low.shape[0], HD), F32)
    sums = lax.fori_loop(0, 2, inner, (zero, zero))
    inner_step(0)
    relay(2)
    early_step(2)
    sums = lax.fori_loop(2, 4, inner, sums)
    shared(2, 0).wait_recv()
    shared(2, 2).wait_recv()
    weight_blocks(2)
    weight_step(0, 2)
    sums = lax.fori_loop(4, 6, inner, sums)
    relay(3)
    sums = lax.fori_loop(6, NT, inner, sums)
    for i in range(2):
        stats[0, i * 8 : (i + 1) * 8, :] = jnp.transpose(lane_sum(sums[i]))[:8]
    for k in range(1, NT):
        stat(k).start()
    inner_step(1)
    shared(3, 0).wait_recv()
    shared(3, 2).wait_recv()
    weight_blocks(3)
    weight_step(0, 3)
    weight_step(1, 2)
    early_step(3)
    weight_step(1, 3)
    weight_step(2, 2)
    ysend[...] = arrived(0).astype(BF16)
    ypair().start()
    weight_step(2, 3)
    weight_step(3, 2)
    all_here(stats.at[0 : NT - 1], recv_st)
    total = stats[0]
    for k in range(1, NT):
        total = total + stats[k]
    row_mean = []
    for i in range(2):
        row = jnp.broadcast_to(total[i * 8 : i * 8 + 1, :], (HD, total.shape[1]))
        row_mean.append(jnp.transpose(row) / features)
    share = arrived(1)
    weight_step(3, 3)

    ypair().wait_recv()
    share = share + yrecv[...].astype(F32)
    for k in range(heads):
        at = slice(k * HD, (k + 1) * HD)
        own_unit = (tb[part, :, at].astype(F32) - norm[0]) * norm[1]
        val = share[:, at] - row_mean[0] - own_unit * row_mean[1]
        branch_out[:, at] = (val * norm[1]).astype(BF16)

    for group in range(4):
        val = weight_part(me, group)
        for way in range(2):
            if group > 1:
                weight_ring(way, 3, group).wait_recv()
            elif group == 0:
                early_ring(way, 3).wait_recv()
            val = val + rdw[way, 3, group].astype(F32)
        if group == 0:
            out_out[...] = val
        else:
            qkv_out[group - 1] = val

    all_sent(g.at[:, :, 0 : NZ * NQ - 1], send_w)
    all_sent(kv.at[0 : NZ - 1], send_ag)
    all_sent(kv.at[0 : NZ - 1], send_rs)
    all_sent(units(28), send_dw)
    for which, here in enumerate((ut, ct)):
        all_sent(here.at[0 : NQ - 1], send_tr.at[which])
    all_sent(act.at[0:3], send_act)
    all_sent(act.at[0:3, 0:2], send_x)
    ypair().wait_send()
    all_sent(stats.at[0 : NT - 1], send_st)


def layer(tokens, cot, own_qkv, own_out):
    rows = tokens.shape[0]
    own, width = own_out.shape
    heads = width // HD
    vmem = pl.BlockSpec(memory_space=pltpu.VMEM)
    hbm = pl.BlockSpec(memory_space=pl.ANY)
    one = (heads, rows, HD)
    dma = pltpu.SemaphoreType.DMA
    return pl.pallas_call(
        lambda *refs: layer_kernel(heads, *refs),
        out_shape=(
            jax.ShapeDtypeStruct((3, own, width), F32),
            jax.ShapeDtypeStruct((own, width), F32),
            jax.ShapeDtypeStruct((rows, width), BF16),
        ),
        in_specs=[hbm] * 4,
        out_specs=(vmem, vmem, vmem),
        scratch_shapes=[
            pltpu.VMEM(one, BF16),
            pltpu.VMEM(one, BF16),
            pltpu.VMEM((2, *one), F32),
            pltpu.VMEM((2, *one), F32),
            pltpu.VMEM((NZ, 2, *one), BF16),
            pltpu.VMEM((NZ, heads, rows, rows), F32),
            pltpu.VMEM((NZ, heads, rows, rows), F32),
            pltpu.VMEM(one, F32),
            pltpu.VMEM(one, F32),
            pltpu.VMEM(one, F32),
            pltpu.VMEM(one, F32),
            pltpu.VMEM(one, F32),
            pltpu.VMEM((2, 4, 2, *one), BF16),
            pltpu.VMEM((2, 4, 2, *one), BF16),
            pltpu.VMEM((4, NQ, rows, width), BF16),
            pltpu.VMEM((rows, 3 * width), BF16),
            pltpu.VMEM((NQ, NZ, own, rows), BF16),
            pltpu.VMEM((NQ, NZ, own, rows), BF16),
            pltpu.VMEM((NZ, NQ, own, rows), BF16),
            pltpu.VMEM((NZ, NQ, own, rows), BF16),
            pltpu.VMEM((2, 2, NZ * NQ, own, width), BF16),
            pltpu.VMEM((NT, rows, width), BF16),
            pltpu.VMEM((NT, rows, width), F32),
            pltpu.VMEM((2, rows, HD), F32),
            pltpu.VMEM((2, 4, 4, own, width), BF16),
            pltpu.VMEM((2, 4, 4, own, width), BF16),
            pltpu.VMEM((4, NZ * own, width), F32),
            pltpu.VMEM((2, 2, 2, rows, width), BF16),
            pltpu.VMEM((2, 2, 2, rows, width), BF16),
            pltpu.VMEM((rows, width), BF16),
            pltpu.VMEM((rows, width), BF16),
            pltpu.VMEM((NT, 16, rows), F32),
            dma,
            dma((2, 4, 2)),
            dma,
            dma((2, 4, 2)),
            dma((2,)),
            dma((2,)),
            dma,
            dma((4, 3)),
            dma,
            dma((2, 4, 4)),
            dma,
            dma((2, 2, 2)),
            dma,
            dma,
            dma,
            dma,
            dma,
            dma((2, 2, 4)),
            dma((2, 2, 2, 4)),
            dma((2, 5)),
            dma((2,)),
            dma((2, 5)),
            dma,
            dma,
            dma,
        ],
        compiler_params=pltpu.CompilerParams(
            collective_id=0, has_side_effects=True, vmem_limit_bytes=67_043_328
        ),
    )(tokens, cot, own_qkv, own_out)


def finish(*arrays):
    def kernel(*refs):
        for i in range(len(arrays)):
            refs[len(arrays) + i][...] = refs[i][...]

    vmem = pl.BlockSpec(memory_space=pltpu.VMEM)
    return pl.pallas_call(
        kernel,
        out_shape=tuple(jax.ShapeDtypeStruct(a.shape, a.dtype) for a in arrays),
        in_specs=[vmem] * len(arrays),
        out_specs=(vmem,) * len(arrays),
    )(*arrays)


def local(tokens, cotangent, qkv_weight, out_weight):
    qkv_grad, out_grad, branch = finish(
        *layer(tokens[0], cotangent[0], jnp.transpose(qkv_weight, (1, 0, 2)), out_weight)
    )
    return (jnp.transpose(qkv_grad, (1, 0, 2)), out_grad, branch[None])


def solution(mesh):
    return jax.shard_map(
        local,
        mesh=mesh,
        in_specs=(
            P("dp", "seq", None),
            P("dp", "seq", None),
            P(("seq", "dp"), None, "tensor"),
            P(("seq", "dp"), "tensor"),
        ),
        out_specs=(
            P(("seq", "dp"), None, "tensor"),
            P(("seq", "dp"), "tensor"),
            P("dp", "seq", "tensor"),
        ),
        check_vma=False,
    )
```

```python
import jax
import jax.numpy as jnp
from jax import lax
from jax.experimental import pallas as pl
from jax.experimental.pallas import tpu as pltpu
from jax.sharding import PartitionSpec as P

HD = 128
NZ = 8
NT = 8
NQ = 4
MESH = pl.DeviceIdType.MESH
F32 = jnp.float32
BF16 = jnp.bfloat16
LAST = (((1,), (1,)), ((), ()))
FIRST = (((0,), (0,)), ((), ()))
epsilon = 1e-06


def dot(a, b, dims=(((1,), (0,)), ((), ()))):
    return lax.dot_general(a, b, dims, preferred_element_type=F32)


def twice(a):
    return jnp.concatenate([a, a], axis=1)


def lane_mean(a):
    return jnp.broadcast_to(jnp.mean(a, axis=1, keepdims=True), a.shape)


def lane_sum(a):
    return jnp.broadcast_to(jnp.sum(a, axis=1, keepdims=True), a.shape)


def layer_kernel(
    heads,
    tokens,
    cot,
    own_qkv,
    own_out,
    qkv_out,
    out_out,
    branch_out,
    q_low,
    do,
    unit,
    inv,
    kv,
    ex,
    dp,
    wsum,
    tsum,
    rtot,
    delta,
    dq,
    sbuf,
    rbuf,
    act,
    low,
    ut,
    ct,
    us,
    cs,
    g,
    tb,
    nb,
    norm,
    sdw,
    rdw,
    dwp,
    xs,
    xr,
    ysend,
    yrecv,
    stats,
    send_ag,
    recv_ag,
    send_rs,
    recv_rs,
    send_tr,
    recv_tr,
    send_act,
    recv_act,
    send_dw,
    recv_dw,
    send_x,
    recv_x,
    send_y,
    recv_y,
    send_st,
    recv_st,
    send_w,
    recv_za,
    recv_zb,
    recv_ya,
    recv_yb,
    recv_d,
    load_g,
    load_t,
    load_c,
):
    me = lax.axis_index("seq")
    quad = lax.axis_index("dp")
    part = lax.axis_index("tensor")
    sides = (lax.rem(me + 1, NZ), lax.rem(me + NZ - 1, NZ))
    mates = (quad + 1 - 2 * lax.rem(quad, 2), lax.rem(quad + 2, NQ), NQ - 1 - quad)
    xsides = (lax.rem(part + 2, NT), lax.rem(part + NT - 2, NT))
    ymate = part + 1 - 2 * lax.rem(part, 2)
    yhalf = lax.rem(part, 2)
    xplace = part // 2
    scale = HD ** (-0.5)
    width = heads * HD
    features = NT * width
    half_block = tokens.shape[0] // 2

    barrier = pltpu.get_barrier_semaphore()
    for side in sides:
        pl.semaphore_signal(barrier, inc=1, device_id={"seq": side}, device_id_type=MESH)
    for mate in mates:
        pl.semaphore_signal(barrier, inc=1, device_id={"dp": mate}, device_id_type=MESH)
    for k in range(1, NT):
        pl.semaphore_signal(
            barrier, inc=1, device_id={"tensor": lax.rem(part + k, NT)}, device_id_type=MESH
        )

    def remote(src, dst, send, recv, where):
        return pltpu.make_async_remote_copy(
            src_ref=src,
            dst_ref=dst,
            send_sem=send,
            recv_sem=recv,
            device_id=where,
            device_id_type=MESH,
        )

    def gather(way, step, j):
        b = lax.rem(me + (NZ - step if way == 0 else step), NZ)
        return remote(
            kv.at[b, j],
            kv.at[b, j],
            send_ag,
            recv_ag.at[way, step, j],
            {"seq": sides[way]},
        )

    def scatter(way, step, j):
        part_of = pl.ds(way * half_block, half_block) if step == 0 else pl.ds(0, 2 * half_block)
        return remote(
            sbuf.at[way, step, j, :, part_of],
            rbuf.at[way, step, j, :, part_of],
            send_rs,
            recv_rs.at[way, step, j],
            {"seq": sides[way]},
        )

    def weight_ring(way, step, group):
        return remote(
            sdw.at[way, step, group],
            rdw.at[way, step, group],
            send_dw,
            recv_dw.at[way, step, group],
            {"seq": sides[way]},
        )

    def transposed(k, which):
        src, dst = ((us, ut), (cs, ct))[which]
        return remote(
            src.at[:, mates[k]],
            dst.at[quad],
            send_tr.at[which],
            recv_tr.at[which],
            {"dp": mates[k]},
        )

    def shared(group, k):
        block = act.at[group, quad if k < 2 else mates[1]]
        return remote(
            block,
            block,
            send_act,
            recv_act.at[group, k],
            {"dp": mates[1] if k == 1 else mates[0]},
        )

    def xring(way, step, half):
        return remote(
            xs.at[way, step, half],
            xr.at[way, step, half],
            send_x,
            recv_x.at[way, step, half],
            {"tensor": xsides[way]},
        )

    def ypair():
        return remote(ysend, yrecv, send_y, recv_y, {"tensor": ymate})

    def stat(k):
        return remote(
            stats.at[0],
            stats.at[k],
            send_st,
            recv_st,
            {"tensor": lax.rem(part + k, NT)},
        )

    def goes(way, step, j):
        return step < 3 or j % 2 == way

    mine = me * NQ + quad
    load_own = [
        pltpu.make_async_copy(own_qkv.at[1], g.at[0, 0, mine], load_g),
        pltpu.make_async_copy(own_qkv.at[2], g.at[0, 1, mine], load_g),
        pltpu.make_async_copy(own_qkv.at[0], g.at[1, 0, mine], load_g),
        pltpu.make_async_copy(own_out, g.at[1, 1, mine], load_g),
    ]
    load_tokens = [
        pltpu.make_async_copy(tokens.at[:, z * width : (z + 1) * width], tb.at[z], load_t)
        for z in range(NZ)
    ]
    load_cot = [
        pltpu.make_async_copy(
            cot.at[:, (z * heads + h) * HD : (z * heads + h + 1) * HD],
            sbuf.at[z // 4, z % 4, 1, h],
            load_c,
        )
        for z in range(NZ)
        for h in range(heads)
    ]
    for c in load_own + load_tokens + load_cot:
        c.start()

    classes = (quad, mates[1])
    half_rows = own_out.shape[0] // 2

    def place(i):
        if i == 0:
            return me
        if i >= 7:
            return lax.rem(me + 4, NZ)
        step, way = (i - 1) // 2, (i - 1) % 2
        return lax.rem(me + (NZ - 1 - step if way == 0 else 1 + step), NZ)

    def first_array(p, i, who):
        b = place(i) * NQ + classes[who]
        if i >= 7:
            return g.at[p, 0, b, (i - 7) * half_rows : (i - 6) * half_rows]
        return g.at[p, 0, b]

    def second_array(p, i, who):
        return g.at[p, 1, place(i) * NQ + classes[who]]

    def stage(i):
        return 4 if i >= 7 else (i + 1) // 2

    def index(way, step):
        return 0 if step == 0 else 1 + 2 * (step - 1) + way

    def same(block, send, recv, where):
        return remote(block, block, send, recv, where)

    def za(p, way, step):
        return same(
            g.at[p, 0, lax.rem(me + (NZ - step if way == 0 else step), NZ) * NQ + quad]
            if step < 3
            else g.at[
                p,
                0,
                lax.rem(me + (NZ - step if way == 0 else step), NZ) * NQ + quad,
                way * half_rows : (way + 1) * half_rows,
            ],
            send_w,
            recv_za.at[p, way, step],
            {"seq": sides[way]},
        )

    def zb(p, who, way, step):
        z = lax.rem(me + (NZ - step if way == 0 else step), NZ)
        return same(
            g.at[p, 1, z * NQ + classes[who]],
            send_w,
            recv_zb.at[p, who, way, step],
            {"seq": sides[way]},
        )

    def ya(p, i):
        return same(
            first_array(p, i, 0), send_w, recv_ya.at[p, stage(i)], {"dp": mates[1]}
        )

    def yb(p):
        return same(second_array(p, 0, 0), send_w, recv_yb.at[p], {"dp": mates[1]})

    def da(p, who, i):
        return same(
            first_array(p, i, who),
            send_w,
            recv_d.at[p, stage(i)],
            {"dp": mates[0]},
        )

    def db(p, who, i):
        return same(
            second_array(p, i, who),
            send_w,
            recv_d.at[p, stage(i)],
            {"dp": mates[0]},
        )

    def whole(ref, sem):
        return pltpu.make_async_copy(ref, ref, sem)

    def units(n):
        return g.at[0, 0, 0:n]

    def all_sent(ref, sem):
        remote(ref, ref, sem, sem, {"seq": sides[0]}).wait_send()

    def all_here(ref, sem):
        remote(ref, ref, sem, sem, {"seq": sides[0]}).wait_recv()

    whole(units(4), load_g).wait()
    pl.semaphore_wait(barrier, 2 + 3 + NT - 1)
    for way in range(2):
        za(0, way, 0).start()
    for p in range(2):
        yb(p).start()
    for way in range(2):
        zb(0, 0, way, 0).start()
    for p in range(2):
        ya(p, 0).start()
    for way in range(2):
        za(1, way, 0).start()
    for p in range(2):
        da(p, 0, 0).start()
        db(p, 0, 0).start()

    rows = tb.shape[1]
    blank = jnp.zeros((rows, HD), F32)
    whole(tb, load_t).wait()

    def fold(a):
        s = a[:, :HD]
        for k in range(1, heads):
            s = s + a[:, k * HD : (k + 1) * HD]
        return s

    def wide(a):
        return jnp.concatenate([a] * heads, axis=1)

    def add_sum(z, s):
        return s + fold(tb[z].astype(F32))

    average = lane_sum(lax.fori_loop(0, NZ, add_sum, blank)) / features

    def add_square(z, s):
        c = tb[z].astype(F32) - wide(average)
        return s + fold(c * c)

    norm[0] = average
    norm[1] = lax.rsqrt(lane_sum(lax.fori_loop(0, NZ, add_square, blank)) / features + epsilon)

    yb(0).wait_recv()
    for way in range(2):
        zb(0, 1, way, 0).start()
    db(0, 1, 0).start()

    def lower(z, c):
        for h in range(heads):
            a = tb[z, :, h * HD : (h + 1) * HD].astype(F32)
            sbuf[z // 4, lax.rem(z, 4), 0, h] = ((a - norm[0]) * norm[1]).astype(BF16)
        return c

    lax.fori_loop(0, NZ, lower, 0)
    for i in range(4):
        nb[i] = jnp.zeros_like(nb[i])
    whole(sbuf.at[:, :, 1], load_c).wait()

    def low_rows(z, which):
        return jnp.concatenate(
            [sbuf[z // 4, lax.rem(z, 4), which, h] for h in range(heads)], axis=1
        )

    def turn(first, count):
        def step(z, c):
            for which, (dst, kept) in enumerate(((us, ut), (cs, ct))):
                dst[z] = jnp.transpose(low_rows(z, which)).reshape(dst.shape[1:])
                kept[quad, z] = dst[z, quad]
            return c

        lax.fori_loop(first, first + count, step, 0)

    def products(p, i):
        def one(z):
            blocks = pl.ds(pl.multiple_of(z * NQ, NQ), NQ)
            for j in range(2):
                left = low_rows(z, 1 if p + j == 2 else 0)
                nb[2 * p + j] = nb[2 * p + j] + dot(left, g[p, j, blocks].reshape(width, width))

        if i == 0 or i >= 7:
            one(place(i))
        else:

            def step(n, c):
                d = (i + 1) // 2
                one(lax.rem(me + NZ - d + 2 * d * n, NZ))
                return c

            lax.fori_loop(0, 2, step, 0)

    def ring_step(p, step):
        for way in range(2):
            i = index(way, step + 1)
            za(p, way, step).wait_recv()
            za(p, way, step + 1).start()
            ya(p, i).start()
            da(p, 0, i).start()
        for who in range(2):
            for way in range(2):
                zb(p, who, way, step).wait_recv()
                if step < 2 or who == way:
                    zb(p, who, way, step + 1).start()
                db(p, who, index(way, step + 1)).start()

    def ring_last(p):
        for way in range(2):
            za(p, way, 3).wait_recv()
            ya(p, 7 + way).start()
            da(p, 0, 7 + way).start()
        for way in range(2):
            zb(p, way, way, 3).wait_recv()
            db(p, way, 7).start()

    def arrivals(step):
        return (0,) if step == 0 else (2 * step - 1, 2 * step) if step < 4 else (7, 8)

    def lift(p, step):
        all_here(units(2 if 0 < step < 4 else 1), recv_ya.at[p, step])
        for i in arrivals(step):
            da(p, 1, i).start()

    def settle(p, step):
        all_here(units(8 if 0 < step < 4 else 4), recv_d.at[p, step])
        products(p, arrivals(step)[0])

    def normal(a, j, h):
        c = a - lane_mean(a)
        r = lax.rsqrt(lane_mean(c * c) + epsilon)
        u = c * r
        unit[j, h] = u
        inv[j, h] = r
        return u.astype(BF16)

    ring_step(0, 0)
    turn(0, 2)
    yb(1).wait_recv()
    db(1, 1, 0).start()
    lift(0, 0)
    ring_step(0, 1)
    for who in range(2):
        for way in range(2):
            zb(1, who, way, 0).start()
    turn(2, 2)
    lift(0, 1)
    settle(0, 0)
    ring_step(0, 2)
    lift(0, 2)
    settle(0, 1)
    ring_step(1, 0)
    ring_last(0)
    turn(4, 2)
    lift(1, 0)
    lift(0, 3)
    settle(0, 2)
    ring_step(1, 1)
    lift(0, 4)
    settle(0, 3)
    settle(1, 0)
    settle(0, 4)
    for h in range(heads):
        at = slice(h * HD, (h + 1) * HD)
        kv[me, 0, h] = normal(nb[0, :, at], 1, h)
        kv[me, 1, h] = nb[1, :, at].astype(BF16)
    for way in range(2):
        gather(way, 0, 0).start()
    ring_step(1, 2)
    for way in range(2):
        gather(way, 0, 1).start()
    lift(1, 1)
    lift(1, 2)
    settle(1, 1)
    turn(6, 2)
    settle(1, 2)
    ring_last(1)
    for which in range(2):
        for k in range(3):
            transposed(k, which).start()
    for way in range(2):
        gather(way, 0, 0).wait_recv()
        gather(way, 1, 0).start()
    lift(1, 3)
    settle(1, 3)
    lift(1, 4)
    settle(1, 4)
    for way in range(2):
        gather(way, 0, 1).wait_recv()
        gather(way, 1, 1).start()
    for h in range(heads):
        at = slice(h * HD, (h + 1) * HD)
        q_low[h] = normal(nb[2, :, at], 0, h)
        do[h] = nb[3, :, at].astype(BF16)
        wsum[h] = jnp.zeros_like(wsum[h])
        tsum[h] = jnp.zeros_like(tsum[h])
        dq[h] = jnp.zeros_like(dq[h])

    def forward(b, h):
        k = kv[b, 0, h]
        v = kv[b, 1, h]
        e = jnp.exp(dot(q_low[h], k, LAST) * scale)
        ex[b, h] = e
        tsum[h] = tsum[h] + (e[:, :HD] + e[:, HD:])
        wsum[h] = wsum[h] + dot(e.astype(BF16), v)
        dp[b, h] = dot(do[h], v, LAST)

    def forward_blocks(ahead, behind):
        def step(i, c):
            b = lax.rem(me + ahead + (i // heads) * (behind - ahead), NZ)
            forward(b, lax.rem(i, heads))
            return c

        lax.fori_loop(0, heads if ahead == behind else 2 * heads, step, 0)

    forward_blocks(0, 0)
    for step in range(3):
        for j in range(2):
            for way in range(2):
                if step == 0:
                    continue
                gather(way, step, j).wait_recv()
                if goes(way, step + 1, j):
                    gather(way, step + 1, j).start()
        forward_blocks(NZ - 1 - step, 1 + step)
    gather(0, 3, 0).wait_recv()
    gather(1, 3, 1).wait_recv()
    forward_blocks(4, 4)

    for h in range(heads):
        total = lane_sum(tsum[h])
        a = (wsum[h] / total).astype(BF16)
        act[0, quad, :, h * HD : (h + 1) * HD] = a
        rtot[h] = 1.0 / total
        delta[h] = lane_sum(do[h].astype(F32) * a.astype(F32))
    shared(0, 1).start()
    shared(0, 0).start()

    def backward(b, h):
        p = ex[b, h] * twice(rtot[h])
        ds = (p * (dp[b, h] - twice(delta[h])) * scale).astype(BF16)
        dq[h] = dq[h] + dot(ds, kv[b, 0, h])
        ex[b, h, :, :HD] = dot(ds, q_low[h], FIRST)
        ex[b, h, :, HD:] = dot(p.astype(BF16), do[h], FIRST)

    def backward_blocks(first, count):
        def step(i, c):
            n = first + i // heads
            away = (n + 1) // 2
            b = lax.rem(me + 4 + lax.rem(n, 2) * (NZ - 2 * away) + away, NZ)
            backward(b, lax.rem(i, heads))
            return c

        lax.fori_loop(0, count * heads, step, 0)

    def scatter_step(step):
        for j in range(2):
            for way in range(2):
                b = lax.rem(me + (4 - step if way == 0 else 4 + step), NZ)
                if step > 0:
                    scatter(way, step - 1, j).wait_recv()
                for h in range(heads):
                    for r in range(2):
                        if step == 0 and r != way:
                            continue
                        at = slice(r * half_block, (r + 1) * half_block)
                        val = ex[b, h, at, j * HD : (j + 1) * HD]
                        if step > 1 or step == 1 and r == way:
                            val = val + rbuf[way, step - 1, j, h, at].astype(F32)
                        sbuf[way, step, j, h, at] = val.astype(BF16)
                scatter(way, step, j).start()

    def relay(group):
        shared(group, 1).wait_recv()
        shared(group, 2).start()

    def back(val, j, h):
        u = unit[j, h]
        return (val - lane_mean(val) - u * lane_mean(val * u)) * inv[j, h]

    backward_blocks(0, 1)
    scatter_step(0)
    backward_blocks(1, 2)
    scatter_step(1)
    backward_blocks(3, 5)
    for h in range(heads):
        a = back(dq[h], 0, h).astype(BF16)
        act[1, quad, :, h * HD : (h + 1) * HD] = a
        low[:, h * HD : (h + 1) * HD] = a
    shared(1, 1).start()
    shared(1, 0).start()
    relay(0)
    scatter_step(2)
    relay(1)

    for which, there in enumerate((ut, ct)):
        all_here(there.at[0 : NQ - 1], recv_tr.at[which])
    for group in range(2):
        shared(group, 0).wait_recv()
        shared(group, 2).wait_recv()

    def weight_blocks(group):
        left = ct if group == 0 else ut
        tall = (left.shape[1] * left.shape[2], left.shape[3])
        for m in range(NQ):
            val = dot(left[m].reshape(tall), act[group, m])
            if m:
                val = val + dwp[group]
            dwp[group] = val

    own_rows = own_out.shape[0]

    def weight_part(z, group):
        return dwp[group, pl.ds(pl.multiple_of(z * own_rows, own_rows), own_rows), :]

    def weight_step(step, group):
        for way in range(2):
            if not goes(way, 3 - step, group):
                continue
            val = weight_part(lax.rem(me + (4 - step if way == 0 else 4 + step), NZ), group)
            if step > 0 and goes(way, 4 - step, group):
                weight_ring(way, step - 1, group).wait_recv()
                val = val + rdw[way, step - 1, group].astype(F32)
            sdw[way, step, group] = val.astype(BF16)
            weight_ring(way, step, group).start()

    def early_ring(way, step):
        both = slice(0, 2)
        return remote(
            sdw.at[way, step, both],
            rdw.at[way, step, both],
            send_dw,
            recv_dw.at[way, step, 0],
            {"seq": sides[way]},
        )

    def early_step(step):
        for way in range(2):
            if step == 1:
                weight_ring(way, 0, way).wait_recv()
            else:
                early_ring(way, step - 1).wait_recv()
            z = lax.rem(me + (4 - step if way == 0 else 4 + step), NZ)
            for group in range(2):
                val = weight_part(z, group)
                if step > 1 or group == way:
                    val = val + rdw[way, step - 1, group].astype(F32)
                sdw[way, step, group] = val.astype(BF16)
            early_ring(way, step).start()

    for group in range(2):
        weight_blocks(group)
        weight_step(0, group)
    scatter_step(3)
    early_step(1)

    for j in range(2):
        for way in range(2):
            scatter(way, 3, j).wait_recv()
        for h in range(heads):
            val = ex[me, h, :, j * HD : (j + 1) * HD]
            val = val + rbuf[0, 3, j, h].astype(F32) + rbuf[1, 3, j, h].astype(F32)
            if j == 0:
                val = back(val, 1, h)
            a = val.astype(BF16)
            act[2 + j, quad, :, h * HD : (h + 1) * HD] = a
            low[:, (j + 1) * width + h * HD : (j + 1) * width + (h + 1) * HD] = a
        shared(2 + j, 1).start()
        shared(2 + j, 0).start()

    def inner(n, sums):
        x = lax.rem(xplace + 2 + n // 2, 4)
        t = 2 * x + lax.rem(n, 2)
        blocks = pl.ds(pl.multiple_of(t * NQ, NQ), NQ)
        a = jnp.zeros_like(nb[t])
        for j, (p, i) in enumerate(((1, 0), (0, 0), (0, 1))):
            left = low[:, j * width : (j + 1) * width]
            a = a + dot(left, g[p, i, blocks].reshape(width, width), LAST)
        nb[t] = a
        one, two = sums
        for k in range(heads):
            at = slice(k * HD, (k + 1) * HD)
            one = one + a[:, at]
            two = two + a[:, at] * ((tb[t, :, at].astype(F32) - norm[0]) * norm[1])
        return one, two

    def piece(x, half):
        return nb[2 * x + (1 - yhalf if half == 0 else yhalf)]

    def inner_step(step):
        for half in range(2):
            for way in range(2):
                if step == 0 and half != way:
                    continue
                x = lax.rem(xplace + (2 - step if way == 0 else 2 + step), 4)
                val = piece(x, half)
                if step > 0 and half == way:
                    xring(way, 0, half).wait_recv()
                    val = val + xr[way, 0, half].astype(F32)
                xs[way, step, half] = val.astype(BF16)
                xring(way, step, half).start()

    def arrived(half):
        for way in range(2):
            xring(way, 1, half).wait_recv()
        val = piece(xplace, half)
        return val + xr[0, 1, half].astype(F32) + xr[1, 1, half].astype(F32)

    zero = jnp.zeros((low.shape[0], HD), F32)
    sums = lax.fori_loop(0, 2, inner, (zero, zero))
    inner_step(0)
    relay(2)
    early_step(2)
    sums = lax.fori_loop(2, 4, inner, sums)
    shared(2, 0).wait_recv()
    shared(2, 2).wait_recv()
    weight_blocks(2)
    weight_step(0, 2)
    sums = lax.fori_loop(4, 6, inner, sums)
    relay(3)
    sums = lax.fori_loop(6, NT, inner, sums)
    for i in range(2):
        stats[0, i * 8 : (i + 1) * 8, :] = jnp.transpose(lane_sum(sums[i]))[:8]
    for k in range(1, NT):
        stat(k).start()
    inner_step(1)
    shared(3, 0).wait_recv()
    shared(3, 2).wait_recv()
    weight_blocks(3)
    weight_step(0, 3)
    weight_step(1, 2)
    weight_step(1, 3)
    weight_step(2, 2)
    early_step(3)
    ysend[...] = arrived(0).astype(BF16)
    ypair().start()
    weight_step(2, 3)
    weight_step(3, 2)
    all_here(stats.at[0 : NT - 1], recv_st)
    total = stats[0]
    for k in range(1, NT):
        total = total + stats[k]
    row_mean = []
    for i in range(2):
        row = jnp.broadcast_to(total[i * 8 : i * 8 + 1, :], (HD, total.shape[1]))
        row_mean.append(jnp.transpose(row) / features)
    share = arrived(1)
    weight_step(3, 3)

    ypair().wait_recv()
    share = share + yrecv[...].astype(F32)
    for k in range(heads):
        at = slice(k * HD, (k + 1) * HD)
        own_unit = (tb[part, :, at].astype(F32) - norm[0]) * norm[1]
        val = share[:, at] - row_mean[0] - own_unit * row_mean[1]
        branch_out[:, at] = (val * norm[1]).astype(BF16)

    for group in range(4):
        val = weight_part(me, group)
        for way in range(2):
            if group > 1:
                weight_ring(way, 3, group).wait_recv()
            elif group == 0:
                early_ring(way, 3).wait_recv()
            val = val + rdw[way, 3, group].astype(F32)
        if group == 0:
            out_out[...] = val
        else:
            qkv_out[group - 1] = val

    all_sent(g.at[:, :, 0 : NZ * NQ - 1], send_w)
    all_sent(kv.at[0 : NZ - 1], send_ag)
    all_sent(kv.at[0 : NZ - 1], send_rs)
    all_sent(units(28), send_dw)
    for which, here in enumerate((ut, ct)):
        all_sent(here.at[0 : NQ - 1], send_tr.at[which])
    all_sent(act.at[0:3], send_act)
    all_sent(act.at[0:3, 0:2], send_x)
    ypair().wait_send()
    all_sent(stats.at[0 : NT - 1], send_st)


def layer(tokens, cot, own_qkv, own_out):
    rows = tokens.shape[0]
    own, width = own_out.shape
    heads = width // HD
    vmem = pl.BlockSpec(memory_space=pltpu.VMEM)
    hbm = pl.BlockSpec(memory_space=pl.ANY)
    one = (heads, rows, HD)
    dma = pltpu.SemaphoreType.DMA
    return pl.pallas_call(
        lambda *refs: layer_kernel(heads, *refs),
        out_shape=(
            jax.ShapeDtypeStruct((3, own, width), F32),
            jax.ShapeDtypeStruct((own, width), F32),
            jax.ShapeDtypeStruct((rows, width), BF16),
        ),
        in_specs=[hbm] * 4,
        out_specs=(vmem, vmem, vmem),
        scratch_shapes=[
            pltpu.VMEM(one, BF16),
            pltpu.VMEM(one, BF16),
            pltpu.VMEM((2, *one), F32),
            pltpu.VMEM((2, *one), F32),
            pltpu.VMEM((NZ, 2, *one), BF16),
            pltpu.VMEM((NZ, heads, rows, rows), F32),
            pltpu.VMEM((NZ, heads, rows, rows), F32),
            pltpu.VMEM(one, F32),
            pltpu.VMEM(one, F32),
            pltpu.VMEM(one, F32),
            pltpu.VMEM(one, F32),
            pltpu.VMEM(one, F32),
            pltpu.VMEM((2, 4, 2, *one), BF16),
            pltpu.VMEM((2, 4, 2, *one), BF16),
            pltpu.VMEM((4, NQ, rows, width), BF16),
            pltpu.VMEM((rows, 3 * width), BF16),
            pltpu.VMEM((NQ, NZ, own, rows), BF16),
            pltpu.VMEM((NQ, NZ, own, rows), BF16),
            pltpu.VMEM((NZ, NQ, own, rows), BF16),
            pltpu.VMEM((NZ, NQ, own, rows), BF16),
            pltpu.VMEM((2, 2, NZ * NQ, own, width), BF16),
            pltpu.VMEM((NT, rows, width), BF16),
            pltpu.VMEM((NT, rows, width), F32),
            pltpu.VMEM((2, rows, HD), F32),
            pltpu.VMEM((2, 4, 4, own, width), BF16),
            pltpu.VMEM((2, 4, 4, own, width), BF16),
            pltpu.VMEM((4, NZ * own, width), F32),
            pltpu.VMEM((2, 2, 2, rows, width), BF16),
            pltpu.VMEM((2, 2, 2, rows, width), BF16),
            pltpu.VMEM((rows, width), BF16),
            pltpu.VMEM((rows, width), BF16),
            pltpu.VMEM((NT, 16, rows), F32),
            dma,
            dma((2, 4, 2)),
            dma,
            dma((2, 4, 2)),
            dma((2,)),
            dma((2,)),
            dma,
            dma((4, 3)),
            dma,
            dma((2, 4, 4)),
            dma,
            dma((2, 2, 2)),
            dma,
            dma,
            dma,
            dma,
            dma,
            dma((2, 2, 4)),
            dma((2, 2, 2, 4)),
            dma((2, 5)),
            dma((2,)),
            dma((2, 5)),
            dma,
            dma,
            dma,
        ],
        compiler_params=pltpu.CompilerParams(
            collective_id=0, has_side_effects=True, vmem_limit_bytes=67_043_328
        ),
    )(tokens, cot, own_qkv, own_out)


def finish(*arrays):
    def kernel(*refs):
        for i in range(len(arrays)):
            refs[len(arrays) + i][...] = refs[i][...]

    vmem = pl.BlockSpec(memory_space=pltpu.VMEM)
    return pl.pallas_call(
        kernel,
        out_shape=tuple(jax.ShapeDtypeStruct(a.shape, a.dtype) for a in arrays),
        in_specs=[vmem] * len(arrays),
        out_specs=(vmem,) * len(arrays),
    )(*arrays)


def local(tokens, cotangent, qkv_weight, out_weight):
    qkv_grad, out_grad, branch = finish(
        *layer(tokens[0], cotangent[0], jnp.transpose(qkv_weight, (1, 0, 2)), out_weight)
    )
    return (jnp.transpose(qkv_grad, (1, 0, 2)), out_grad, branch[None])


def solution(mesh):
    return jax.shard_map(
        local,
        mesh=mesh,
        in_specs=(
            P("dp", "seq", None),
            P("dp", "seq", None),
            P(("seq", "dp"), None, "tensor"),
            P(("seq", "dp"), "tensor"),
        ),
        out_specs=(
            P(("seq", "dp"), None, "tensor"),
            P(("seq", "dp"), "tensor"),
            P("dp", "seq", "tensor"),
        ),
        check_vma=False,
    )
```

```python
import jax
import jax.numpy as jnp
from jax import lax
from jax.experimental import pallas as pl
from jax.experimental.pallas import tpu as pltpu
from jax.sharding import PartitionSpec as P

HD = 128
NZ = 8
NT = 8
NQ = 4
MESH = pl.DeviceIdType.MESH
F32 = jnp.float32
BF16 = jnp.bfloat16
LAST = (((1,), (1,)), ((), ()))
FIRST = (((0,), (0,)), ((), ()))
epsilon = 1e-06


def dot(a, b, dims=(((1,), (0,)), ((), ()))):
    return lax.dot_general(a, b, dims, preferred_element_type=F32)


def twice(a):
    return jnp.concatenate([a, a], axis=1)


def lane_mean(a):
    return jnp.broadcast_to(jnp.mean(a, axis=1, keepdims=True), a.shape)


def lane_sum(a):
    return jnp.broadcast_to(jnp.sum(a, axis=1, keepdims=True), a.shape)


def layer_kernel(
    heads,
    tokens,
    cot,
    own_qkv,
    own_out,
    qkv_out,
    out_out,
    branch_out,
    q_low,
    do,
    unit,
    inv,
    kv,
    ex,
    dp,
    wsum,
    tsum,
    rtot,
    delta,
    dq,
    sbuf,
    rbuf,
    act,
    low,
    ut,
    ct,
    us,
    cs,
    g,
    tb,
    nb,
    norm,
    sdw,
    rdw,
    dwp,
    xs,
    xr,
    ysend,
    yrecv,
    stats,
    send_ag,
    recv_ag,
    send_rs,
    recv_rs,
    send_tr,
    recv_tr,
    send_act,
    recv_act,
    send_dw,
    recv_dw,
    send_x,
    recv_x,
    send_y,
    recv_y,
    send_st,
    recv_st,
    send_w,
    recv_za,
    recv_zb,
    recv_ya,
    recv_yb,
    recv_d,
    load_g,
    load_t,
    load_c,
):
    me = lax.axis_index("seq")
    quad = lax.axis_index("dp")
    part = lax.axis_index("tensor")
    sides = (lax.rem(me + 1, NZ), lax.rem(me + NZ - 1, NZ))
    mates = (quad + 1 - 2 * lax.rem(quad, 2), lax.rem(quad + 2, NQ), NQ - 1 - quad)
    xsides = (lax.rem(part + 2, NT), lax.rem(part + NT - 2, NT))
    ymate = part + 1 - 2 * lax.rem(part, 2)
    yhalf = lax.rem(part, 2)
    xplace = part // 2
    scale = HD ** (-0.5)
    width = heads * HD
    features = NT * width
    half_block = tokens.shape[0] // 2

    barrier = pltpu.get_barrier_semaphore()
    for side in sides:
        pl.semaphore_signal(barrier, inc=1, device_id={"seq": side}, device_id_type=MESH)
    for mate in mates:
        pl.semaphore_signal(barrier, inc=1, device_id={"dp": mate}, device_id_type=MESH)
    for k in range(1, NT):
        pl.semaphore_signal(
            barrier, inc=1, device_id={"tensor": lax.rem(part + k, NT)}, device_id_type=MESH
        )

    def remote(src, dst, send, recv, where):
        return pltpu.make_async_remote_copy(
            src_ref=src,
            dst_ref=dst,
            send_sem=send,
            recv_sem=recv,
            device_id=where,
            device_id_type=MESH,
        )

    def gather(way, step, j):
        b = lax.rem(me + (NZ - step if way == 0 else step), NZ)
        return remote(
            kv.at[b, j],
            kv.at[b, j],
            send_ag,
            recv_ag.at[way, step, j],
            {"seq": sides[way]},
        )

    def scatter(way, step, j):
        part_of = pl.ds(way * half_block, half_block) if step == 0 else pl.ds(0, 2 * half_block)
        return remote(
            sbuf.at[way, step, j, :, part_of],
            rbuf.at[way, step, j, :, part_of],
            send_rs,
            recv_rs.at[way, step, j],
            {"seq": sides[way]},
        )

    def weight_ring(way, step, group):
        return remote(
            sdw.at[way, step, group],
            rdw.at[way, step, group],
            send_dw,
            recv_dw.at[way, step, group],
            {"seq": sides[way]},
        )

    def transposed(k, which):
        src, dst = ((us, ut), (cs, ct))[which]
        return remote(
            src.at[:, mates[k]],
            dst.at[quad],
            send_tr.at[which],
            recv_tr.at[which],
            {"dp": mates[k]},
        )

    def shared(group, k):
        block = act.at[group, quad if k < 2 else mates[1]]
        return remote(
            block,
            block,
            send_act,
            recv_act.at[group, k],
            {"dp": mates[1] if k == 1 else mates[0]},
        )

    def xring(way, step, half):
        return remote(
            xs.at[way, step, half],
            xr.at[way, step, half],
            send_x,
            recv_x.at[way, step, half],
            {"tensor": xsides[way]},
        )

    def ypair():
        return remote(ysend, yrecv, send_y, recv_y, {"tensor": ymate})

    def stat(k):
        return remote(
            stats.at[0],
            stats.at[k],
            send_st,
            recv_st,
            {"tensor": lax.rem(part + k, NT)},
        )

    def goes(way, step, j):
        return step < 3 or j % 2 == way

    mine = me * NQ + quad
    load_own = [
        pltpu.make_async_copy(own_qkv.at[1], g.at[0, 0, mine], load_g),
        pltpu.make_async_copy(own_qkv.at[2], g.at[0, 1, mine], load_g),
        pltpu.make_async_copy(own_qkv.at[0], g.at[1, 0, mine], load_g),
        pltpu.make_async_copy(own_out, g.at[1, 1, mine], load_g),
    ]
    load_tokens = [
        pltpu.make_async_copy(tokens.at[:, z * width : (z + 1) * width], tb.at[z], load_t)
        for z in range(NZ)
    ]
    load_cot = [
        pltpu.make_async_copy(
            cot.at[:, (z * heads + h) * HD : (z * heads + h + 1) * HD],
            sbuf.at[z // 4, z % 4, 1, h],
            load_c,
        )
        for z in range(NZ)
        for h in range(heads)
    ]
    for c in load_own + load_tokens + load_cot:
        c.start()

    classes = (quad, mates[1])
    half_rows = own_out.shape[0] // 2

    def place(i):
        if i == 0:
            return me
        if i >= 7:
            return lax.rem(me + 4, NZ)
        step, way = (i - 1) // 2, (i - 1) % 2
        return lax.rem(me + (NZ - 1 - step if way == 0 else 1 + step), NZ)

    def first_array(p, i, who):
        b = place(i) * NQ + classes[who]
        if i >= 7:
            return g.at[p, 0, b, (i - 7) * half_rows : (i - 6) * half_rows]
        return g.at[p, 0, b]

    def second_array(p, i, who):
        return g.at[p, 1, place(i) * NQ + classes[who]]

    def stage(i):
        return 4 if i >= 7 else (i + 1) // 2

    def index(way, step):
        return 0 if step == 0 else 1 + 2 * (step - 1) + way

    def same(block, send, recv, where):
        return remote(block, block, send, recv, where)

    def za(p, way, step):
        return same(
            g.at[p, 0, lax.rem(me + (NZ - step if way == 0 else step), NZ) * NQ + quad]
            if step < 3
            else g.at[
                p,
                0,
                lax.rem(me + (NZ - step if way == 0 else step), NZ) * NQ + quad,
                way * half_rows : (way + 1) * half_rows,
            ],
            send_w,
            recv_za.at[p, way, step],
            {"seq": sides[way]},
        )

    def zb(p, who, way, step):
        z = lax.rem(me + (NZ - step if way == 0 else step), NZ)
        return same(
            g.at[p, 1, z * NQ + classes[who]],
            send_w,
            recv_zb.at[p, who, way, step],
            {"seq": sides[way]},
        )

    def ya(p, i):
        return same(
            first_array(p, i, 0), send_w, recv_ya.at[p, stage(i)], {"dp": mates[1]}
        )

    def yb(p):
        return same(second_array(p, 0, 0), send_w, recv_yb.at[p], {"dp": mates[1]})

    def da(p, who, i):
        return same(
            first_array(p, i, who),
            send_w,
            recv_d.at[p, stage(i)],
            {"dp": mates[0]},
        )

    def db(p, who, i):
        return same(
            second_array(p, i, who),
            send_w,
            recv_d.at[p, stage(i)],
            {"dp": mates[0]},
        )

    def whole(ref, sem):
        return pltpu.make_async_copy(ref, ref, sem)

    def units(n):
        return g.at[0, 0, 0:n]

    def all_sent(ref, sem):
        remote(ref, ref, sem, sem, {"seq": sides[0]}).wait_send()

    def all_here(ref, sem):
        remote(ref, ref, sem, sem, {"seq": sides[0]}).wait_recv()

    whole(units(4), load_g).wait()
    pl.semaphore_wait(barrier, 2 + 3 + NT - 1)
    for way in range(2):
        za(0, way, 0).start()
    for p in range(2):
        yb(p).start()
    for way in range(2):
        zb(0, 0, way, 0).start()
    for p in range(2):
        ya(p, 0).start()
    for p in range(2):
        da(p, 0, 0).start()
        db(p, 0, 0).start()

    rows = tb.shape[1]
    blank = jnp.zeros((rows, HD), F32)
    whole(tb, load_t).wait()

    def fold(a):
        s = a[:, :HD]
        for k in range(1, heads):
            s = s + a[:, k * HD : (k + 1) * HD]
        return s

    def wide(a):
        return jnp.concatenate([a] * heads, axis=1)

    def add_sum(z, s):
        return s + fold(tb[z].astype(F32))

    average = lane_sum(lax.fori_loop(0, NZ, add_sum, blank)) / features

    def add_square(z, s):
        c = tb[z].astype(F32) - wide(average)
        return s + fold(c * c)

    norm[0] = average
    norm[1] = lax.rsqrt(lane_sum(lax.fori_loop(0, NZ, add_square, blank)) / features + epsilon)

    yb(0).wait_recv()
    for way in range(2):
        zb(0, 1, way, 0).start()
    db(0, 1, 0).start()

    def lower(z, c):
        for h in range(heads):
            a = tb[z, :, h * HD : (h + 1) * HD].astype(F32)
            sbuf[z // 4, lax.rem(z, 4), 0, h] = ((a - norm[0]) * norm[1]).astype(BF16)
        return c

    lax.fori_loop(0, NZ, lower, 0)
    for i in range(4):
        nb[i] = jnp.zeros_like(nb[i])
    whole(sbuf.at[:, :, 1], load_c).wait()

    def low_rows(z, which):
        return jnp.concatenate(
            [sbuf[z // 4, lax.rem(z, 4), which, h] for h in range(heads)], axis=1
        )

    def turn(first, count):
        def step(z, c):
            for which, (dst, kept) in enumerate(((us, ut), (cs, ct))):
                dst[z] = jnp.transpose(low_rows(z, which)).reshape(dst.shape[1:])
                kept[quad, z] = dst[z, quad]
            return c

        lax.fori_loop(first, first + count, step, 0)

    def products(p, i):
        def one(z):
            blocks = pl.ds(pl.multiple_of(z * NQ, NQ), NQ)
            for j in range(2):
                left = low_rows(z, 1 if p + j == 2 else 0)
                nb[2 * p + j] = nb[2 * p + j] + dot(left, g[p, j, blocks].reshape(width, width))

        if i == 0 or i >= 7:
            one(place(i))
        else:

            def step(n, c):
                d = (i + 1) // 2
                one(lax.rem(me + NZ - d + 2 * d * n, NZ))
                return c

            lax.fori_loop(0, 2, step, 0)

    def ring_step(p, step):
        for way in range(2):
            i = index(way, step + 1)
            za(p, way, step).wait_recv()
            za(p, way, step + 1).start()
            ya(p, i).start()
            da(p, 0, i).start()
        for who in range(2):
            for way in range(2):
                zb(p, who, way, step).wait_recv()
                if step < 2 or who == way:
                    zb(p, who, way, step + 1).start()
                db(p, who, index(way, step + 1)).start()

    def ring_last(p):
        for way in range(2):
            za(p, way, 3).wait_recv()
            ya(p, 7 + way).start()
            da(p, 0, 7 + way).start()
        for way in range(2):
            zb(p, way, way, 3).wait_recv()
            db(p, way, 7).start()

    def arrivals(step):
        return (0,) if step == 0 else (2 * step - 1, 2 * step) if step < 4 else (7, 8)

    def lift(p, step):
        all_here(units(2 if 0 < step < 4 else 1), recv_ya.at[p, step])
        for i in arrivals(step):
            da(p, 1, i).start()

    def settle(p, step):
        all_here(units(8 if 0 < step < 4 else 4), recv_d.at[p, step])
        products(p, arrivals(step)[0])

    def normal(a, j, h):
        c = a - lane_mean(a)
        r = lax.rsqrt(lane_mean(c * c) + epsilon)
        u = c * r
        unit[j, h] = u
        inv[j, h] = r
        return u.astype(BF16)

    ring_step(0, 0)
    for way in range(2):
        za(1, way, 0).start()
    turn(0, 2)
    yb(1).wait_recv()
    db(1, 1, 0).start()
    lift(0, 0)
    ring_step(0, 1)
    for who in range(2):
        for way in range(2):
            zb(1, who, way, 0).start()
    turn(2, 2)
    lift(0, 1)
    settle(0, 0)
    ring_step(0, 2)
    lift(0, 2)
    settle(0, 1)
    ring_step(1, 0)
    ring_last(0)
    turn(4, 2)
    lift(1, 0)
    lift(0, 3)
    settle(0, 2)
    ring_step(1, 1)
    lift(0, 4)
    settle(0, 3)
    settle(1, 0)
    settle(0, 4)
    for h in range(heads):
        at = slice(h * HD, (h + 1) * HD)
        kv[me, 0, h] = normal(nb[0, :, at], 1, h)
        kv[me, 1, h] = nb[1, :, at].astype(BF16)
    for way in range(2):
        gather(way, 0, 0).start()
    ring_step(1, 2)
    for way in range(2):
        gather(way, 0, 1).start()
    lift(1, 1)
    lift(1, 2)
    settle(1, 1)
    turn(6, 2)
    settle(1, 2)
    ring_last(1)
    for which in range(2):
        for k in range(3):
            transposed(k, which).start()
    for way in range(2):
        gather(way, 0, 0).wait_recv()
        gather(way, 1, 0).start()
    lift(1, 3)
    settle(1, 3)
    lift(1, 4)
    settle(1, 4)
    for way in range(2):
        gather(way, 0, 1).wait_recv()
        gather(way, 1, 1).start()
    for h in range(heads):
        at = slice(h * HD, (h + 1) * HD)
        q_low[h] = normal(nb[2, :, at], 0, h)
        do[h] = nb[3, :, at].astype(BF16)
        wsum[h] = jnp.zeros_like(wsum[h])
        tsum[h] = jnp.zeros_like(tsum[h])
        dq[h] = jnp.zeros_like(dq[h])

    def forward(b, h):
        k = kv[b, 0, h]
        v = kv[b, 1, h]
        e = jnp.exp(dot(q_low[h], k, LAST) * scale)
        ex[b, h] = e
        tsum[h] = tsum[h] + (e[:, :HD] + e[:, HD:])
        wsum[h] = wsum[h] + dot(e.astype(BF16), v)
        dp[b, h] = dot(do[h], v, LAST)

    def forward_blocks(ahead, behind):
        def step(i, c):
            b = lax.rem(me + ahead + (i // heads) * (behind - ahead), NZ)
            forward(b, lax.rem(i, heads))
            return c

        lax.fori_loop(0, heads if ahead == behind else 2 * heads, step, 0)

    forward_blocks(0, 0)
    for step in range(3):
        for j in range(2):
            for way in range(2):
                if step == 0:
                    continue
                gather(way, step, j).wait_recv()
                if goes(way, step + 1, j):
                    gather(way, step + 1, j).start()
        forward_blocks(NZ - 1 - step, 1 + step)
    gather(0, 3, 0).wait_recv()
    gather(1, 3, 1).wait_recv()
    forward_blocks(4, 4)

    for h in range(heads):
        total = lane_sum(tsum[h])
        a = (wsum[h] / total).astype(BF16)
        act[0, quad, :, h * HD : (h + 1) * HD] = a
        rtot[h] = 1.0 / total
        delta[h] = lane_sum(do[h].astype(F32) * a.astype(F32))
    shared(0, 1).start()
    shared(0, 0).start()

    def backward(b, h):
        p = ex[b, h] * twice(rtot[h])
        ds = (p * (dp[b, h] - twice(delta[h])) * scale).astype(BF16)
        dq[h] = dq[h] + dot(ds, kv[b, 0, h])
        ex[b, h, :, :HD] = dot(ds, q_low[h], FIRST)
        ex[b, h, :, HD:] = dot(p.astype(BF16), do[h], FIRST)

    def backward_blocks(first, count):
        def step(i, c):
            n = first + i // heads
            away = (n + 1) // 2
            b = lax.rem(me + 4 + lax.rem(n, 2) * (NZ - 2 * away) + away, NZ)
            backward(b, lax.rem(i, heads))
            return c

        lax.fori_loop(0, count * heads, step, 0)

    def scatter_step(step):
        for j in range(2):
            for way in range(2):
                b = lax.rem(me + (4 - step if way == 0 else 4 + step), NZ)
                if step > 0:
                    scatter(way, step - 1, j).wait_recv()
                for h in range(heads):
                    for r in range(2):
                        if step == 0 and r != way:
                            continue
                        at = slice(r * half_block, (r + 1) * half_block)
                        val = ex[b, h, at, j * HD : (j + 1) * HD]
                        if step > 1 or step == 1 and r == way:
                            val = val + rbuf[way, step - 1, j, h, at].astype(F32)
                        sbuf[way, step, j, h, at] = val.astype(BF16)
                scatter(way, step, j).start()

    def relay(group):
        shared(group, 1).wait_recv()
        shared(group, 2).start()

    def back(val, j, h):
        u = unit[j, h]
        return (val - lane_mean(val) - u * lane_mean(val * u)) * inv[j, h]

    backward_blocks(0, 1)
    scatter_step(0)
    backward_blocks(1, 2)
    scatter_step(1)
    backward_blocks(3, 5)
    for h in range(heads):
        a = back(dq[h], 0, h).astype(BF16)
        act[1, quad, :, h * HD : (h + 1) * HD] = a
        low[:, h * HD : (h + 1) * HD] = a
    shared(1, 1).start()
    shared(1, 0).start()
    relay(0)
    scatter_step(2)
    relay(1)

    for which, there in enumerate((ut, ct)):
        all_here(there.at[0 : NQ - 1], recv_tr.at[which])
    for group in range(2):
        shared(group, 0).wait_recv()
        shared(group, 2).wait_recv()

    def weight_blocks(group):
        left = ct if group == 0 else ut
        tall = (left.shape[1] * left.shape[2], left.shape[3])
        for m in range(NQ):
            val = dot(left[m].reshape(tall), act[group, m])
            if m:
                val = val + dwp[group]
            dwp[group] = val

    own_rows = own_out.shape[0]

    def weight_part(z, group):
        return dwp[group, pl.ds(pl.multiple_of(z * own_rows, own_rows), own_rows), :]

    def weight_step(step, group):
        for way in range(2):
            if not goes(way, 3 - step, group):
                continue
            val = weight_part(lax.rem(me + (4 - step if way == 0 else 4 + step), NZ), group)
            if step > 0 and goes(way, 4 - step, group):
                weight_ring(way, step - 1, group).wait_recv()
                val = val + rdw[way, step - 1, group].astype(F32)
            sdw[way, step, group] = val.astype(BF16)
            weight_ring(way, step, group).start()

    def early_ring(way, step):
        both = slice(0, 2)
        return remote(
            sdw.at[way, step, both],
            rdw.at[way, step, both],
            send_dw,
            recv_dw.at[way, step, 0],
            {"seq": sides[way]},
        )

    def early_step(step):
        for way in range(2):
            if step == 1:
                weight_ring(way, 0, way).wait_recv()
            else:
                early_ring(way, step - 1).wait_recv()
            z = lax.rem(me + (4 - step if way == 0 else 4 + step), NZ)
            for group in range(2):
                val = weight_part(z, group)
                if step > 1 or group == way:
                    val = val + rdw[way, step - 1, group].astype(F32)
                sdw[way, step, group] = val.astype(BF16)
            early_ring(way, step).start()

    for group in range(2):
        weight_blocks(group)
        weight_step(0, group)
    scatter_step(3)
    early_step(1)

    for j in range(2):
        for way in range(2):
            scatter(way, 3, j).wait_recv()
        for h in range(heads):
            val = ex[me, h, :, j * HD : (j + 1) * HD]
            val = val + rbuf[0, 3, j, h].astype(F32) + rbuf[1, 3, j, h].astype(F32)
            if j == 0:
                val = back(val, 1, h)
            a = val.astype(BF16)
            act[2 + j, quad, :, h * HD : (h + 1) * HD] = a
            low[:, (j + 1) * width + h * HD : (j + 1) * width + (h + 1) * HD] = a
        shared(2 + j, 1).start()
        shared(2 + j, 0).start()

    def inner(n, sums):
        x = lax.rem(xplace + 2 + n // 2, 4)
        t = 2 * x + lax.rem(n, 2)
        blocks = pl.ds(pl.multiple_of(t * NQ, NQ), NQ)
        a = jnp.zeros_like(nb[t])
        for j, (p, i) in enumerate(((1, 0), (0, 0), (0, 1))):
            left = low[:, j * width : (j + 1) * width]
            a = a + dot(left, g[p, i, blocks].reshape(width, width), LAST)
        nb[t] = a
        one, two = sums
        for k in range(heads):
            at = slice(k * HD, (k + 1) * HD)
            one = one + a[:, at]
            two = two + a[:, at] * ((tb[t, :, at].astype(F32) - norm[0]) * norm[1])
        return one, two

    def piece(x, half):
        return nb[2 * x + (1 - yhalf if half == 0 else yhalf)]

    def inner_step(step):
        for half in range(2):
            for way in range(2):
                if step == 0 and half != way:
                    continue
                x = lax.rem(xplace + (2 - step if way == 0 else 2 + step), 4)
                val = piece(x, half)
                if step > 0 and half == way:
                    xring(way, 0, half).wait_recv()
                    val = val + xr[way, 0, half].astype(F32)
                xs[way, step, half] = val.astype(BF16)
                xring(way, step, half).start()

    def arrived(half):
        for way in range(2):
            xring(way, 1, half).wait_recv()
        val = piece(xplace, half)
        return val + xr[0, 1, half].astype(F32) + xr[1, 1, half].astype(F32)

    zero = jnp.zeros((low.shape[0], HD), F32)
    sums = lax.fori_loop(0, 2, inner, (zero, zero))
    inner_step(0)
    relay(2)
    early_step(2)
    sums = lax.fori_loop(2, 4, inner, sums)
    shared(2, 0).wait_recv()
    shared(2, 2).wait_recv()
    weight_blocks(2)
    weight_step(0, 2)
    sums = lax.fori_loop(4, 6, inner, sums)
    relay(3)
    sums = lax.fori_loop(6, NT, inner, sums)
    for i in range(2):
        stats[0, i * 8 : (i + 1) * 8, :] = jnp.transpose(lane_sum(sums[i]))[:8]
    for k in range(1, NT):
        stat(k).start()
    inner_step(1)
    shared(3, 0).wait_recv()
    shared(3, 2).wait_recv()
    weight_blocks(3)
    weight_step(0, 3)
    weight_step(1, 2)
    weight_step(1, 3)
    weight_step(2, 2)
    early_step(3)
    ysend[...] = arrived(0).astype(BF16)
    ypair().start()
    weight_step(2, 3)
    weight_step(3, 2)
    all_here(stats.at[0 : NT - 1], recv_st)
    total = stats[0]
    for k in range(1, NT):
        total = total + stats[k]
    row_mean = []
    for i in range(2):
        row = jnp.broadcast_to(total[i * 8 : i * 8 + 1, :], (HD, total.shape[1]))
        row_mean.append(jnp.transpose(row) / features)
    share = arrived(1)
    weight_step(3, 3)

    ypair().wait_recv()
    share = share + yrecv[...].astype(F32)
    for k in range(heads):
        at = slice(k * HD, (k + 1) * HD)
        own_unit = (tb[part, :, at].astype(F32) - norm[0]) * norm[1]
        val = share[:, at] - row_mean[0] - own_unit * row_mean[1]
        branch_out[:, at] = (val * norm[1]).astype(BF16)

    for group in range(4):
        val = weight_part(me, group)
        for way in range(2):
            if group > 1:
                weight_ring(way, 3, group).wait_recv()
            elif group == 0:
                early_ring(way, 3).wait_recv()
            val = val + rdw[way, 3, group].astype(F32)
        if group == 0:
            out_out[...] = val
        else:
            qkv_out[group - 1] = val

    all_sent(g.at[:, :, 0 : NZ * NQ - 1], send_w)
    all_sent(kv.at[0 : NZ - 1], send_ag)
    all_sent(kv.at[0 : NZ - 1], send_rs)
    all_sent(units(28), send_dw)
    for which, here in enumerate((ut, ct)):
        all_sent(here.at[0 : NQ - 1], send_tr.at[which])
    all_sent(act.at[0:3], send_act)
    all_sent(act.at[0:3, 0:2], send_x)
    ypair().wait_send()
    all_sent(stats.at[0 : NT - 1], send_st)


def layer(tokens, cot, own_qkv, own_out):
    rows = tokens.shape[0]
    own, width = own_out.shape
    heads = width // HD
    vmem = pl.BlockSpec(memory_space=pltpu.VMEM)
    hbm = pl.BlockSpec(memory_space=pl.ANY)
    one = (heads, rows, HD)
    dma = pltpu.SemaphoreType.DMA
    return pl.pallas_call(
        lambda *refs: layer_kernel(heads, *refs),
        out_shape=(
            jax.ShapeDtypeStruct((3, own, width), F32),
            jax.ShapeDtypeStruct((own, width), F32),
            jax.ShapeDtypeStruct((rows, width), BF16),
        ),
        in_specs=[hbm] * 4,
        out_specs=(vmem, vmem, vmem),
        scratch_shapes=[
            pltpu.VMEM(one, BF16),
            pltpu.VMEM(one, BF16),
            pltpu.VMEM((2, *one), F32),
            pltpu.VMEM((2, *one), F32),
            pltpu.VMEM((NZ, 2, *one), BF16),
            pltpu.VMEM((NZ, heads, rows, rows), F32),
            pltpu.VMEM((NZ, heads, rows, rows), F32),
            pltpu.VMEM(one, F32),
            pltpu.VMEM(one, F32),
            pltpu.VMEM(one, F32),
            pltpu.VMEM(one, F32),
            pltpu.VMEM(one, F32),
            pltpu.VMEM((2, 4, 2, *one), BF16),
            pltpu.VMEM((2, 4, 2, *one), BF16),
            pltpu.VMEM((4, NQ, rows, width), BF16),
            pltpu.VMEM((rows, 3 * width), BF16),
            pltpu.VMEM((NQ, NZ, own, rows), BF16),
            pltpu.VMEM((NQ, NZ, own, rows), BF16),
            pltpu.VMEM((NZ, NQ, own, rows), BF16),
            pltpu.VMEM((NZ, NQ, own, rows), BF16),
            pltpu.VMEM((2, 2, NZ * NQ, own, width), BF16),
            pltpu.VMEM((NT, rows, width), BF16),
            pltpu.VMEM((NT, rows, width), F32),
            pltpu.VMEM((2, rows, HD), F32),
            pltpu.VMEM((2, 4, 4, own, width), BF16),
            pltpu.VMEM((2, 4, 4, own, width), BF16),
            pltpu.VMEM((4, NZ * own, width), F32),
            pltpu.VMEM((2, 2, 2, rows, width), BF16),
            pltpu.VMEM((2, 2, 2, rows, width), BF16),
            pltpu.VMEM((rows, width), BF16),
            pltpu.VMEM((rows, width), BF16),
            pltpu.VMEM((NT, 16, rows), F32),
            dma,
            dma((2, 4, 2)),
            dma,
            dma((2, 4, 2)),
            dma((2,)),
            dma((2,)),
            dma,
            dma((4, 3)),
            dma,
            dma((2, 4, 4)),
            dma,
            dma((2, 2, 2)),
            dma,
            dma,
            dma,
            dma,
            dma,
            dma((2, 2, 4)),
            dma((2, 2, 2, 4)),
            dma((2, 5)),
            dma((2,)),
            dma((2, 5)),
            dma,
            dma,
            dma,
        ],
        compiler_params=pltpu.CompilerParams(
            collective_id=0, has_side_effects=True, vmem_limit_bytes=67_043_328
        ),
    )(tokens, cot, own_qkv, own_out)


def finish(*arrays):
    def kernel(*refs):
        for i in range(len(arrays)):
            refs[len(arrays) + i][...] = refs[i][...]

    vmem = pl.BlockSpec(memory_space=pltpu.VMEM)
    return pl.pallas_call(
        kernel,
        out_shape=tuple(jax.ShapeDtypeStruct(a.shape, a.dtype) for a in arrays),
        in_specs=[vmem] * len(arrays),
        out_specs=(vmem,) * len(arrays),
    )(*arrays)


def local(tokens, cotangent, qkv_weight, out_weight):
    qkv_grad, out_grad, branch = finish(
        *layer(tokens[0], cotangent[0], jnp.transpose(qkv_weight, (1, 0, 2)), out_weight)
    )
    return (jnp.transpose(qkv_grad, (1, 0, 2)), out_grad, branch[None])


def solution(mesh):
    return jax.shard_map(
        local,
        mesh=mesh,
        in_specs=(
            P("dp", "seq", None),
            P("dp", "seq", None),
            P(("seq", "dp"), None, "tensor"),
            P(("seq", "dp"), "tensor"),
        ),
        out_specs=(
            P(("seq", "dp"), None, "tensor"),
            P(("seq", "dp"), "tensor"),
            P("dp", "seq", "tensor"),
        ),
        check_vma=False,
    )
```
